8 devices in a mesh: rep: 2 (over z, y), kv: 4 (over x, core).
Axes of the slice: x: 2, y: 2, z: 1, core: 2. Of those that a mesh axis runs over, the one named last changes fastest.
Arguments:
- embeds: bfloat16 [2, 128, 4096], P(None, ('rep', 'kv')), parts along dimension 1
- w_query: bfloat16 [2, 4096, 4096], replicated
- w_key: bfloat16 [2, 4096, 1024], replicated
- w_value: bfloat16 [2, 4096, 1024], replicated
- w_out: bfloat16 [2, 4096, 4096], replicated
- w_up: bfloat16 [2, 4096, 14336], replicated
- w_down: bfloat16 [2, 14336, 4096], replicated
- k_pool: bfloat16 [768, 2, 32, 8, 128], P(('rep', 'kv')), parts along dimension 0
- v_pool: bfloat16 [768, 2, 32, 8, 128], P(('rep', 'kv')), parts along dimension 0
- new_table: int32 [128, 2], P('rep'), parts along dimension 0
- seq_lens: int32 [128], P('rep'), parts along dimension 0
- mig_src: int32 [128], P('rep'), parts along dimension 0
- mig_dst: int32 [128], P('rep'), parts along dimension 0
Outputs:
- output 1: bfloat16 [2, 128, 4096], P(None, ('rep', 'kv')), parts along dimension 1
- output 2: bfloat16 [768, 2, 32, 8, 128], P(('rep', 'kv')), parts along dimension 0
- output 3: bfloat16 [768, 2, 32, 8, 128], P(('rep', 'kv')), parts along dimension 0
There are 2 independent parts. The reference program is written for one: setup_inputs(seed, part) draws one part's arguments, and reference() takes and returns one part's arrays. A program takes and returns all parts, laid end to end along the dimension named above; an argument that names none is the same for every part.
All inputs are finite; a program needn't handle non-finite values.
Results may differ from the reference program's by a relative error of at most 0.0163449.
Values are sent between devices in bfloat16 or wider.
A program may use at most 2.75 GiB of HBM per device.

```python
import jax
import jax.numpy as jnp
from jax import lax

D = 4096
HEADS = 32
KV_HEADS = 8
HEAD = 128
FF = 14336
PAGE = 32
LAYERS = 2
GROUP = 4
SEQ_DEV = 16
PAGES_SEQ = 2
MIG = 64
BATCH = GROUP * SEQ_DEV
SLOTS = PAGES_SEQ * SEQ_DEV + MIG


def draw_layout(layout_key):
    key_hot, key_shift, key_perm, key_rank, key_len = jax.random.split(layout_key, 5)
    hot_dev = jax.random.randint(key_hot, (), 0, GROUP)
    alt_dev = (hot_dev + GROUP // 2) % GROUP
    dev_shift = jax.random.randint(key_shift, (), 0, GROUP)
    slot_perm = jax.vmap(lambda sub_key: jax.random.permutation(sub_key, SLOTS))(jax.random.split(key_perm, GROUP))
    seq_ids = jnp.arange(BATCH)[:, None]
    page_ids = jnp.arange(PAGES_SEQ)[None, :]
    home_dev = seq_ids // SEQ_DEV
    base_dev = (home_dev + page_ids + dev_shift) % GROUP
    base_local = slot_perm[base_dev, page_ids * SEQ_DEV + seq_ids % SEQ_DEV]
    new_table = (base_dev * SLOTS + base_local).astype(jnp.int32)
    eligible = (base_dev != hot_dev) & (base_dev != alt_dev)
    is_last = jnp.broadcast_to(page_ids == PAGES_SEQ - 1, (BATCH, PAGES_SEQ))
    total_pages = BATCH * PAGES_SEQ
    rank_ids = jax.random.permutation(key_rank, total_pages).reshape(BATCH, PAGES_SEQ)
    priority = jnp.where(eligible, jnp.where(is_last, 0, total_pages), 2 * total_pages) + rank_ids
    chosen = jnp.argsort(priority.reshape(-1))[:MIG]
    entry_ids = jnp.arange(MIG)
    src_dev = jnp.where(entry_ids % 8 == 7, alt_dev, hot_dev)
    src_local = slot_perm[src_dev, PAGES_SEQ * SEQ_DEV + entry_ids]
    mig_src = (src_dev * SLOTS + src_local).astype(jnp.int32)
    mig_dst = new_table.reshape(-1)[chosen]
    len_offsets = jax.random.randint(key_len, (BATCH,), 0, PAGE - 1)
    len_offsets = len_offsets.at[0].set(PAGE - 2).at[1].set(0)
    seq_lens = ((PAGES_SEQ - 1) * PAGE + len_offsets).astype(jnp.int32)
    return new_table, seq_lens, mig_src, mig_dst


def setup_inputs(seed: int = 0, part: int = 0) -> dict:
    base_key = jax.random.key(seed)
    part_key = jax.random.fold_in(base_key, part)
    w_keys = jax.random.split(base_key, 6)
    p_keys = jax.random.split(part_key, 5)
    new_table, seq_lens, mig_src, mig_dst = draw_layout(p_keys[0])
    embeds = jax.random.normal(p_keys[1], (2, BATCH, D), jnp.float32).astype(jnp.bfloat16)
    out_scale = (PAGES_SEQ / (HEADS * HEAD)) ** 0.5
    w_query = (jax.random.normal(w_keys[0], (LAYERS, D, HEADS * HEAD), jnp.float32) * 0.5 * D ** -0.5).astype(jnp.bfloat16)
    w_key = (jax.random.normal(w_keys[1], (LAYERS, D, KV_HEADS * HEAD), jnp.float32) * D ** -0.5).astype(jnp.bfloat16)
    w_value = (jax.random.normal(w_keys[2], (LAYERS, D, KV_HEADS * HEAD), jnp.float32) * D ** -0.5).astype(jnp.bfloat16)
    w_out = (jax.random.normal(w_keys[3], (LAYERS, HEADS * HEAD, D), jnp.float32) * out_scale).astype(jnp.bfloat16)
    w_up = (jax.random.normal(w_keys[4], (LAYERS, D, FF), jnp.float32) * D ** -0.5).astype(jnp.bfloat16)
    w_down = (jax.random.normal(w_keys[5], (LAYERS, FF, D), jnp.float32) * FF ** -0.5).astype(jnp.bfloat16)
    pool_shape = (GROUP * SLOTS, LAYERS, PAGE, KV_HEADS, HEAD)
    k_pool = jax.random.normal(p_keys[2], pool_shape, jnp.float32).astype(jnp.bfloat16)
    slot_mean = jax.random.normal(p_keys[3], (GROUP * SLOTS, LAYERS, 1, KV_HEADS, HEAD), jnp.float32)
    v_pool = (0.5 * jax.random.normal(p_keys[4], pool_shape, jnp.float32) + slot_mean).astype(jnp.bfloat16)
    return {'embeds': embeds, 'w_query': w_query, 'w_key': w_key, 'w_value': w_value, 'w_out': w_out, 'w_up': w_up, 'w_down': w_down, 'k_pool': k_pool, 'v_pool': v_pool, 'new_table': new_table, 'seq_lens': seq_lens, 'mig_src': mig_src, 'mig_dst': mig_dst}


def attend_all(queries, k_layer, v_layer, new_table, seq_lens, step_idx):
    group_heads = HEADS // KV_HEADS
    positions = jnp.arange(PAGES_SEQ)[:, None] * PAGE + jnp.arange(PAGE)[None, :]

    def one_seq(args):
        q_row, row_slots, seq_len = args
        keys_f = k_layer[row_slots].astype(jnp.float32)
        vals_f = v_layer[row_slots].astype(jnp.float32)
        q_grp = q_row.astype(jnp.float32).reshape(KV_HEADS, group_heads, HEAD)
        scores = jnp.einsum('kgd,pikd->kgpi', q_grp, keys_f) * HEAD ** -0.5
        scores = jnp.where(positions <= seq_len + step_idx, scores, -jnp.inf)
        flat_scores = scores.reshape(KV_HEADS, group_heads, PAGES_SEQ * PAGE)
        probs_f = jax.nn.softmax(flat_scores, axis=-1).reshape(scores.shape)
        attn_f = jnp.einsum('kgpi,pikd->kgd', probs_f, vals_f)
        return attn_f.reshape(HEADS * HEAD).astype(jnp.bfloat16)

    return lax.map(one_seq, (queries, new_table, seq_lens))


def reference(embeds, w_query, w_key, w_value, w_out, w_up, w_down, k_pool, v_pool, new_table, seq_lens, mig_src, mig_dst):
    k_pool = k_pool.at[mig_dst].set(k_pool[mig_src]).at[mig_src].set(0)
    v_pool = v_pool.at[mig_dst].set(v_pool[mig_src]).at[mig_src].set(0)
    batch_rows = embeds.shape[1]
    step_outs = []
    for step_idx in range(2):
        hidden = embeds[step_idx]
        positions = seq_lens + step_idx
        slot_ids = jnp.take_along_axis(new_table, (positions // PAGE)[:, None], axis=1)[:, 0]
        offsets = positions % PAGE
        for layer_idx in range(LAYERS):
            queries = jnp.dot(hidden, w_query[layer_idx], preferred_element_type=jnp.float32).astype(jnp.bfloat16)
            new_keys = jnp.dot(hidden, w_key[layer_idx], preferred_element_type=jnp.float32).astype(jnp.bfloat16).reshape(batch_rows, KV_HEADS, HEAD)
            new_vals = jnp.dot(hidden, w_value[layer_idx], preferred_element_type=jnp.float32).astype(jnp.bfloat16).reshape(batch_rows, KV_HEADS, HEAD)
            k_pool = k_pool.at[slot_ids, layer_idx, offsets].set(new_keys)
            v_pool = v_pool.at[slot_ids, layer_idx, offsets].set(new_vals)
            attn_out = attend_all(queries.reshape(batch_rows, HEADS, HEAD), k_pool[:, layer_idx], v_pool[:, layer_idx], new_table, seq_lens, step_idx)
            hidden = (hidden.astype(jnp.float32) + jnp.dot(attn_out, w_out[layer_idx], preferred_element_type=jnp.float32)).astype(jnp.bfloat16)
            up_proj = jnp.dot(hidden, w_up[layer_idx], preferred_element_type=jnp.float32).astype(jnp.bfloat16)
            act_vals = jax.nn.gelu(up_proj.astype(jnp.float32), approximate=True).astype(jnp.bfloat16)
            hidden = (hidden.astype(jnp.float32) + jnp.dot(act_vals, w_down[layer_idx], preferred_element_type=jnp.float32)).astype(jnp.bfloat16)
        step_outs.append(hidden)
    return jnp.stack(step_outs), k_pool, v_pool
```

```python
import functools

import jax
import jax.numpy as jnp
from jax import lax
from jax.experimental import pallas as pl
from jax.experimental.pallas import tpu as pltpu
from jax.sharding import PartitionSpec as P

BF16 = jnp.bfloat16
F32 = jnp.float32
MESH = pl.DeviceIdType.MESH
NEG = -3.0e38
VMEM_LIMIT = 60 * 1024 * 1024

D = 4096
HEADS = 32
KV_HEADS = 8
HEAD = 128
FF = 14336
PAGE = 32
LAYERS = 2
SEQS = 64
TOK = 64
HALF_HEADS = HEADS // 2
ROWS = TOK * HALF_HEADS
TN = 512
SCALE = HEAD ** -0.5


def dot(a, b):
    return jnp.dot(a, b, preferred_element_type=F32)


def places():
    me = lax.axis_index('kv')
    core = lax.rem(me, 2)
    chip = me // 2
    partner = me + 1 - 2 * core
    across = lax.rem(me + 2, 4)
    diag = lax.rem(partner + 2, 4)
    return me, chip, core, partner, across, diag


def meet(peers):
    barrier = pltpu.get_barrier_semaphore()
    for peer in peers:
        pl.semaphore_signal(barrier, inc=1, device_id={'kv': peer}, device_id_type=MESH)
    pl.semaphore_wait(barrier, len(peers))


def send(src, dst, send_sem, recv_sem, peer):
    return pltpu.make_async_remote_copy(src_ref=src, dst_ref=dst, send_sem=send_sem, recv_sem=recv_sem, device_id={'kv': peer}, device_id_type=MESH)


VMEM = pl.BlockSpec(memory_space=pltpu.VMEM)
ANY = pl.BlockSpec(memory_space=pl.ANY)
DMA = pltpu.SemaphoreType.DMA


def qkv_kernel(layer, first, *refs):
    if first:
        emb, wq, wk, wv, q_all, kv, h, wbuf, wsem, psend, precv, xsend, xrecv, fsend, frecv, hsend, hrecv = refs
    else:
        h, wq, wk, wv, q_all, kv, wbuf, wsem, psend, precv, xsend, xrecv, fsend, frecv = refs
    me, chip, core, partner, across, diag = places()

    def fetch(j):
        if j < 4:
            src = wq.at[layer, :, pl.ds(pl.multiple_of(core * 2048 + j * TN, TN), TN)]
        else:
            src = (wk, wv)[j - 4].at[layer, :, pl.ds(pl.multiple_of(core * TN, TN), TN)]
        return pltpu.make_async_copy(src, wbuf.at[j], wsem.at[j])

    for j in range(6):
        fetch(j).start()
    meet((partner, across))
    if first:
        copies = []
        for t in range(2):
            rows = pl.ds(pl.multiple_of(t * 32 + core * 16, 16), 16)
            h[rows, :] = emb[t]
            copies.append(send(emb.at[t], h.at[rows, :], hsend.at[t], hrecv.at[t], partner))
        for copy in copies:
            copy.start()
        for copy in copies:
            copy.wait()

    def to_partner(j):
        ref = q_all.at[chip, core * 4 + j]
        return send(ref, ref, psend.at[j], precv.at[j], partner)

    def to_across(j):
        ref = q_all.at[chip, core * 4 + j]
        return send(ref, ref, xsend.at[j], xrecv.at[j], across)

    def forward(j):
        ref = q_all.at[1 - chip, core * 4 + j]
        return send(ref, ref, fsend.at[j], frecv.at[j], partner)

    for j in range(6):
        fetch(j).wait()
        tile = dot(h[...], wbuf[j]).astype(BF16)
        if j < 4:
            q_all[chip, core * 4 + j] = tile
        else:
            kv[:, (j - 4) * TN:(j - 3) * TN] = tile
        if 1 <= j <= 4:
            to_across(j - 1).start()
            to_partner(j - 1).start()
    for j in range(4):
        to_across(j).wait_recv()
        forward(j).start()
    for j in range(4):
        to_across(j).wait_send()
        to_partner(j).wait()
        forward(j).wait()


def run_qkv(layer, h, weights, first):
    wq, wk, wv = weights[:3]
    out_shape = [jax.ShapeDtypeStruct((2, 8, TOK, TN), BF16), jax.ShapeDtypeStruct((TOK, 2 * TN), BF16)]
    if first:
        out_shape.append(jax.ShapeDtypeStruct((TOK, D), BF16))
    scratch = [pltpu.VMEM((6, D, TN), BF16), DMA((6,))] + [DMA((4,))] * 6
    if first:
        scratch += [DMA((2,))] * 2
    return pl.pallas_call(
        functools.partial(qkv_kernel, layer, first),
        name=f'qkv{layer}',
        out_shape=out_shape,
        in_specs=[VMEM, ANY, ANY, ANY],
        out_specs=[VMEM] * len(out_shape),
        scratch_shapes=scratch,
        cost_estimate=pl.CostEstimate(flops=2 * TOK * D * 6 * TN * 8, bytes_accessed=D * 6 * TN * 2, transcendentals=0),
        compiler_params=pltpu.CompilerParams(collective_id=layer * 3, has_side_effects=True, vmem_limit_bytes=VMEM_LIMIT),
    )(h, wq, wk, wv)


UNROLL = 2
NBUF = 3


def attend_kernel(layer, count, table, q_all, k_pool, v_pool, part_o, part_l, q_rows, kbuf, vbuf, sems):
    part_o[...] = jnp.zeros_like(part_o)
    part_l[...] = jnp.full_like(part_l, NEG)
    groups = (count[0] + UNROLL - 1) // UNROLL

    def copies(g, start):
        slot = lax.rem(g, NBUF)
        for u in range(UNROLL):
            for j in range(2):
                page = table[1 + j, g * UNROLL + u]
                for pool, buf in ((k_pool, kbuf), (v_pool, vbuf)):
                    copy = pltpu.make_async_copy(pool.at[page, layer], buf.at[slot, u, j], sems.at[slot])
                    copy.start() if start else copy.wait()

    for g in range(NBUF - 1):
        @pl.when(g < groups)
        def _():
            copies(g, True)

    for chip in range(2):
        for tile in range(8):
            for i in range(4):
                rows = q_all[chip, tile, :, i * HEAD:(i + 1) * HEAD].astype(F32)
                q_rows[pl.ds(chip * TOK * HEADS + tile * 4 + i, TOK, stride=HEADS), :] = rows

    row = lax.broadcasted_iota(jnp.int32, (2 * HEADS, 256), 0)
    col = lax.broadcasted_iota(jnp.int32, (2 * HEADS, 256), 1)
    pos = jnp.where((row % HEADS) // 4 == col % KV_HEADS, col // KV_HEADS, PAGE)

    def step(g, carry):
        slot = lax.rem(g, NBUF)
        copies(g, False)

        @pl.when(g + NBUF - 1 < groups)
        def _():
            copies(g + NBUF - 1, True)

        outs = []
        for u in range(UNROLL):
            item = g * UNROLL + u
            seq = table[0, item]
            base = (seq // 32) * TOK * HEADS + (seq % 32) * HEADS
            q0 = q_rows[pl.ds(pl.multiple_of(base, HEADS), HEADS), :]
            q1 = q_rows[pl.ds(pl.multiple_of(base + 32 * HEADS, HEADS), HEADS), :]
            q = jnp.concatenate([q0, q1], axis=0).astype(BF16)
            scores = []
            for j in range(2):
                s = lax.dot_general(q, kbuf[slot, u, j], (((1,), (1,)), ((), ())), preferred_element_type=F32) * SCALE
                scores.append(jnp.where(pos < table[3 + j, item], s, NEG))
            top = jnp.max(jnp.maximum(scores[0], scores[1]), axis=1, keepdims=True)
            probs = [jnp.where(s > NEG, jnp.exp(s - top), 0.0) for s in scores]
            total = jnp.sum(probs[0] + probs[1], axis=1, keepdims=True)
            out = sum(dot(p.astype(BF16), vbuf[slot, u, j]) for j, p in enumerate(probs))
            live = total > 0.0
            safe = jnp.where(live, total, 1.0)
            lse = jnp.where(live, top + jnp.log(safe), NEG)
            outs.append((seq, out / safe, jnp.broadcast_to(lse, (2 * HEADS, HEAD))))
        for seq, out, lse in outs:
            for t in range(2):
                for half in range(2):
                    rows = slice(t * HEADS + half * HALF_HEADS, t * HEADS + (half + 1) * HALF_HEADS)
                    part_o[seq // 32, half, t * 32 + seq % 32] = out[rows]
                    part_l[seq // 32, half, t * 32 + seq % 32] = lse[rows]
        return carry

    lax.fori_loop(0, groups, step, 0)


def run_attend(layer, count, table, q_all, k_pool, v_pool):
    slots = k_pool.shape[0]
    shape = jax.ShapeDtypeStruct((2, 2, TOK, HALF_HEADS, HEAD), F32)
    page = (UNROLL, 2, PAGE * KV_HEADS, HEAD)
    smem = pl.BlockSpec(memory_space=pltpu.SMEM)
    return pl.pallas_call(
        functools.partial(attend_kernel, layer),
        name=f'attend{layer}',
        out_shape=[shape, shape],
        in_specs=[smem, smem, VMEM, ANY, ANY],
        out_specs=[VMEM, VMEM],
        scratch_shapes=[
            pltpu.VMEM((2 * TOK * HEADS, HEAD), F32),
            pltpu.VMEM((NBUF,) + page, BF16),
            pltpu.VMEM((NBUF,) + page, BF16),
            DMA((NBUF,)),
        ],
        cost_estimate=pl.CostEstimate(flops=2 * 10 ** 10, bytes_accessed=16 * 2 ** 20, transcendentals=0),
        compiler_params=pltpu.CompilerParams(vmem_limit_bytes=VMEM_LIMIT),
    )(count, table, q_all, k_pool.reshape(slots, LAYERS, PAGE * KV_HEADS, HEAD), v_pool.reshape(slots, LAYERS, PAGE * KV_HEADS, HEAD))


def merge(parts):
    top = functools.reduce(jnp.maximum, [l for _, l in parts])
    weights = [jnp.exp(l - top) for _, l in parts]
    total = functools.reduce(jnp.add, weights)
    out = functools.reduce(jnp.add, [w * o for w, (o, _) in zip(weights, parts)]) / total
    return out, top + jnp.log(total)


CH = 64


def out_kernel(layer, h, q_all, kv, part_o, part_l, wo, out, wbuf, wsem, got_o, got_l, mine_o, mine_l, give_o, give_l, far_o, far_l,
               q_rows, k_rows, v_rows, attn, psend, precv, dsend, drecv, xsend, xrecv, ssem, rsem):
    me, chip, core, partner, across, diag = places()

    def fetch(j):
        src = wo.at[layer, pl.ds(pl.multiple_of(core * 2048, 2048), 2048), pl.ds(j * TN, TN)]
        return pltpu.make_async_copy(src, wbuf.at[j], wsem.at[j])

    for j in range(8):
        fetch(j).start()
    meet((partner, across))

    near = []
    for which in range(2):
        owner = 1 - chip if which == 0 else chip
        pair = [
            send(part_o.at[owner, 1 - core], got_o.at[which], dsend.at[which, 0], drecv.at[which, 0], partner),
            send(part_l.at[owner, 1 - core], got_l.at[which], dsend.at[which, 1], drecv.at[which, 1], partner),
        ]
        for copy in pair:
            copy.start()
        near.append(pair)

    lane = lax.broadcasted_iota(jnp.int32, (8, HEAD), 1)

    for copy in near[0]:
        copy.wait_recv()
    compact = jnp.zeros((8, HEAD), F32)
    for i in range(TOK):
        o, l = merge([(part_o[1 - chip, core, i], part_l[1 - chip, core, i]), (got_o[0, i], got_l[0, i])])
        give_o[i] = o
        compact = jnp.where(lane == 2 * i, l[:8], compact)
        compact = jnp.where(lane == 2 * i + 1, l[8:], compact)
    give_l[...] = compact
    far = [
        send(give_l, far_l, xsend.at[0], xrecv.at[0], across),
        send(give_o, far_o, xsend.at[1], xrecv.at[1], across),
    ]
    for copy in far:
        copy.start()

    for head in range(HALF_HEADS):
        tile = core * 4 + head // 4
        rows = pl.ds(head, TOK, stride=HALF_HEADS)
        q_rows[rows, :] = q_all[chip, tile, :, (head % 4) * HEAD:(head % 4 + 1) * HEAD].astype(F32)
        k_rows[rows, :] = kv[:, (head // 4) * HEAD:(head // 4 + 1) * HEAD].astype(F32)
        v_rows[rows, :] = kv[:, TN + (head // 4) * HEAD:TN + (head // 4 + 1) * HEAD].astype(F32)
    for copy in near[1]:
        copy.wait_recv()

    half = ROWS // 2

    def score(q, k):
        s = jnp.sum(q * k, axis=1, keepdims=True) * SCALE
        return jnp.broadcast_to(s, q.shape)

    def own(i, carry):
        a = pl.ds(pl.multiple_of(i * HALF_HEADS, HALF_HEADS), HALF_HEADS)
        b = pl.ds(pl.multiple_of(half + i * HALF_HEADS, HALF_HEADS), HALF_HEADS)
        k0, v0, k1, v1 = k_rows[a, :], v_rows[a, :], k_rows[b, :], v_rows[b, :]
        q0, q1 = q_rows[a, :], q_rows[b, :]
        j = i + TOK // 2
        o, l = merge([(part_o[chip, core, i], part_l[chip, core, i]), (got_o[1, i], got_l[1, i]), (v0, score(q0, k0))])
        mine_o[i] = o
        mine_l[i] = l
        o, l = merge([(part_o[chip, core, j], part_l[chip, core, j]), (got_o[1, j], got_l[1, j]), (v0, score(q1, k0)), (v1, score(q1, k1))])
        mine_o[j] = o
        mine_l[j] = l
        return carry

    lax.fori_loop(0, TOK // 2, own, 0)

    for copy in far:
        copy.wait_recv()
    spread = far_l[...]
    for i in range(TOK):
        l = jnp.concatenate([
            jnp.broadcast_to(spread[:, 2 * i:2 * i + 1], (8, HEAD)),
            jnp.broadcast_to(spread[:, 2 * i + 1:2 * i + 2], (8, HEAD)),
        ], axis=0)
        o, _ = merge([(mine_o[i], mine_l[i]), (far_o[i], l)])
        q_rows[i * HALF_HEADS:(i + 1) * HALF_HEADS, :] = o
    for head in range(HALF_HEADS):
        attn[:, head * HEAD:(head + 1) * HEAD] = q_rows[pl.ds(head, TOK, stride=HALF_HEADS), :].astype(BF16)

    def reduce(j):
        return send(psend.at[j], precv.at[j], ssem.at[j], rsem.at[j], partner)

    def project(j, carry):
        pltpu.make_async_copy(wo.at[layer, pl.ds(0, 2048), pl.ds(0, TN)], wbuf.at[j], wsem.at[j]).wait()
        psend[j] = dot(attn[...], wbuf[j])

        @pl.when(j > 0)
        def _():
            reduce(j - 1).start()
        return carry

    lax.fori_loop(0, 8, project, 0)
    reduce(7).start()
    for j in range(8):
        reduce(j).wait_recv()
        cols = slice(j * TN, (j + 1) * TN)
        out[:, cols] = (h[:, cols].astype(F32) + (psend[j] + precv[j])).astype(BF16)
    for j in range(8):
        reduce(j).wait_send()
    for pair in near:
        for copy in pair:
            copy.wait_send()
    for copy in far:
        copy.wait_send()


def run_out(layer, h, q_all, kv, part_o, part_l, w_out):
    token = (TOK, HALF_HEADS, HEAD)
    return pl.pallas_call(
        functools.partial(out_kernel, layer),
        name=f'out{layer}',
        out_shape=jax.ShapeDtypeStruct((TOK, D), BF16),
        in_specs=[VMEM] * 5 + [ANY],
        out_specs=VMEM,
        scratch_shapes=[
            pltpu.VMEM((8, 2048, TN), BF16),
            DMA((8,)),
            pltpu.VMEM((2,) + token, F32),
            pltpu.VMEM((2,) + token, F32),
            pltpu.VMEM(token, F32),
            pltpu.VMEM(token, F32),
            pltpu.VMEM(token, F32),
            pltpu.VMEM((8, HEAD), F32),
            pltpu.VMEM(token, F32),
            pltpu.VMEM((8, HEAD), F32),
            pltpu.VMEM((ROWS, HEAD), F32),
            pltpu.VMEM((ROWS, HEAD), F32),
            pltpu.VMEM((ROWS, HEAD), F32),
            pltpu.VMEM((TOK, 2048), BF16),
            pltpu.VMEM((8, TOK, TN), F32),
            pltpu.VMEM((8, TOK, TN), F32),
            DMA((2, 2)),
            DMA((2, 2)),
            DMA((2,)),
            DMA((2,)),
            DMA((8,)),
            DMA((8,)),
        ],
        cost_estimate=pl.CostEstimate(flops=10 ** 11, bytes_accessed=20 * 2 ** 20, transcendentals=0),
        compiler_params=pltpu.CompilerParams(collective_id=layer * 3 + 1, has_side_effects=True, vmem_limit_bytes=VMEM_LIMIT),
    )(h, q_all, kv, part_o, part_l, w_out)


NU = 4
ND = 4
UP_TILES = FF // 2 // TN
KROWS = FF // 4
DOWN_TILES = 2 * (D // TN)


def mlp_kernel(layer, h, kv, w_up, w_down, out, kv_all, ubuf, dbuf, act, psend, precv, usem, dsem, ssem, rsem, ksend, krecv):
    me, chip, core, partner, across, diag = places()

    def fetch_up(s):
        src = w_up.at[layer, :, pl.ds(pl.multiple_of(core * (FF // 2) + s * TN, TN), TN)]
        slot = lax.rem(s, NU)
        return pltpu.make_async_copy(src, ubuf.at[slot], usem.at[slot])

    def fetch_down(s):
        src = w_down.at[layer, pl.ds(pl.multiple_of(core * (FF // 2) + lax.rem(s, 2) * KROWS, KROWS), KROWS), pl.ds(pl.multiple_of((s // 2) * TN, TN), TN)]
        slot = lax.rem(s, ND)
        return pltpu.make_async_copy(src, dbuf.at[slot], dsem.at[slot])

    for s in range(NU):
        fetch_up(jnp.int32(s)).start()
    meet((partner, across, diag))
    kv_all[me] = kv[...]
    rows = [send(kv, kv_all.at[me], ksend.at[i], krecv.at[i], peer) for i, peer in enumerate((partner, across, diag))]
    for copy in rows:
        copy.start()

    def up(s, carry):
        fetch_up(s).wait()
        u = dot(h[...], ubuf[lax.rem(s, NU)]).astype(BF16)
        a = jax.nn.gelu(u.astype(F32), approximate=True).astype(BF16)
        act[s // 7, :, pl.ds(pl.multiple_of(lax.rem(s, 7) * TN, TN), TN)] = a

        @pl.when(s + NU < UP_TILES)
        def _():
            fetch_up(s + NU).start()

        @pl.when(s + NU >= UP_TILES)
        def _():
            fetch_down(s + NU - UP_TILES).start()
        return carry

    lax.fori_loop(0, UP_TILES, up, 0)

    def reduce(j):
        return send(psend.at[j], precv.at[j], ssem.at[j], rsem.at[j], partner)

    def down(j, carry):
        total = None
        for k in range(2):
            s = 2 * j + k
            fetch_down(s).wait()
            part = dot(act[k], dbuf[lax.rem(s, ND)])
            total = part if total is None else total + part

            @pl.when(s + ND < DOWN_TILES)
            def _():
                fetch_down(s + ND).start()
        psend[j] = total

        @pl.when(j > 0)
        def _():
            reduce(j - 1).start()
        return carry

    lax.fori_loop(0, 8, down, 0)
    reduce(7).start()
    for j in range(8):
        reduce(j).wait_recv()
        cols = slice(j * TN, (j + 1) * TN)
        out[:, cols] = (h[:, cols].astype(F32) + (psend[j] + precv[j])).astype(BF16)
    for j in range(8):
        reduce(j).wait_send()
    for copy in rows:
        copy.wait()


def run_mlp(layer, h, kv, w_up, w_down):
    return pl.pallas_call(
        functools.partial(mlp_kernel, layer),
        name=f'mlp{layer}',
        out_shape=[jax.ShapeDtypeStruct((TOK, D), BF16), jax.ShapeDtypeStruct((4, TOK, 2 * TN), BF16)],
        in_specs=[VMEM, VMEM, ANY, ANY],
        out_specs=[VMEM, VMEM],
        scratch_shapes=[
            pltpu.VMEM((NU, D, TN), BF16),
            pltpu.VMEM((ND, KROWS, TN), BF16),
            pltpu.VMEM((2, TOK, KROWS), BF16),
            pltpu.VMEM((8, TOK, TN), F32),
            pltpu.VMEM((8, TOK, TN), F32),
            DMA((NU,)),
            DMA((ND,)),
            DMA((8,)),
            DMA((8,)),
            DMA((3,)),
            DMA((3,)),
        ],
        cost_estimate=pl.CostEstimate(flops=2 * TOK * D * FF * 8, bytes_accessed=D * FF * 2, transcendentals=0),
        compiler_params=pltpu.CompilerParams(collective_id=layer * 3 + 2, has_side_effects=True, vmem_limit_bytes=VMEM_LIMIT),
    )(h, kv, w_up, w_down)


RING = 8


def pools_kernel(table, k_pool, v_pool, k_moved, v_moved, k_rows, v_rows, k_out, v_out, buf, in_sem, out_sem):
    slots = k_pool.shape[0]

    def load(i, wait):
        slot = lax.rem(i, RING)
        kind = table[0, i]
        for p, (pool, moved) in enumerate(((k_pool, k_moved), (v_pool, v_moved))):
            dst = buf.at[slot, p]
            if wait:
                pltpu.make_async_copy(pool.at[0], dst, in_sem.at[slot, p]).wait()
            else:
                @pl.when(kind < 0)
                def _():
                    pltpu.make_async_copy(pool.at[i], dst, in_sem.at[slot, p]).start()

                @pl.when(kind >= 0)
                def _():
                    pltpu.make_async_copy(moved.at[kind], dst, in_sem.at[slot, p]).start()

    def store(i):
        slot = lax.rem(i, RING)
        return [pltpu.make_async_copy(buf.at[slot, p], ref.at[i], out_sem.at[slot, p]) for p, ref in enumerate((k_out, v_out))]

    AHEAD = RING // 2
    for i in range(AHEAD):
        load(jnp.int32(i), False)

    def step(i, carry):
        @pl.when((i + AHEAD < slots) & (i + AHEAD >= RING))
        def _():
            for copy in store(i + AHEAD - RING):
                copy.wait()

        @pl.when(i + AHEAD < slots)
        def _():
            load(i + AHEAD, False)
        load(i, True)
        slot = lax.rem(i, RING)

        @pl.when(table[1, i] > 0)
        def _():
            buf[slot] = jnp.zeros(buf.shape[1:], BF16)
        for t in range(2):
            row = table[2 + t, i]

            @pl.when(row >= 0)
            def _():
                off = table[4 + t, i]
                for l in range(LAYERS):
                    buf[slot, 0, l, off] = k_rows[l, row]
                    buf[slot, 1, l, off] = v_rows[l, row]
        for copy in store(i):
            copy.start()
        return carry

    lax.fori_loop(0, slots, step, 0)

    def drain(i, carry):
        for copy in store(i):
            copy.wait()
        return carry

    lax.fori_loop(slots - RING, slots, drain, 0)


def run_pools(table, k_pool, v_pool, k_moved, v_moved, k_rows, v_rows):
    smem = pl.BlockSpec(memory_space=pltpu.SMEM)
    shape = jax.ShapeDtypeStruct(k_pool.shape, BF16)
    return pl.pallas_call(
        pools_kernel,
        name='pools',
        out_shape=[shape, shape],
        in_specs=[smem, ANY, ANY, ANY, ANY, VMEM, VMEM],
        out_specs=[ANY, ANY],
        scratch_shapes=[
            pltpu.VMEM((RING, 2) + k_pool.shape[1:], BF16),
            DMA((RING, 2)),
            DMA((RING, 2)),
        ],
        cost_estimate=pl.CostEstimate(flops=2 * 10 ** 10, bytes_accessed=50 * 2 ** 20, transcendentals=0),
        compiler_params=pltpu.CompilerParams(vmem_limit_bytes=VMEM_LIMIT),
    )(table, k_pool, v_pool, k_moved, v_moved, k_rows, v_rows)


def pick(mask, values, fallback):
    return jnp.where(jnp.any(mask, axis=1), jnp.sum(jnp.where(mask, values[None, :], 0), axis=1), fallback)


def attend_tables(old_table, seq_lens, me, slots):
    local = old_table - me * slots
    owned = (local >= 0) & (local < slots)
    some = owned[:, 0] | owned[:, 1]
    ids = jnp.arange(SEQS, dtype=jnp.int32)
    rank = jnp.sum(jnp.where(some[None, :] & (ids[None, :] < ids[:, None]), 1, 0), axis=1)
    count = jnp.sum(some.astype(jnp.int32))
    first = jnp.where(owned[:, 0], local[:, 0], local[:, 1])
    second = jnp.where(owned[:, 1], local[:, 1], local[:, 0])
    lim_a = jnp.where(owned[:, 0], jnp.minimum(seq_lens, PAGE), 0)
    lim_b = jnp.where(owned[:, 1], jnp.maximum(seq_lens - PAGE, 0), 0)
    want = jnp.minimum(ids, count - 1)
    hit = some[None, :] & (rank[None, :] == want[:, None])
    features = jnp.stack([ids, first, second, lim_a, lim_b])
    table = jnp.sum(jnp.where(hit[None], features[:, None, :], 0), axis=2)
    return count.reshape(1), table.astype(jnp.int32)


def pool_tables(new_table, seq_lens, mig_src, mig_dst, me, slots):
    ids = me * slots + jnp.arange(slots, dtype=jnp.int32)
    moved = pick(ids[:, None] == mig_dst[None, :], jnp.arange(mig_dst.shape[0], dtype=jnp.int32), -1)
    gone = jnp.any(ids[:, None] == mig_src[None, :], axis=1).astype(jnp.int32)
    out = [moved, gone]
    seqs = jnp.arange(SEQS, dtype=jnp.int32)
    offsets = []
    for t in range(2):
        pos = seq_lens + t
        page = pos // PAGE
        slot = jnp.where(page == 0, new_table[:, 0], new_table[:, 1])
        hit = ids[:, None] == slot[None, :]
        out.append(pick(hit, (seqs // 32) * TOK + t * 32 + seqs % 32, -1))
        offsets.append(pick(hit, pos - page * PAGE, 0))
    return jnp.stack(out + offsets).astype(jnp.int32)


def moved_pages(k_pool, v_pool, mig_src, me):
    slots = k_pool.shape[0]
    local = mig_src - me * slots
    local = jnp.where((local >= 0) & (local < slots), local, slots)
    k_pages = jnp.take(k_pool, local, axis=0, mode='fill', fill_value=0)
    v_pages = jnp.take(v_pool, local, axis=0, mode='fill', fill_value=0)
    return lax.psum((k_pages, v_pages), 'kv')


def by_token(kv_all):
    x = kv_all.reshape(2, 2, TOK, 2, 4, HEAD)
    return x.transpose(3, 0, 2, 1, 4, 5).reshape(2, 2 * TOK, KV_HEADS, HEAD)


def solution(mesh):
    pool_spec = P(('rep', 'kv'))
    tok_spec = P(None, ('rep', 'kv'), None)

    def device_fn(embeds, w_query, w_key, w_value, w_out, w_up, w_down, k_pool, v_pool, new_table, seq_lens, mig_src, mig_dst):
        me = lax.axis_index('kv')
        slots = k_pool.shape[0]
        weights = (w_query, w_key, w_value)
        flat = new_table.reshape(-1)
        old_table = pick(flat[:, None] == mig_dst[None, :], mig_src, flat).reshape(new_table.shape)
        count, table = attend_tables(old_table, seq_lens, me, slots)
        k_moved, v_moved = moved_pages(k_pool, v_pool, mig_src, me)
        rows = []
        h = None
        for layer in range(LAYERS):
            if layer == 0:
                q_all, kv, h = run_qkv(layer, embeds, weights, True)
            else:
                q_all, kv = run_qkv(layer, h, weights, False)
            part_o, part_l = run_attend(layer, count, table, q_all, k_pool, v_pool)
            h = run_out(layer, h, q_all, kv, part_o, part_l, w_out)
            h, kv_all = run_mlp(layer, h, kv, w_up, w_down)
            rows.append(by_token(kv_all))
        rows = jnp.stack(rows)
        k_out, v_out = run_pools(pool_tables(new_table, seq_lens, mig_src, mig_dst, me, slots), k_pool, v_pool, k_moved, v_moved, rows[:, 0], rows[:, 1])
        y = lax.dynamic_slice_in_dim(h.reshape(2, 32, D), (me % 2) * 16, 16, axis=1)
        return y, k_out, v_out

    return jax.shard_map(device_fn, mesh=mesh, in_specs=(tok_spec, P(), P(), P(), P(), P(), P(), pool_spec, pool_spec, P('rep', None), P('rep'), P('rep'), P('rep')), out_specs=(tok_spec, pool_spec, pool_spec), check_vma=False)
```

```python
import functools

import jax
import jax.numpy as jnp
from jax import lax
from jax.experimental import pallas as pl
from jax.experimental.pallas import tpu as pltpu
from jax.sharding import PartitionSpec as P

BF16 = jnp.bfloat16
F32 = jnp.float32
MESH = pl.DeviceIdType.MESH
NEG = -3.0e38
VMEM_LIMIT = 60 * 1024 * 1024

D = 4096
HEADS = 32
KV_HEADS = 8
HEAD = 128
FF = 14336
PAGE = 32
LAYERS = 2
SEQS = 64
MIG = 64
TOK = 64
HALF_HEADS = HEADS // 2
ROWS = TOK * HALF_HEADS
TN = 512
SCALE = HEAD ** -0.5
LOG2E = 1.4426950408889634
SLOTS = 96
UNROLL = 4
FAST_PAGES = 32
BOX = jax.ShapeDtypeStruct((3 * MIG, 2, PAGE * KV_HEADS, HEAD), BF16)


def flat_pool(pool):
    return pool.reshape(pool.shape[0], LAYERS, PAGE * KV_HEADS, HEAD)


def dot(a, b):
    return jnp.dot(a, b, preferred_element_type=F32)


def places():
    me = lax.axis_index('kv')
    core = lax.rem(me, 2)
    chip = me // 2
    partner = me + 1 - 2 * core
    across = lax.rem(me + 2, 4)
    diag = lax.rem(partner + 2, 4)
    return me, chip, core, partner, across, diag


def meet(peers):
    barrier = pltpu.get_barrier_semaphore()
    for peer in peers:
        pl.semaphore_signal(barrier, inc=1, device_id={'kv': peer}, device_id_type=MESH)
    pl.semaphore_wait(barrier, len(peers))


def send(src, dst, send_sem, recv_sem, peer):
    return pltpu.make_async_remote_copy(src_ref=src, dst_ref=dst, send_sem=send_sem, recv_sem=recv_sem, device_id={'kv': peer}, device_id_type=MESH)


VMEM = pl.BlockSpec(memory_space=pltpu.VMEM)
SMEM = pl.BlockSpec(memory_space=pltpu.SMEM)
ANY = pl.BlockSpec(memory_space=pl.ANY)
DMA = pltpu.SemaphoreType.DMA


WINDOW = 3


def qkv_kernel(layer, first, *refs):
    if first:
        emb, wq, wk, wv, q_all, kv, h, wbuf, wsem, psend, precv, xsend, xrecv, fsend, frecv, hsend, hrecv = refs
    else:
        h, wq, wk, wv, q_all, kv, wbuf, wsem, psend, precv, xsend, xrecv, fsend, frecv = refs
    me, chip, core, partner, across, diag = places()

    def fetch(j):
        if j < 4:
            src = wq.at[layer, :, pl.ds(pl.multiple_of(core * 2048 + j * TN, TN), TN)]
        else:
            src = (wk, wv)[j - 4].at[layer, :, pl.ds(pl.multiple_of(core * TN, TN), TN)]
        return pltpu.make_async_copy(src, wbuf.at[j], wsem.at[j])

    for j in range(WINDOW):
        fetch(j).start()
    meet((partner, across))
    if first:
        copies = []
        for t in range(2):
            rows = pl.ds(pl.multiple_of(t * 32 + core * 16, 16), 16)
            h[rows, :] = emb[t]
            copies.append(send(emb.at[t], h.at[rows, :], hsend.at[t], hrecv.at[t], partner))
        for copy in copies:
            copy.start()
        for copy in copies:
            copy.wait()

    def to_partner(j):
        ref = q_all.at[chip, core * 4 + j]
        return send(ref, ref, psend.at[j], precv.at[j], partner)

    def to_across(j):
        ref = q_all.at[chip, core * 4 + j]
        return send(ref, ref, xsend.at[j], xrecv.at[j], across)

    def forward(j):
        ref = q_all.at[1 - chip, core * 4 + j]
        return send(ref, ref, fsend.at[j], frecv.at[j], partner)

    def tile(j, carry):
        pltpu.make_async_copy(wq.at[layer, :, pl.ds(0, TN)], wbuf.at[j], wsem.at[j]).wait()
        q_all[chip, core * 4 + j] = dot(h[...], wbuf[j]).astype(BF16)
        for i in range(4):
            if i + WINDOW < 6:
                pl.when(j == i)(lambda i=i: fetch(i + WINDOW).start())

        @pl.when(j > 0)
        def _():
            to_across(j - 1).start()
            to_partner(j - 1).start()
        return carry

    lax.fori_loop(0, 4, tile, 0)
    for j in range(4, 6):
        fetch(j).wait()
        kv[:, (j - 4) * TN:(j - 3) * TN] = dot(h[...], wbuf[j]).astype(BF16)
        if j == 4:
            to_across(3).start()
            to_partner(3).start()
    for j in range(4):
        to_across(j).wait_recv()
        forward(j).start()
    for j in range(4):
        to_across(j).wait_send()
        to_partner(j).wait()
        forward(j).wait()


def run_qkv(layer, h, weights, first):
    wq, wk, wv = weights[:3]
    out_shape = [jax.ShapeDtypeStruct((2, 8, TOK, TN), BF16), jax.ShapeDtypeStruct((TOK, 2 * TN), BF16)]
    if first:
        out_shape.append(jax.ShapeDtypeStruct((TOK, D), BF16))
    scratch = [pltpu.VMEM((6, D, TN), BF16), DMA((6,))] + [DMA((4,))] * 6
    if first:
        scratch += [DMA((2,))] * 2
    return pl.pallas_call(
        functools.partial(qkv_kernel, layer, first),
        name=f'qkv{layer}',
        out_shape=out_shape,
        in_specs=[VMEM, ANY, ANY, ANY],
        out_specs=[VMEM] * len(out_shape),
        scratch_shapes=scratch,
        cost_estimate=pl.CostEstimate(flops=2 * TOK * D * 6 * TN * 8, bytes_accessed=D * 6 * TN * 2, transcendentals=0),
        compiler_params=pltpu.CompilerParams(collective_id=layer, has_side_effects=True, vmem_limit_bytes=VMEM_LIMIT),
    )(h, wq, wk, wv)


def plan_kernel(new_table, seq_lens, mig_src, mig_dst, meta, items, slots, moved, rows, source, place_of, counts):
    me = lax.axis_index('kv')
    base = me * SLOTS

    def home(slot):
        return sum((slot >= i * SLOTS).astype(jnp.int32) for i in range(1, 4))

    def clear(i, carry):
        source[i] = -1
        place_of[i] = -1
        return carry

    lax.fori_loop(0, 4 * SLOTS, clear, 0, unroll=16)
    for i in range(16):
        counts[i] = 0

    def keep(i, carry):
        slots[i] = 0
        return carry

    lax.fori_loop(0, SLOTS, keep, 0, unroll=16)

    def entry(e, carry):
        n, even, odd = carry
        s, d = mig_src[e], mig_dst[e]
        hs, hd = home(s), home(d)
        pair = hs * 4 + hd
        rank = counts[pair]
        counts[pair] = rank + 1
        channel = (hs ^ hd) - 1
        place = channel * MIG + rank
        source[d] = s
        place_of[d] = place
        misfit = ((channel == 1) | (rank >= FAST_PAGES)).astype(jnp.int32)
        even = even | misfit | (hs & 1)
        odd = odd | misfit | (1 - (hs & 1))

        @pl.when(hs == me)
        def _():
            slots[s - base] = 1

        @pl.when(hd == me)
        def _():
            slots[d - base] = 2
        moved[0, n] = d - base
        moved[1, n] = place
        return n + (hd == me).astype(jnp.int32), even, odd

    zero = jnp.int32(0)
    n_moved, even, odd = lax.fori_loop(0, MIG, entry, (zero, zero, zero), unroll=4)

    def sequence(b, carry):
        n, m = carry
        length = seq_lens[b]
        local, own, place = [], [], []
        for j in range(2):
            slot = new_table[j, b]
            src = source[slot]
            old = jnp.where(src >= 0, src, slot) - base
            mine = (old >= 0) & (old < SLOTS)
            local.append(old)
            own.append(mine)
            place.append(jnp.where(mine, place_of[slot], -1))
        items[0, n] = b
        items[1, n] = jnp.where(own[0], local[0], local[1])
        items[2, n] = jnp.where(own[1], local[1], local[0])
        items[3, n] = jnp.where(own[0], jnp.minimum(length, PAGE), 0)
        items[4, n] = jnp.where(own[1], jnp.maximum(length - PAGE, 0), 0)
        items[5, n] = place[0]
        items[6, n] = place[1]
        for t in range(2):
            pos = length + t
            second = pos >= PAGE
            here = jnp.where(second, new_table[1, b], new_table[0, b]) - base
            rows[0, m] = here
            rows[1, m] = jnp.where(second, pos - PAGE, pos)
            rows[2, m] = (b // 32) * TOK + t * 32 + b % 32
            m = m + ((here >= 0) & (here < SLOTS)).astype(jnp.int32)
        return n + (own[0] | own[1]).astype(jnp.int32), m

    n_items, n_rows = lax.fori_loop(0, SEQS, sequence, (zero, zero), unroll=4)

    @pl.when(n_items > 0)
    def _():
        for i in range(UNROLL - 1):
            for f in range(5):
                items[f, n_items + i] = items[f, n_items - 1]
            for f in range(5, 7):
                items[f, n_items + i] = -1
    meta[0] = n_items
    meta[1] = jnp.where(even == 0, 0, jnp.where(odd == 0, 1, 2))
    meta[2] = n_moved
    meta[3] = n_rows


def run_plan(new_table, seq_lens, mig_src, mig_dst):
    shapes = [(4,), (7, SEQS + UNROLL), (SLOTS,), (2, MIG + 1), (3, 2 * SEQS + 1)]
    return pl.pallas_call(
        plan_kernel,
        name='plan',
        out_shape=[jax.ShapeDtypeStruct(shape, jnp.int32) for shape in shapes],
        in_specs=[SMEM] * 4,
        out_specs=[SMEM] * len(shapes),
        scratch_shapes=[pltpu.SMEM((4 * SLOTS,), jnp.int32), pltpu.SMEM((4 * SLOTS,), jnp.int32), pltpu.SMEM((16,), jnp.int32)],
    )(new_table.T, seq_lens, mig_src, mig_dst)


NBUF = 3
STEPS = SEQS // UNROLL
SLOTS_STEP = SLOTS // STEPS


def attend_kernel(layer, meta, table, slots, q_all, k_pool, v_pool, part_o, part_l, outbox, pool_out, q_rows, kbuf, vbuf, ring, zeros, sems, out_sems, ring_in, ring_out):
    groups = (meta[0] + UNROLL - 1) // UNROLL
    pool = (k_pool, v_pool)[layer]

    def copies(g, start):
        slot = lax.rem(g, NBUF)
        for u in range(UNROLL):
            for j in range(2):
                page = table[1 + j, g * UNROLL + u]
                for ref, buf in ((k_pool, kbuf), (v_pool, vbuf)):
                    copy = pltpu.make_async_copy(ref.at[page, layer], buf.at[slot, u, j], sems.at[slot])
                    copy.start() if start else copy.wait()

    def packs(g, start):
        slot = lax.rem(g, NBUF)
        for u in range(UNROLL):
            for j in range(2):
                place = table[5 + j, g * UNROLL + u]

                @pl.when(place >= 0)
                def _():
                    for p, buf in enumerate((kbuf, vbuf)):
                        copy = pltpu.make_async_copy(buf.at[slot, u, j], outbox.at[place, p], out_sems.at[slot])
                        copy.start() if start else copy.wait()

    def keep(s, phase):
        place = lax.rem(s, NBUF)
        for i in range(SLOTS_STEP):
            slot = s * SLOTS_STEP + i
            state = slots[slot]


            def load():
                return pltpu.make_async_copy(pool.at[slot], ring.at[place, i], ring_in.at[place, i])

            def store():
                return pltpu.make_async_copy(ring.at[place, i], pool_out.at[slot], ring_out.at[place, i])

            if phase == 'load':
                pl.when(state == 0)(lambda: load().start())
            elif phase == 'store':
                @pl.when(state == 0)
                def _():
                    load().wait()
                    store().start()

                @pl.when(state == 1)
                def _():
                    pltpu.make_async_copy(zeros, pool_out.at[slot], ring_out.at[place, i]).start()
            else:
                pl.when(state < 2)(lambda: store().wait())

    for g in range(NBUF - 1):
        @pl.when(g < groups)
        def _():
            copies(g, True)
        keep(g, 'load')
    zeros[...] = jnp.zeros_like(zeros)
    part_o[...] = jnp.zeros_like(part_o)
    part_l[...] = jnp.full_like(part_l, NEG)

    for chip in range(2):
        for tile in range(8):
            for i in range(4):
                rows = q_all[chip, tile, :, i * HEAD:(i + 1) * HEAD].astype(F32)
                q_rows[pl.ds(chip * TOK * HEADS + tile * 4 + i, TOK, stride=HEADS), :] = rows

    row = lax.broadcasted_iota(jnp.int32, (2 * HEADS, 256), 0)
    col = lax.broadcasted_iota(jnp.int32, (2 * HEADS, 256), 1)
    pos = jnp.where((row % HEADS) // 4 == col % KV_HEADS, col // KV_HEADS, PAGE)

    def attend(g):
        slot = lax.rem(g, NBUF)
        outs = []
        for u in range(UNROLL):
            item = g * UNROLL + u
            seq = table[0, item]
            base = (seq // 32) * TOK * HEADS + (seq % 32) * HEADS
            q0 = q_rows[pl.ds(pl.multiple_of(base, HEADS), HEADS), :]
            q1 = q_rows[pl.ds(pl.multiple_of(base + 32 * HEADS, HEADS), HEADS), :]
            q = jnp.concatenate([q0, q1], axis=0).astype(BF16)
            scores = []
            for j in range(2):
                s = lax.dot_general(q, kbuf[slot, u, j], (((1,), (1,)), ((), ())), preferred_element_type=F32)
                scores.append(jnp.where(pos < table[3 + j, item], s, NEG))
            top = jnp.max(jnp.maximum(scores[0], scores[1]), axis=1, keepdims=True)
            probs = [jnp.exp2((s - top) * (SCALE * LOG2E)) for s in scores]
            total = jnp.sum(probs[0] + probs[1], axis=1, keepdims=True)
            out = sum(dot(p.astype(BF16), vbuf[slot, u, j]) for j, p in enumerate(probs))
            live = top > NEG
            lse = jnp.where(live, top * SCALE + jnp.log(total), NEG)
            outs.append((seq, jnp.where(live, out / total, 0.0), jnp.broadcast_to(lse, (2 * HEADS, HEAD))))
        for seq, out, lse in outs:
            for t in range(2):
                for half in range(2):
                    rows = slice(t * HEADS + half * HALF_HEADS, t * HEADS + (half + 1) * HALF_HEADS)
                    part_o[seq // 32, half, t * 32 + seq % 32] = out[rows]
                    part_l[seq // 32, half, t * 32 + seq % 32] = lse[rows]

    def step(g, carry):
        keep(g, 'store')

        @pl.when(g < groups)
        def _():
            copies(g, False)
            packs(g, True)

        @pl.when(g > 0)
        def _():
            keep(g - 1, 'drain')

        @pl.when((g > 0) & (g <= groups))
        def _():
            packs(g - 1, False)

        @pl.when(g + NBUF - 1 < STEPS)
        def _():
            keep(g + NBUF - 1, 'load')

        @pl.when(g + NBUF - 1 < groups)
        def _():
            copies(g + NBUF - 1, True)

        @pl.when(g < groups)
        def _():
            attend(g)
        return carry

    lax.fori_loop(0, STEPS, step, 0)
    keep(STEPS - 1, 'drain')

    @pl.when(groups == STEPS)
    def _():
        packs(groups - 1, False)


def run_attend(layer, meta, table, slots, q_all, k_flat, v_flat):
    shape = jax.ShapeDtypeStruct((2, 2, TOK, HALF_HEADS, HEAD), F32)
    page = (UNROLL, 2, PAGE * KV_HEADS, HEAD)
    return pl.pallas_call(
        functools.partial(attend_kernel, layer),
        name=f'attend{layer}',
        out_shape=[shape, shape, BOX, jax.ShapeDtypeStruct(k_flat.shape, BF16)],
        in_specs=[SMEM, SMEM, SMEM, VMEM, ANY, ANY],
        out_specs=[VMEM, VMEM, ANY, ANY],
        scratch_shapes=[
            pltpu.VMEM((2 * TOK * HEADS, HEAD), F32),
            pltpu.VMEM((NBUF,) + page, BF16),
            pltpu.VMEM((NBUF,) + page, BF16),
            pltpu.VMEM((NBUF, SLOTS_STEP) + k_flat.shape[1:], BF16),
            pltpu.VMEM(k_flat.shape[1:], BF16),
            DMA((NBUF,)),
            DMA((NBUF,)),
            DMA((NBUF, SLOTS_STEP)),
            DMA((NBUF, SLOTS_STEP)),
        ],
        cost_estimate=pl.CostEstimate(flops=2 * 10 ** 10, bytes_accessed=16 * 2 ** 20, transcendentals=0),
        compiler_params=pltpu.CompilerParams(vmem_limit_bytes=VMEM_LIMIT),
    )(meta, table, slots, q_all, k_flat, v_flat)


def merge(parts):
    top = functools.reduce(jnp.maximum, [l for _, l in parts])
    weights = [jnp.exp(l - top) for _, l in parts]
    total = functools.reduce(jnp.add, weights)
    out = functools.reduce(jnp.add, [w * o for w, (o, _) in zip(weights, parts)]) / total
    return out, top + jnp.log(total)


EARLY = 6
MODES = tuple(
    ([((core,), 2, 0, EARLY)], [((core,), 2, EARLY, FAST_PAGES), ((core,), 0, 0, FAST_PAGES)]) for core in range(2)
) + (([], [((0, 1), channel, 0, MIG) for channel in range(3)]),)
CHUNK = 2


class Boxes:
    def __init__(self, moves, outbox, inbox, send_sems, recv_sems):
        me, chip, self.core, partner, across, diag = places()
        self.peers = (partner, across, diag)
        self.moves, self.outbox, self.inbox, self.send_sems, self.recv_sems = moves, outbox, inbox, send_sems, recv_sems

    def each(self, sending, act):
        for cores, channel, first, end in self.moves:
            def run(cores=cores, channel=channel, first=first, end=end):
                def one(i, carry):
                    rows = pl.ds(channel * MIG + i * CHUNK, CHUNK)
                    act(send(self.outbox.at[rows], self.inbox.at[rows], self.send_sems.at[channel, i], self.recv_sems.at[channel, i], self.peers[channel]))
                    return carry

                lax.fori_loop(first // CHUNK, end // CHUNK, one, 0)

            if len(cores) == 2:
                run()
            else:
                cross = 0 if channel == 1 else 1
                at = cores[0] if sending else (cores[0] + cross) % 2
                pl.when(self.core == at)(run)

    def start(self):
        self.each(True, lambda copy: copy.start())

    def wait(self):
        self.each(True, lambda copy: copy.wait_send())
        self.each(False, lambda copy: copy.wait_recv())


def out_kernel(layer, mode, h, q_all, kv, part_o, part_l, wo, outbox, out, inbox, wbuf, wsem, got_o, got_l, mine_o, mine_l, give_o, give_l, far_o, far_l,
               q_rows, k_rows, v_rows, attn, psend, precv, dsend, drecv, xsend, xrecv, ssem, rsem, bsend, brecv):
    boxes = Boxes(MODES[mode][0], outbox, inbox, bsend, brecv)
    me, chip, core, partner, across, diag = places()

    def fetch(j):
        src = wo.at[layer, pl.ds(pl.multiple_of(core * 2048, 2048), 2048), pl.ds(j * TN, TN)]
        return pltpu.make_async_copy(src, wbuf.at[j], wsem.at[j])

    for j in range(8):
        fetch(j).start()
    meet((partner, across, diag))

    near = []
    for which in range(2):
        owner = 1 - chip if which == 0 else chip
        pair = [
            send(part_o.at[owner, 1 - core], got_o.at[which], dsend.at[which, 0], drecv.at[which, 0], partner),
            send(part_l.at[owner, 1 - core], got_l.at[which], dsend.at[which, 1], drecv.at[which, 1], partner),
        ]
        for copy in pair:
            copy.start()
        near.append(pair)

    lane = lax.broadcasted_iota(jnp.int32, (8, HEAD), 1)

    for copy in near[0]:
        copy.wait_recv()

    def chip_merge(i, compact):
        o, l = merge([(part_o[1 - chip, core, i], part_l[1 - chip, core, i]), (got_o[0, i], got_l[0, i])])
        give_o[i] = o
        compact = jnp.where(lane == 2 * i, l[:8], compact)
        return jnp.where(lane == 2 * i + 1, l[8:], compact)

    compact = lax.fori_loop(0, TOK, chip_merge, jnp.zeros((8, HEAD), F32), unroll=8)
    give_l[...] = compact
    far = [
        send(give_l, far_l, xsend.at[0], xrecv.at[0], across),
        send(give_o, far_o, xsend.at[1], xrecv.at[1], across),
    ]
    for copy in far:
        copy.start()

    for head in range(HALF_HEADS):
        tile = core * 4 + head // 4
        rows = pl.ds(head, TOK, stride=HALF_HEADS)
        q_rows[rows, :] = q_all[chip, tile, :, (head % 4) * HEAD:(head % 4 + 1) * HEAD].astype(F32)
        k_rows[rows, :] = kv[:, (head // 4) * HEAD:(head // 4 + 1) * HEAD].astype(F32)
        v_rows[rows, :] = kv[:, TN + (head // 4) * HEAD:TN + (head // 4 + 1) * HEAD].astype(F32)
    for copy in near[1]:
        copy.wait_recv()

    half = ROWS // 2

    def score(q, k):
        s = jnp.sum(q * k, axis=1, keepdims=True) * SCALE
        return jnp.broadcast_to(s, q.shape)

    def own(i, carry):
        a = pl.ds(pl.multiple_of(i * HALF_HEADS, HALF_HEADS), HALF_HEADS)
        b = pl.ds(pl.multiple_of(half + i * HALF_HEADS, HALF_HEADS), HALF_HEADS)
        k0, v0, k1, v1 = k_rows[a, :], v_rows[a, :], k_rows[b, :], v_rows[b, :]
        q0, q1 = q_rows[a, :], q_rows[b, :]
        j = i + TOK // 2
        o, l = merge([(part_o[chip, core, i], part_l[chip, core, i]), (got_o[1, i], got_l[1, i]), (v0, score(q0, k0))])
        mine_o[i] = o
        mine_l[i] = l
        o, l = merge([(part_o[chip, core, j], part_l[chip, core, j]), (got_o[1, j], got_l[1, j]), (v0, score(q1, k0)), (v1, score(q1, k1))])
        mine_o[j] = o
        mine_l[j] = l
        return carry

    lax.fori_loop(0, TOK // 2, own, 0, unroll=4)

    for copy in far:
        copy.wait_recv()
    boxes.start()
    spread = far_l[...]

    def last_merge(i, carry):
        l = jnp.concatenate([
            jnp.broadcast_to(jnp.sum(jnp.where(lane == 2 * i + k, spread, 0.0), axis=1, keepdims=True), (8, HEAD)) for k in range(2)
        ], axis=0)
        o, _ = merge([(mine_o[i], mine_l[i]), (far_o[i], l)])
        q_rows[pl.ds(pl.multiple_of(i * HALF_HEADS, HALF_HEADS), HALF_HEADS), :] = o
        return carry

    lax.fori_loop(0, TOK, last_merge, 0, unroll=8)
    for head in range(HALF_HEADS):
        attn[:, head * HEAD:(head + 1) * HEAD] = q_rows[pl.ds(head, TOK, stride=HALF_HEADS), :].astype(BF16)

    def reduce(j):
        return send(psend.at[j], precv.at[j], ssem.at[j], rsem.at[j], partner)

    def project(j, carry):
        pltpu.make_async_copy(wo.at[layer, pl.ds(0, 2048), pl.ds(0, TN)], wbuf.at[j], wsem.at[j]).wait()
        psend[j] = dot(attn[...], wbuf[j])

        @pl.when(j > 0)
        def _():
            reduce(j - 1).start()
        return carry

    lax.fori_loop(0, 8, project, 0)
    reduce(7).start()
    for j in range(8):
        reduce(j).wait_recv()
        cols = slice(j * TN, (j + 1) * TN)
        out[:, cols] = (h[:, cols].astype(F32) + (psend[j] + precv[j])).astype(BF16)
    for j in range(8):
        reduce(j).wait_send()
    for pair in near:
        for copy in pair:
            copy.wait_send()
    for copy in far:
        copy.wait_send()
    boxes.wait()


def run_out(layer, mode, h, q_all, kv, part_o, part_l, w_out, outbox):
    token = (TOK, HALF_HEADS, HEAD)
    return pl.pallas_call(
        functools.partial(out_kernel, layer, mode),
        name=f'out{layer}_{mode}',
        out_shape=[jax.ShapeDtypeStruct((TOK, D), BF16), BOX],
        in_specs=[VMEM] * 5 + [ANY, ANY],
        out_specs=[VMEM, ANY],
        scratch_shapes=[
            pltpu.VMEM((8, 2048, TN), BF16),
            DMA((8,)),
            pltpu.VMEM((2,) + token, F32),
            pltpu.VMEM((2,) + token, F32),
            pltpu.VMEM(token, F32),
            pltpu.VMEM(token, F32),
            pltpu.VMEM(token, F32),
            pltpu.VMEM((8, HEAD), F32),
            pltpu.VMEM(token, F32),
            pltpu.VMEM((8, HEAD), F32),
            pltpu.VMEM((ROWS, HEAD), F32),
            pltpu.VMEM((ROWS, HEAD), F32),
            pltpu.VMEM((ROWS, HEAD), F32),
            pltpu.VMEM((TOK, 2048), BF16),
            pltpu.VMEM((8, TOK, TN), F32),
            pltpu.VMEM((8, TOK, TN), F32),
            DMA((2, 2)),
            DMA((2, 2)),
            DMA((2,)),
            DMA((2,)),
            DMA((8,)),
            DMA((8,)),
            DMA((3, MIG // CHUNK)),
            DMA((3, MIG // CHUNK)),
        ],
        cost_estimate=pl.CostEstimate(flops=10 ** 11, bytes_accessed=20 * 2 ** 20, transcendentals=0),
        compiler_params=pltpu.CompilerParams(collective_id=2 + layer * 3 + mode, has_side_effects=True, vmem_limit_bytes=VMEM_LIMIT),
    )(h, q_all, kv, part_o, part_l, w_out, outbox)


NU = 4
ND = 4
UP_TILES = FF // 2 // TN
KROWS = FF // 4
DOWN_TILES = 2 * (D // TN)


def mlp_kernel(layer, mode, h, kv, w_up, w_down, outbox, inbox_in, out, kv_all, inbox, ubuf, dbuf, act, psend, precv, usem, dsem, ssem, rsem, ksend, krecv, bsend, brecv):
    me, chip, core, partner, across, diag = places()
    boxes = Boxes(MODES[mode][1], outbox, inbox, bsend, brecv)

    def fetch_up(s):
        src = w_up.at[layer, :, pl.ds(pl.multiple_of(core * (FF // 2) + s * TN, TN), TN)]
        slot = lax.rem(s, NU)
        return pltpu.make_async_copy(src, ubuf.at[slot], usem.at[slot])

    def fetch_down(s):
        src = w_down.at[layer, pl.ds(pl.multiple_of(core * (FF // 2) + lax.rem(s, 2) * KROWS, KROWS), KROWS), pl.ds(pl.multiple_of((s // 2) * TN, TN), TN)]
        slot = lax.rem(s, ND)
        return pltpu.make_async_copy(src, dbuf.at[slot], dsem.at[slot])

    for s in range(NU):
        fetch_up(jnp.int32(s)).start()
    meet((partner, across, diag))
    kv_all[me] = kv[...]
    rows = [send(kv, kv_all.at[me], ksend.at[i], krecv.at[i], peer) for i, peer in enumerate((partner, across))]
    rows.append(send(kv_all.at[across], kv_all.at[across], ksend.at[2], krecv.at[2], partner))
    for copy in rows[:2]:
        copy.start()
    boxes.start()

    def up(s, carry):
        fetch_up(s).wait()
        u = dot(h[...], ubuf[lax.rem(s, NU)]).astype(BF16)
        a = jax.nn.gelu(u.astype(F32), approximate=True).astype(BF16)
        act[s // 7, :, pl.ds(pl.multiple_of(lax.rem(s, 7) * TN, TN), TN)] = a

        @pl.when(s + NU < UP_TILES)
        def _():
            fetch_up(s + NU).start()

        @pl.when(s + NU >= UP_TILES)
        def _():
            fetch_down(s + NU - UP_TILES).start()
        return carry

    lax.fori_loop(0, UP_TILES, up, 0)
    rows[1].wait_recv()
    rows[2].start()

    def reduce(j):
        return send(psend.at[j], precv.at[j], ssem.at[j], rsem.at[j], partner)

    def down(j, carry):
        total = None
        for k in range(2):
            s = 2 * j + k
            fetch_down(s).wait()
            part = dot(act[k], dbuf[lax.rem(s, ND)])
            total = part if total is None else total + part

            @pl.when(s + ND < DOWN_TILES)
            def _():
                fetch_down(s + ND).start()
        psend[j] = total

        @pl.when(j > 0)
        def _():
            reduce(j - 1).start()
        return carry

    lax.fori_loop(0, 8, down, 0)
    reduce(7).start()
    for j in range(8):
        reduce(j).wait_recv()
        cols = slice(j * TN, (j + 1) * TN)
        out[:, cols] = (h[:, cols].astype(F32) + (psend[j] + precv[j])).astype(BF16)
    for j in range(8):
        reduce(j).wait_send()
    rows[0].wait()
    rows[1].wait_send()
    rows[2].wait()
    boxes.wait()


def run_mlp(layer, mode, h, kv, w_up, w_down, outbox, inbox):
    return pl.pallas_call(
        functools.partial(mlp_kernel, layer, mode),
        name=f'mlp{layer}_{mode}',
        out_shape=[jax.ShapeDtypeStruct((TOK, D), BF16), jax.ShapeDtypeStruct((4, TOK, 2 * TN), BF16), BOX],
        in_specs=[VMEM, VMEM, ANY, ANY, ANY, ANY],
        out_specs=[VMEM, VMEM, ANY],
        input_output_aliases={5: 2},
        scratch_shapes=[
            pltpu.VMEM((NU, D, TN), BF16),
            pltpu.VMEM((ND, KROWS, TN), BF16),
            pltpu.VMEM((2, TOK, KROWS), BF16),
            pltpu.VMEM((8, TOK, TN), F32),
            pltpu.VMEM((8, TOK, TN), F32),
            DMA((NU,)),
            DMA((ND,)),
            DMA((8,)),
            DMA((8,)),
            DMA((3,)),
            DMA((3,)),
            DMA((3, MIG // CHUNK)),
            DMA((3, MIG // CHUNK)),
        ],
        cost_estimate=pl.CostEstimate(flops=2 * TOK * D * FF * 8, bytes_accessed=D * FF * 2, transcendentals=0),
        compiler_params=pltpu.CompilerParams(collective_id=8 + layer * 3 + mode, has_side_effects=True, vmem_limit_bytes=VMEM_LIMIT),
    )(h, kv, w_up, w_down, outbox, inbox)


RING = 16
AHEAD = RING // 2


def finish_kernel(meta, moved, rows, inbox0, inbox1, k_rows, v_rows, k_in, v_in, k_out, v_out, buf, in_sem, out_sem, row_sem):
    del k_in, v_in
    inboxes = (inbox0, inbox1)
    outs = (k_out, v_out)
    count = meta[2]

    def load(i):
        slot = lax.rem(i, RING)
        return [pltpu.make_async_copy(inboxes[l].at[moved[1, i], p], buf.at[slot, p, l], in_sem.at[slot, p, l]) for p in range(2) for l in range(LAYERS)]

    def store(i):
        slot = lax.rem(i, RING)
        return [pltpu.make_async_copy(buf.at[slot, p], outs[p].at[moved[0, i]], out_sem.at[slot, p]) for p in range(2)]

    def begin(group):
        for copy in group:
            copy.start()

    def end(group):
        for copy in group:
            copy.wait()

    def loop(first, last, body):
        lax.fori_loop(first, last, lambda i, carry: (body(i), carry)[1], 0)

    loop(0, jnp.minimum(count, AHEAD), lambda i: begin(load(i)))

    def page(i):
        end(load(i))
        begin(store(i))

        @pl.when(i + AHEAD < count)
        def _():
            @pl.when(i >= AHEAD)
            def _():
                end(store(i - AHEAD))
            begin(load(i + AHEAD))

    loop(0, count, page)
    loop(jnp.maximum(count - RING, 0), count, lambda i: end(store(i)))

    def row(i):
        at = pl.ds(pl.multiple_of(rows[1, i] * KV_HEADS, KV_HEADS), KV_HEADS)
        return [pltpu.make_async_copy(src.at[l, rows[2, i]], outs[p].at[rows[0, i], l, at, :], row_sem.at[p, l]) for p, src in enumerate((k_rows, v_rows)) for l in range(LAYERS)]

    loop(0, meta[3], lambda i: begin(row(i)))
    loop(0, meta[3], lambda i: end(row(i)))


def run_finish(meta, moved, rows, inboxes, k_rows, v_rows, k_part, v_part):
    shape = jax.ShapeDtypeStruct(k_part.shape, BF16)
    return pl.pallas_call(
        finish_kernel,
        name='finish',
        out_shape=[shape, shape],
        in_specs=[SMEM, SMEM, SMEM, ANY, ANY, VMEM, VMEM, ANY, ANY],
        out_specs=[ANY, ANY],
        scratch_shapes=[
            pltpu.VMEM((RING, 2) + k_part.shape[1:], BF16),
            DMA((RING, 2, LAYERS)),
            DMA((RING, 2)),
            DMA((2, LAYERS)),
        ],
        input_output_aliases={7: 0, 8: 1},
        cost_estimate=pl.CostEstimate(flops=10 ** 10, bytes_accessed=16 * 2 ** 20, transcendentals=0),
        compiler_params=pltpu.CompilerParams(vmem_limit_bytes=VMEM_LIMIT),
    )(meta, moved, rows, *inboxes, k_rows, v_rows, k_part, v_part)


def by_token(kv_all):
    x = kv_all.reshape(2, 2, TOK, 2, 4, HEAD)
    return x.transpose(3, 0, 2, 1, 4, 5).reshape(2, 2 * TOK, KV_HEADS, HEAD)


def solution(mesh):
    pool_spec = P(('rep', 'kv'))
    tok_spec = P(None, ('rep', 'kv'), None)

    def device_fn(embeds, w_query, w_key, w_value, w_out, w_up, w_down, k_pool, v_pool, new_table, seq_lens, mig_src, mig_dst):
        me = lax.axis_index('kv')
        weights = (w_query, w_key, w_value)
        k_flat, v_flat = flat_pool(k_pool), flat_pool(v_pool)
        meta, items, slots, moved, where = run_plan(new_table, seq_lens, mig_src, mig_dst)
        rows, inboxes, pools = [], [], []
        h = None
        for layer in range(LAYERS):
            if layer == 0:
                q_all, kv, h = run_qkv(layer, embeds, weights, True)
            else:
                q_all, kv = run_qkv(layer, h, weights, False)
            part_o, part_l, outbox, pool = run_attend(layer, meta, items, slots, q_all, k_flat, v_flat)

            def rest(mode, h, q_all, kv, part_o, part_l, outbox, w_out, w_up, w_down, layer=layer):
                h, inbox = run_out(layer, mode, h, q_all, kv, part_o, part_l, w_out, outbox)
                return run_mlp(layer, mode, h, kv, w_up, w_down, outbox, inbox)

            forms = [functools.partial(rest, mode) for mode in range(len(MODES))]
            h, kv_all, inbox = lax.switch(meta[1], forms, h, q_all, kv, part_o, part_l, outbox, w_out, w_up, w_down)
            inboxes.append(inbox)
            rows.append(by_token(kv_all))
            pools.append(pool)
        rows = jnp.stack(rows)
        k_out, v_out = run_finish(meta, moved, where, inboxes, rows[:, 0], rows[:, 1], *pools)
        k_out, v_out = k_out.reshape(k_pool.shape), v_out.reshape(v_pool.shape)
        y = lax.dynamic_slice_in_dim(h.reshape(2, 32, D), (me % 2) * 16, 16, axis=1)
        return y, k_out, v_out

    return jax.shard_map(device_fn, mesh=mesh, in_specs=(tok_spec, P(), P(), P(), P(), P(), P(), pool_spec, pool_spec, P('rep', None), P('rep'), P('rep'), P('rep')), out_specs=(tok_spec, pool_spec, pool_spec), check_vma=False)
```

```python
import functools

import jax
import jax.numpy as jnp
from jax import lax
from jax.experimental import pallas as pl
from jax.experimental.pallas import tpu as pltpu
from jax.sharding import PartitionSpec as P

BF16 = jnp.bfloat16
F32 = jnp.float32
MESH = pl.DeviceIdType.MESH
NEG = -3.0e38
VMEM_LIMIT = 60 * 1024 * 1024

D = 4096
HEADS = 32
KV_HEADS = 8
HEAD = 128
FF = 14336
PAGE = 32
LAYERS = 2
SEQS = 64
MIG = 64
TOK = 64
HALF_HEADS = HEADS // 2
ROWS = TOK * HALF_HEADS
TN = 512
SCALE = HEAD ** -0.5
LOG2E = 1.4426950408889634
SLOTS = 96
UNROLL = 4
FAST_PAGES = 32
BOX = jax.ShapeDtypeStruct((3 * MIG, 2, PAGE * KV_HEADS, HEAD), BF16)


def flat_pool(pool):
    return pool.reshape(pool.shape[0], LAYERS, PAGE * KV_HEADS, HEAD)


def dot(a, b):
    return jnp.dot(a, b, preferred_element_type=F32)


def places():
    me = lax.axis_index('kv')
    core = lax.rem(me, 2)
    chip = me // 2
    partner = me + 1 - 2 * core
    across = lax.rem(me + 2, 4)
    diag = lax.rem(partner + 2, 4)
    return me, chip, core, partner, across, diag


def meet(peers):
    barrier = pltpu.get_barrier_semaphore()
    for peer in peers:
        pl.semaphore_signal(barrier, inc=1, device_id={'kv': peer}, device_id_type=MESH)
    pl.semaphore_wait(barrier, len(peers))


def send(src, dst, send_sem, recv_sem, peer):
    return pltpu.make_async_remote_copy(src_ref=src, dst_ref=dst, send_sem=send_sem, recv_sem=recv_sem, device_id={'kv': peer}, device_id_type=MESH)


VMEM = pl.BlockSpec(memory_space=pltpu.VMEM)
SMEM = pl.BlockSpec(memory_space=pltpu.SMEM)
ANY = pl.BlockSpec(memory_space=pl.ANY)
DMA = pltpu.SemaphoreType.DMA


WINDOW = 3


def qkv_kernel(layer, first, *refs):
    if first:
        emb, wq, wk, wv, q_all, kv, h, wbuf, wsem, psend, precv, xsend, xrecv, fsend, frecv, hsend, hrecv = refs
    else:
        h, wq, wk, wv, q_all, kv, wbuf, wsem, psend, precv, xsend, xrecv, fsend, frecv = refs
    me, chip, core, partner, across, diag = places()

    def fetch(j):
        if j < 4:
            src = wq.at[layer, :, pl.ds(pl.multiple_of(core * 2048 + j * TN, TN), TN)]
        else:
            src = (wk, wv)[j - 4].at[layer, :, pl.ds(pl.multiple_of(core * TN, TN), TN)]
        return pltpu.make_async_copy(src, wbuf.at[j], wsem.at[j])

    for j in range(WINDOW):
        fetch(j).start()
    meet((partner, across))
    if first:
        copies = []
        for t in range(2):
            rows = pl.ds(pl.multiple_of(t * 32 + core * 16, 16), 16)
            h[rows, :] = emb[t]
            copies.append(send(emb.at[t], h.at[rows, :], hsend.at[t], hrecv.at[t], partner))
        for copy in copies:
            copy.start()
        for copy in copies:
            copy.wait()

    def to_partner(j):
        ref = q_all.at[chip, core * 4 + j]
        return send(ref, ref, psend.at[j], precv.at[j], partner)

    def to_across(j):
        ref = q_all.at[chip, core * 4 + j]
        return send(ref, ref, xsend.at[j], xrecv.at[j], across)

    def forward(j):
        ref = q_all.at[1 - chip, core * 4 + j]
        return send(ref, ref, fsend.at[j], frecv.at[j], partner)

    def tile(j, carry):
        pltpu.make_async_copy(wq.at[layer, :, pl.ds(0, TN)], wbuf.at[j], wsem.at[j]).wait()
        q_all[chip, core * 4 + j] = dot(h[...], wbuf[j]).astype(BF16)
        for i in range(4):
            if i + WINDOW < 6:
                pl.when(j == i)(lambda i=i: fetch(i + WINDOW).start())

        @pl.when(j > 0)
        def _():
            to_across(j - 1).start()
            to_partner(j - 1).start()
        return carry

    lax.fori_loop(0, 4, tile, 0)
    for j in range(4, 6):
        fetch(j).wait()
        kv[:, (j - 4) * TN:(j - 3) * TN] = dot(h[...], wbuf[j]).astype(BF16)
        if j == 4:
            to_across(3).start()
            to_partner(3).start()
    for j in range(4):
        to_across(j).wait_recv()
        forward(j).start()
    for j in range(4):
        to_across(j).wait_send()
        to_partner(j).wait()
        forward(j).wait()


def run_qkv(layer, h, weights, first):
    wq, wk, wv = weights[:3]
    out_shape = [jax.ShapeDtypeStruct((2, 8, TOK, TN), BF16), jax.ShapeDtypeStruct((TOK, 2 * TN), BF16)]
    if first:
        out_shape.append(jax.ShapeDtypeStruct((TOK, D), BF16))
    scratch = [pltpu.VMEM((6, D, TN), BF16), DMA((6,))] + [DMA((4,))] * 6
    if first:
        scratch += [DMA((2,))] * 2
    return pl.pallas_call(
        functools.partial(qkv_kernel, layer, first),
        name=f'qkv{layer}',
        out_shape=out_shape,
        in_specs=[VMEM, ANY, ANY, ANY],
        out_specs=[VMEM] * len(out_shape),
        scratch_shapes=scratch,
        cost_estimate=pl.CostEstimate(flops=2 * TOK * D * 6 * TN * 8, bytes_accessed=D * 6 * TN * 2, transcendentals=0),
        compiler_params=pltpu.CompilerParams(collective_id=layer, has_side_effects=True, vmem_limit_bytes=VMEM_LIMIT),
    )(h, wq, wk, wv)


def plan_kernel(new_table, seq_lens, mig_src, mig_dst, meta, items, slots, moved, rows, source, place_of, counts):
    me = lax.axis_index('kv')
    base = me * SLOTS

    def home(slot):
        return sum((slot >= i * SLOTS).astype(jnp.int32) for i in range(1, 4))

    def clear(i, carry):
        source[i] = -1
        place_of[i] = -1
        return carry

    lax.fori_loop(0, 4 * SLOTS, clear, 0, unroll=16)
    for i in range(16):
        counts[i] = 0

    def keep(i, carry):
        slots[i] = 0
        return carry

    lax.fori_loop(0, SLOTS, keep, 0, unroll=16)

    def entry(e, carry):
        n, even, odd = carry
        s, d = mig_src[e], mig_dst[e]
        hs, hd = home(s), home(d)
        pair = hs * 4 + hd
        rank = counts[pair]
        counts[pair] = rank + 1
        channel = (hs ^ hd) - 1
        place = channel * MIG + rank
        source[d] = s
        place_of[d] = place
        misfit = ((channel == 1) | (rank >= FAST_PAGES)).astype(jnp.int32)
        even = even | misfit | (hs & 1)
        odd = odd | misfit | (1 - (hs & 1))

        slots[jnp.where(hs == me, s - base, SLOTS)] = 1
        slots[jnp.where(hd == me, d - base, SLOTS)] = 2
        moved[0, n] = d - base
        moved[1, n] = place
        return n + (hd == me).astype(jnp.int32), even, odd

    zero = jnp.int32(0)
    n_moved, even, odd = lax.fori_loop(0, MIG, entry, (zero, zero, zero), unroll=4)

    def sequence(b, carry):
        n, m = carry
        length = seq_lens[b]
        local, own, place = [], [], []
        for j in range(2):
            slot = new_table[j, b]
            src = source[slot]
            old = jnp.where(src >= 0, src, slot) - base
            mine = (old >= 0) & (old < SLOTS)
            local.append(old)
            own.append(mine)
            place.append(jnp.where(mine, place_of[slot], -1))
        items[0, n] = b
        items[1, n] = jnp.where(own[0], local[0], local[1])
        items[2, n] = jnp.where(own[1], local[1], local[0])
        items[3, n] = jnp.where(own[0], jnp.minimum(length, PAGE), 0)
        items[4, n] = jnp.where(own[1], jnp.maximum(length - PAGE, 0), 0)
        items[5, n] = place[0]
        items[6, n] = place[1]
        for t in range(2):
            pos = length + t
            second = pos >= PAGE
            here = jnp.where(second, new_table[1, b], new_table[0, b]) - base
            rows[0, m] = here
            rows[1, m] = jnp.where(second, pos - PAGE, pos)
            rows[2, m] = (b // 32) * TOK + t * 32 + b % 32
            m = m + ((here >= 0) & (here < SLOTS)).astype(jnp.int32)
        return n + (own[0] | own[1]).astype(jnp.int32), m

    n_items, n_rows = lax.fori_loop(0, SEQS, sequence, (zero, zero), unroll=4)

    @pl.when(n_items > 0)
    def _():
        for i in range(UNROLL - 1):
            for f in range(5):
                items[f, n_items + i] = items[f, n_items - 1]
            for f in range(5, 7):
                items[f, n_items + i] = -1
    meta[0] = n_items
    meta[1] = jnp.where(even == 0, 0, jnp.where(odd == 0, 1, 2))
    meta[2] = n_moved
    meta[3] = n_rows


def run_plan(new_table, seq_lens, mig_src, mig_dst):
    shapes = [(4,), (7, SEQS + UNROLL), (SLOTS + 1,), (2, MIG + 1), (3, 2 * SEQS + 1)]
    return pl.pallas_call(
        plan_kernel,
        name='plan',
        out_shape=[jax.ShapeDtypeStruct(shape, jnp.int32) for shape in shapes],
        in_specs=[SMEM] * 4,
        out_specs=[SMEM] * len(shapes),
        scratch_shapes=[pltpu.SMEM((4 * SLOTS,), jnp.int32), pltpu.SMEM((4 * SLOTS,), jnp.int32), pltpu.SMEM((16,), jnp.int32)],
    )(new_table.T, seq_lens, mig_src, mig_dst)


NBUF = 3
STEPS = SEQS // UNROLL
SLOTS_STEP = SLOTS // STEPS


def attend_kernel(layer, meta, table, slots, q_all, k_pool, v_pool, *refs):
    if layer == 0:
        part_o, part_l, outbox, pool_out, q_rows, kbuf, vbuf, ring, zeros, sems, out_sems, ring_in, ring_out = refs
    else:
        moved, inbox, _, part_o, part_l, outbox, pool_out, k_out, q_rows, kbuf, vbuf, ring, zeros, sems, out_sems, ring_in, ring_out, pages, page_in, page_out = refs
    groups = (meta[0] + UNROLL - 1) // UNROLL
    pool = (k_pool, v_pool)[layer]

    def copies(g, start):
        slot = lax.rem(g, NBUF)
        for u in range(UNROLL):
            for j in range(2):
                page = table[1 + j, g * UNROLL + u]
                for ref, buf in ((k_pool, kbuf), (v_pool, vbuf)):
                    copy = pltpu.make_async_copy(ref.at[page, layer], buf.at[slot, u, j], sems.at[slot])
                    copy.start() if start else copy.wait()

    def packs(g, start):
        slot = lax.rem(g, NBUF)
        for u in range(UNROLL):
            for j in range(2):
                place = table[5 + j, g * UNROLL + u]

                @pl.when(place >= 0)
                def _():
                    for p, buf in enumerate((kbuf, vbuf)):
                        copy = pltpu.make_async_copy(buf.at[slot, u, j], outbox.at[place, p], out_sems.at[slot])
                        copy.start() if start else copy.wait()

    def keep(s, phase):
        place = lax.rem(s, NBUF)
        for i in range(SLOTS_STEP):
            slot = s * SLOTS_STEP + i
            state = slots[slot]


            def load():
                return pltpu.make_async_copy(pool.at[slot], ring.at[place, i], ring_in.at[place, i])

            def store():
                return pltpu.make_async_copy(ring.at[place, i], pool_out.at[slot], ring_out.at[place, i])

            if phase == 'load':
                pl.when(state == 0)(lambda: load().start())
            elif phase == 'store':
                @pl.when(state == 0)
                def _():
                    load().wait()
                    store().start()

                @pl.when(state == 1)
                def _():
                    pltpu.make_async_copy(zeros, pool_out.at[slot], ring_out.at[place, i]).start()
            else:
                pl.when(state < 2)(lambda: store().wait())

    def settle(phase):
        def one(i, carry):
            for p, dst in enumerate((k_out, pool_out)):
                if phase < 2:
                    copy = pltpu.make_async_copy(inbox.at[moved[1, i], p], pages.at[i, p], page_in)
                else:
                    copy = pltpu.make_async_copy(pages.at[i, p], dst.at[moved[0, i], 0], page_out)
                copy.wait() if phase % 2 else copy.start()
            return carry

        lax.fori_loop(0, meta[2], one, 0)

    for g in range(NBUF - 1):
        @pl.when(g < groups)
        def _():
            copies(g, True)
        keep(g, 'load')
    if layer == 1:
        settle(0)
    zeros[...] = jnp.zeros_like(zeros)
    part_o[...] = jnp.zeros_like(part_o)
    part_l[...] = jnp.full_like(part_l, NEG)

    for chip in range(2):
        for tile in range(8):
            for i in range(4):
                rows = q_all[chip, tile, :, i * HEAD:(i + 1) * HEAD].astype(F32)
                q_rows[pl.ds(chip * TOK * HEADS + tile * 4 + i, TOK, stride=HEADS), :] = rows

    row = lax.broadcasted_iota(jnp.int32, (2 * HEADS, 256), 0)
    col = lax.broadcasted_iota(jnp.int32, (2 * HEADS, 256), 1)
    pos = jnp.where((row % HEADS) // 4 == col % KV_HEADS, col // KV_HEADS, PAGE)

    def attend(g):
        slot = lax.rem(g, NBUF)
        outs = []
        for u in range(UNROLL):
            item = g * UNROLL + u
            seq = table[0, item]
            base = (seq // 32) * TOK * HEADS + (seq % 32) * HEADS
            q0 = q_rows[pl.ds(pl.multiple_of(base, HEADS), HEADS), :]
            q1 = q_rows[pl.ds(pl.multiple_of(base + 32 * HEADS, HEADS), HEADS), :]
            q = jnp.concatenate([q0, q1], axis=0).astype(BF16)
            scores = []
            for j in range(2):
                s = lax.dot_general(q, kbuf[slot, u, j], (((1,), (1,)), ((), ())), preferred_element_type=F32)
                scores.append(jnp.where(pos < table[3 + j, item], s, NEG))
            top = jnp.max(jnp.maximum(scores[0], scores[1]), axis=1, keepdims=True)
            probs = [jnp.exp2((s - top) * (SCALE * LOG2E)) for s in scores]
            total = jnp.sum(probs[0] + probs[1], axis=1, keepdims=True)
            out = sum(dot(p.astype(BF16), vbuf[slot, u, j]) for j, p in enumerate(probs))
            live = top > NEG
            lse = jnp.where(live, top * SCALE + jnp.log(total), NEG)
            outs.append((seq, jnp.where(live, out / total, 0.0), jnp.broadcast_to(lse, (2 * HEADS, HEAD))))
        for seq, out, lse in outs:
            for t in range(2):
                for half in range(2):
                    rows = slice(t * HEADS + half * HALF_HEADS, t * HEADS + (half + 1) * HALF_HEADS)
                    part_o[seq // 32, half, t * 32 + seq % 32] = out[rows]
                    part_l[seq // 32, half, t * 32 + seq % 32] = lse[rows]

    def step(g, carry):
        keep(g, 'store')
        if layer == 1:
            @pl.when(g == STEPS // 2)
            def _():
                settle(1)
                settle(2)

        @pl.when(g < groups)
        def _():
            copies(g, False)
            packs(g, True)

        @pl.when(g > 0)
        def _():
            keep(g - 1, 'drain')

        @pl.when((g > 0) & (g <= groups))
        def _():
            packs(g - 1, False)

        @pl.when(g + NBUF - 1 < STEPS)
        def _():
            keep(g + NBUF - 1, 'load')

        @pl.when(g + NBUF - 1 < groups)
        def _():
            copies(g + NBUF - 1, True)

        @pl.when(g < groups)
        def _():
            attend(g)
        return carry

    lax.fori_loop(0, STEPS, step, 0)
    keep(STEPS - 1, 'drain')
    if layer == 1:
        settle(3)

    @pl.when(groups == STEPS)
    def _():
        packs(groups - 1, False)


def run_attend(layer, meta, table, slots, q_all, k_flat, v_flat, extra=()):
    shape = jax.ShapeDtypeStruct((2, 2, TOK, HALF_HEADS, HEAD), F32)
    page = (UNROLL, 2, PAGE * KV_HEADS, HEAD)
    return pl.pallas_call(
        functools.partial(attend_kernel, layer),
        name=f'attend{layer}',
        out_shape=[shape, shape, BOX] + [jax.ShapeDtypeStruct(k_flat.shape, BF16)] * (layer + 1),
        in_specs=[SMEM, SMEM, SMEM, VMEM, ANY, ANY] + [SMEM, ANY, ANY] * layer,
        out_specs=[VMEM, VMEM, ANY, ANY] + [ANY] * layer,
        input_output_aliases={8: 4} if layer else {},
        scratch_shapes=[
            pltpu.VMEM((2 * TOK * HEADS, HEAD), F32),
            pltpu.VMEM((NBUF,) + page, BF16),
            pltpu.VMEM((NBUF,) + page, BF16),
            pltpu.VMEM((NBUF, SLOTS_STEP) + k_flat.shape[1:], BF16),
            pltpu.VMEM(k_flat.shape[1:], BF16),
            DMA((NBUF,)),
            DMA((NBUF,)),
            DMA((NBUF, SLOTS_STEP)),
            DMA((NBUF, SLOTS_STEP)),
        ] + [pltpu.VMEM((MIG, 2, PAGE * KV_HEADS, HEAD), BF16), DMA, DMA] * layer,
        cost_estimate=pl.CostEstimate(flops=2 * 10 ** 10, bytes_accessed=16 * 2 ** 20, transcendentals=0),
        compiler_params=pltpu.CompilerParams(vmem_limit_bytes=VMEM_LIMIT),
    )(meta, table, slots, q_all, k_flat, v_flat, *extra)


def merge(parts):
    top = functools.reduce(jnp.maximum, [l for _, l in parts])
    weights = [jnp.exp(l - top) for _, l in parts]
    total = functools.reduce(jnp.add, weights)
    out = functools.reduce(jnp.add, [w * o for w, (o, _) in zip(weights, parts)]) / total
    return out, top + jnp.log(total)


MODES = ([((0,), 2, FAST_PAGES), ((0,), 0, FAST_PAGES)], [((1,), 2, FAST_PAGES), ((1,), 0, FAST_PAGES)], [((0, 1), i, MIG) for i in range(3)])
CHUNK = 2


class Boxes:
    def __init__(self, moves, outbox, inbox, send_sems, recv_sems):
        me, chip, self.core, partner, across, diag = places()
        self.peers = (partner, across, diag)
        self.moves, self.outbox, self.inbox, self.send_sems, self.recv_sems = moves, outbox, inbox, send_sems, recv_sems

    def each(self, sending, act):
        for cores, channel, pages in self.moves:
            def run(channel=channel, pages=pages):
                def one(i, carry):
                    rows = pl.ds(channel * MIG + i * CHUNK, CHUNK)
                    act(send(self.outbox.at[rows], self.inbox.at[rows], self.send_sems.at[channel, i], self.recv_sems.at[channel, i], self.peers[channel]))
                    return carry

                lax.fori_loop(0, pages // CHUNK, one, 0)

            if len(cores) == 2:
                run()
            else:
                cross = 0 if channel == 1 else 1
                at = cores[0] if sending else (cores[0] + cross) % 2
                pl.when(self.core == at)(run)

    def start(self):
        self.each(True, lambda copy: copy.start())

    def wait(self):
        self.each(True, lambda copy: copy.wait_send())
        self.each(False, lambda copy: copy.wait_recv())


RING_W = 20
TK = 2048
UP_TILES = FF // 2 // TN
TD = FF // 8
OUT_END = D // TN
UP_END = OUT_END + 2 * UP_TILES
ALL_TILES = UP_END + 4 * (D // TN)
PART = TOK // 2


def rest_kernel(layer, mode, h_in, q_all, kv, part_o, part_l, wo, w_up, w_down, outbox, out, kv_all, inbox, ring, ring_sem, own_o, own_l, own_sem,
                got_o, got_l, mine_o, mine_l, give_o, give_l, far_o, far_l, q_rows, k_rows, v_rows, attn, act, h, psend, precv,
                dsend, drecv, xsend, xrecv, ssem, rsem, ksend, krecv, bsend, brecv):
    me, chip, core, partner, across, diag = places()
    boxes = Boxes(MODES[mode], outbox, inbox, bsend, brecv)

    def tile_copy(t, kind):
        slot = lax.rem(t, RING_W)
        if kind == 0:
            src = wo.at[layer, pl.ds(pl.multiple_of(core * TK, TK), TK), pl.ds(pl.multiple_of(t * TN, TN), TN)]
        elif kind == 1:
            i = t - OUT_END
            src = w_up.at[layer, pl.ds(pl.multiple_of(lax.rem(i, 2) * TK, TK), TK), pl.ds(pl.multiple_of(core * (FF // 2) + (i // 2) * TN, TN), TN)]
        else:
            i = t - UP_END
            src = w_down.at[layer, pl.ds(pl.multiple_of(core * (FF // 2) + lax.rem(i, 4) * TD, TD), TD), pl.ds(pl.multiple_of((i // 4) * TN, TN), TN)]
        dst = ring.at[slot, pl.ds(0, TD)] if kind == 2 else ring.at[slot]
        return pltpu.make_async_copy(src, dst, ring_sem.at[slot])

    def fetch(t):
        pl.when(t < OUT_END)(lambda: tile_copy(t, 0).start())
        pl.when((t >= OUT_END) & (t < UP_END))(lambda: tile_copy(t, 1).start())
        pl.when((t >= UP_END) & (t < ALL_TILES))(lambda: tile_copy(t, 2).start())

    own, near = [], []
    for which, (owner, first, size) in enumerate(((1 - chip, 0, PART), (1 - chip, PART, PART), (chip, 0, TOK))):
        at = pl.ds(which * PART, size)
        rows = pl.ds(first, size)
        for i, (src, dst) in enumerate(((part_o, own_o), (part_l, own_l))):
            copy = pltpu.make_async_copy(src.at[owner, core, rows], dst.at[at], own_sem.at[which, i])
            copy.start()
            own.append(copy)
        near.append([
            send(part_o.at[owner, 1 - core, rows], got_o.at[at], dsend.at[which, 0], drecv.at[which, 0], partner),
            send(part_l.at[owner, 1 - core, rows], got_l.at[at], dsend.at[which, 1], drecv.at[which, 1], partner),
        ])
    meet((partner, across, diag))
    for pair in near:
        for copy in pair:
            copy.start()
    lax.fori_loop(0, RING_W, lambda t, carry: (fetch(t), carry)[1], 0)

    lane = lax.broadcasted_iota(jnp.int32, (8, HEAD), 1)
    far = []
    for part in range(2):
        for copy in own[2 * part:2 * part + 2]:
            copy.wait()
        for copy in near[part]:
            copy.wait_recv()

        def chip_merge(i, compact, part=part):
            j = part * PART + i
            o, l = merge([(own_o[j], own_l[j]), (got_o[j], got_l[j])])
            give_o[j] = o
            compact = jnp.where(lane == 2 * i, l[:8], compact)
            return jnp.where(lane == 2 * i + 1, l[8:], compact)

        give_l[part] = lax.fori_loop(0, PART, chip_merge, jnp.zeros((8, HEAD), F32), unroll=8)
        rows = pl.ds(part * PART, PART)
        pair = [
            send(give_l.at[part], far_l.at[part], xsend.at[part, 0], xrecv.at[part, 0], across),
            send(give_o.at[rows], far_o.at[rows], xsend.at[part, 1], xrecv.at[part, 1], across),
        ]
        for copy in pair:
            copy.start()
        far.append(pair)

    kv_all[me] = kv[...]
    new_rows = [send(kv, kv_all.at[me], ksend.at[i], krecv.at[i], peer) for i, peer in enumerate((partner, across))]
    new_rows.append(send(kv_all.at[across], kv_all.at[across], ksend.at[2], krecv.at[2], partner))

    for head in range(HALF_HEADS):
        tile = core * 4 + head // 4
        rows = pl.ds(head, TOK, stride=HALF_HEADS)
        q_rows[rows, :] = q_all[chip, tile, :, (head % 4) * HEAD:(head % 4 + 1) * HEAD].astype(F32)
        k_rows[rows, :] = kv[:, (head // 4) * HEAD:(head // 4 + 1) * HEAD].astype(F32)
        v_rows[rows, :] = kv[:, TN + (head // 4) * HEAD:TN + (head // 4 + 1) * HEAD].astype(F32)
    for copy in own[4:]:
        copy.wait()
    for copy in near[2]:
        copy.wait_recv()

    half = ROWS // 2

    def score(q, k):
        s = jnp.sum(q * k, axis=1, keepdims=True) * SCALE
        return jnp.broadcast_to(s, q.shape)

    def own_merge(i, carry):
        a = pl.ds(pl.multiple_of(i * HALF_HEADS, HALF_HEADS), HALF_HEADS)
        b = pl.ds(pl.multiple_of(half + i * HALF_HEADS, HALF_HEADS), HALF_HEADS)
        k0, v0, k1, v1 = k_rows[a, :], v_rows[a, :], k_rows[b, :], v_rows[b, :]
        q0, q1 = q_rows[a, :], q_rows[b, :]
        j = i + PART
        m, n = TOK + i, TOK + j
        o, l = merge([(own_o[m], own_l[m]), (got_o[m], got_l[m]), (v0, score(q0, k0))])
        mine_o[i] = o
        mine_l[i] = l
        o, l = merge([(own_o[n], own_l[n]), (got_o[n], got_l[n]), (v0, score(q1, k0)), (v1, score(q1, k1))])
        mine_o[j] = o
        mine_l[j] = l
        return carry

    lax.fori_loop(0, PART, own_merge, 0, unroll=4)

    for part in range(2):
        for copy in far[part]:
            copy.wait_recv()
        if part == 1:
            for copy in new_rows[:2]:
                copy.start()
            boxes.start()
        spread = far_l[part]

        def last_merge(i, carry, part=part, spread=spread):
            l = jnp.concatenate([
                jnp.broadcast_to(jnp.sum(jnp.where(lane == 2 * i + k, spread, 0.0), axis=1, keepdims=True), (8, HEAD)) for k in range(2)
            ], axis=0)
            j = part * PART + i
            o, _ = merge([(mine_o[j], mine_l[j]), (far_o[j], l)])
            q_rows[pl.ds(pl.multiple_of(j * HALF_HEADS, HALF_HEADS), HALF_HEADS), :] = o
            return carry

        lax.fori_loop(0, PART, last_merge, 0, unroll=8)
    for head in range(HALF_HEADS):
        attn[:, head * HEAD:(head + 1) * HEAD] = q_rows[pl.ds(head, TOK, stride=HALF_HEADS), :].astype(BF16)

    def reduce(j):
        return send(psend.at[j], precv.at[j], ssem.at[j], rsem.at[j], partner)

    def finish_sum(first, res, target):
        reduce(first + 7).start()
        for j in range(8):
            reduce(first + j).wait_recv()
            cols = slice(j * TN, (j + 1) * TN)
            target[:, cols] = (res[:, cols].astype(F32) + (psend[first + j] + precv[first + j])).astype(BF16)

    def project(j, carry):
        tile_copy(j, 0).wait()
        psend[j] = dot(attn[...], ring[lax.rem(j, RING_W)])
        fetch(j + RING_W)

        @pl.when(j > 0)
        def _():
            reduce(j - 1).start()
        return carry

    lax.fori_loop(0, OUT_END, project, 0)
    finish_sum(0, h_in, h)

    def up(s, carry):
        u = None
        for k in range(2):
            t = OUT_END + 2 * s + k
            tile_copy(t, 1).wait()
            part = dot(h[:, k * TK:(k + 1) * TK], ring[lax.rem(t, RING_W)])
            u = part if u is None else u + part
            fetch(t + RING_W)
        a = jax.nn.gelu(u.astype(BF16).astype(F32), approximate=True).astype(BF16)
        act[:, pl.ds(pl.multiple_of(s * TN, TN), TN)] = a
        return carry

    lax.fori_loop(0, UP_TILES, up, 0)
    new_rows[1].wait_recv()
    new_rows[2].start()

    def down(j, carry):
        total = None
        for k in range(4):
            t = UP_END + 4 * j + k
            tile_copy(t, 2).wait()
            part = dot(act[:, k * TD:(k + 1) * TD], ring[lax.rem(t, RING_W), :TD])
            total = part if total is None else total + part
            fetch(t + RING_W)
        psend[8 + j] = total

        @pl.when(j > 0)
        def _():
            reduce(8 + j - 1).start()
        return carry

    lax.fori_loop(0, D // TN, down, 0)
    finish_sum(8, h, out)
    for j in range(16):
        reduce(j).wait_send()
    for pair in near + far:
        for copy in pair:
            copy.wait_send()
    new_rows[0].wait()
    new_rows[1].wait_send()
    new_rows[2].wait()
    boxes.wait()


def run_rest(layer, mode, h, q_all, kv, part_o, part_l, outbox, w_out, w_up, w_down):
    token = (HALF_HEADS, HEAD)
    return pl.pallas_call(
        functools.partial(rest_kernel, layer, mode),
        name=f'rest{layer}_{mode}',
        out_shape=[jax.ShapeDtypeStruct((TOK, D), BF16), jax.ShapeDtypeStruct((4, TOK, 2 * TN), BF16), BOX],
        in_specs=[VMEM] * 3 + [ANY] * 6,
        out_specs=[VMEM, VMEM, ANY],
        scratch_shapes=[
            pltpu.VMEM((RING_W, TK, TN), BF16),
            DMA((RING_W,)),
            pltpu.VMEM((2 * TOK,) + token, F32),
            pltpu.VMEM((2 * TOK,) + token, F32),
            DMA((3, 2)),
            pltpu.VMEM((2 * TOK,) + token, F32),
            pltpu.VMEM((2 * TOK,) + token, F32),
            pltpu.VMEM((TOK,) + token, F32),
            pltpu.VMEM((TOK,) + token, F32),
            pltpu.VMEM((TOK,) + token, F32),
            pltpu.VMEM((2, 8, HEAD), F32),
            pltpu.VMEM((TOK,) + token, F32),
            pltpu.VMEM((2, 8, HEAD), F32),
            pltpu.VMEM((ROWS, HEAD), F32),
            pltpu.VMEM((ROWS, HEAD), F32),
            pltpu.VMEM((ROWS, HEAD), F32),
            pltpu.VMEM((TOK, 2048), BF16),
            pltpu.VMEM((TOK, FF // 2), BF16),
            pltpu.VMEM((TOK, D), BF16),
            pltpu.VMEM((16, TOK, TN), F32),
            pltpu.VMEM((16, TOK, TN), F32),
            DMA((3, 2)),
            DMA((3, 2)),
            DMA((2, 2)),
            DMA((2, 2)),
            DMA((16,)),
            DMA((16,)),
            DMA((3,)),
            DMA((3,)),
            DMA((3, MIG // CHUNK)),
            DMA((3, MIG // CHUNK)),
        ],
        cost_estimate=pl.CostEstimate(flops=2 * TOK * D * FF * 8, bytes_accessed=D * FF * 2, transcendentals=0),
        compiler_params=pltpu.CompilerParams(collective_id=2 + layer * 3 + mode, has_side_effects=True, vmem_limit_bytes=67043328),
    )(h, q_all, kv, part_o, part_l, w_out, w_up, w_down, outbox)


RING = 32
AHEAD = RING // 2


def finish_kernel(meta, moved, rows, inbox, k_rows, v_rows, k_in, v_in, k_out, v_out, buf, in_sem, out_sem, row_sem):
    del k_in, v_in
    outs = (k_out, v_out)
    count = meta[2]

    def load(i):
        slot = lax.rem(i, RING)
        return [pltpu.make_async_copy(inbox.at[moved[1, i], p], buf.at[slot, p], in_sem.at[slot, p]) for p in range(2)]

    def store(i):
        slot = lax.rem(i, RING)
        return [pltpu.make_async_copy(buf.at[slot, p], outs[p].at[moved[0, i], 1], out_sem.at[slot, p]) for p in range(2)]

    def begin(group):
        for copy in group:
            copy.start()

    def end(group):
        for copy in group:
            copy.wait()

    def loop(first, last, body):
        lax.fori_loop(first, last, lambda i, carry: (body(i), carry)[1], 0)

    loop(0, jnp.minimum(count, AHEAD), lambda i: begin(load(i)))

    def page(i):
        end(load(i))
        begin(store(i))

        @pl.when(i + AHEAD < count)
        def _():
            @pl.when(i >= AHEAD)
            def _():
                end(store(i - AHEAD))
            begin(load(i + AHEAD))

    loop(0, count, page)
    loop(jnp.maximum(count - RING, 0), count, lambda i: end(store(i)))

    def row(i):
        at = pl.ds(pl.multiple_of(rows[1, i] * KV_HEADS, KV_HEADS), KV_HEADS)
        return [pltpu.make_async_copy(src.at[l, rows[2, i]], outs[p].at[rows[0, i], l, at, :], row_sem.at[p, l]) for p, src in enumerate((k_rows, v_rows)) for l in range(LAYERS)]

    loop(0, meta[3], lambda i: begin(row(i)))
    loop(0, meta[3], lambda i: end(row(i)))


def run_finish(meta, moved, rows, inbox, k_rows, v_rows, k_part, v_part):
    shape = jax.ShapeDtypeStruct(k_part.shape, BF16)
    return pl.pallas_call(
        finish_kernel,
        name='finish',
        out_shape=[shape, shape],
        in_specs=[SMEM, SMEM, SMEM, ANY, VMEM, VMEM, ANY, ANY],
        out_specs=[ANY, ANY],
        scratch_shapes=[
            pltpu.VMEM((RING, 2) + k_part.shape[2:], BF16),
            DMA((RING, 2)),
            DMA((RING, 2)),
            DMA((2, LAYERS)),
        ],
        input_output_aliases={6: 0, 7: 1},
        cost_estimate=pl.CostEstimate(flops=10 ** 10, bytes_accessed=16 * 2 ** 20, transcendentals=0),
        compiler_params=pltpu.CompilerParams(vmem_limit_bytes=VMEM_LIMIT),
    )(meta, moved, rows, inbox, k_rows, v_rows, k_part, v_part)


def by_token(kv_all):
    x = kv_all.reshape(2, 2, TOK, 2, 4, HEAD)
    return x.transpose(3, 0, 2, 1, 4, 5).reshape(2, 2 * TOK, KV_HEADS, HEAD)


def solution(mesh):
    pool_spec = P(('rep', 'kv'))
    tok_spec = P(None, ('rep', 'kv'), None)

    def device_fn(embeds, w_query, w_key, w_value, w_out, w_up, w_down, k_pool, v_pool, new_table, seq_lens, mig_src, mig_dst):
        me = lax.axis_index('kv')
        weights = (w_query, w_key, w_value)
        k_flat, v_flat = flat_pool(k_pool), flat_pool(v_pool)
        meta, items, slots, moved, where = run_plan(new_table, seq_lens, mig_src, mig_dst)
        rows = []
        h = None
        for layer in range(LAYERS):
            if layer == 0:
                q_all, kv, h = run_qkv(layer, embeds, weights, True)
            else:
                q_all, kv = run_qkv(layer, h, weights, False)
            extra = (moved, inbox, pools[0]) if layer else ()
            part_o, part_l, outbox, *pools = run_attend(layer, meta, items, slots, q_all, k_flat, v_flat, extra)

            forms = [functools.partial(run_rest, layer, mode) for mode in range(len(MODES))]
            h, kv_all, inbox = lax.switch(meta[1], forms, h, q_all, kv, part_o, part_l, outbox, w_out, w_up, w_down)
            rows.append(by_token(kv_all))
        rows = jnp.stack(rows)
        k_out, v_out = run_finish(meta, moved, where, inbox, rows[:, 0], rows[:, 1], pools[1], pools[0])
        k_out, v_out = k_out.reshape(k_pool.shape), v_out.reshape(v_pool.shape)
        y = lax.dynamic_slice_in_dim(h.reshape(2, 32, D), (me % 2) * 16, 16, axis=1)
        return y, k_out, v_out

    return jax.shard_map(device_fn, mesh=mesh, in_specs=(tok_spec, P(), P(), P(), P(), P(), P(), pool_spec, pool_spec, P('rep', None), P('rep'), P('rep'), P('rep')), out_specs=(tok_spec, pool_spec, pool_spec), check_vma=False)
```

```python
import functools

import jax
import jax.numpy as jnp
from jax import lax
from jax.experimental import pallas as pl
from jax.experimental.pallas import tpu as pltpu
from jax.sharding import PartitionSpec as P

BF16 = jnp.bfloat16
F32 = jnp.float32
MESH = pl.DeviceIdType.MESH
NEG = -3.0e38
VMEM_LIMIT = 60 * 1024 * 1024

D = 4096
HEADS = 32
KV_HEADS = 8
HEAD = 128
FF = 14336
PAGE = 32
LAYERS = 2
SEQS = 64
MIG = 64
TOK = 64
HALF_HEADS = HEADS // 2
ROWS = TOK * HALF_HEADS
TN = 512
SCALE = HEAD ** -0.5
LOG2E = 1.4426950408889634
SLOTS = 96
UNROLL = 4
FAST_PAGES = 32
BOX = jax.ShapeDtypeStruct((3 * MIG, 2, PAGE * KV_HEADS, HEAD), BF16)


def flat_pool(pool):
    return pool.reshape(pool.shape[0], LAYERS, PAGE * KV_HEADS, HEAD)


def dot(a, b):
    return jnp.dot(a, b, preferred_element_type=F32)


def places():
    me = lax.axis_index('kv')
    core = lax.rem(me, 2)
    chip = me // 2
    partner = me + 1 - 2 * core
    across = lax.rem(me + 2, 4)
    diag = lax.rem(partner + 2, 4)
    return me, chip, core, partner, across, diag


def meet(peers):
    barrier = pltpu.get_barrier_semaphore()
    for peer in peers:
        pl.semaphore_signal(barrier, inc=1, device_id={'kv': peer}, device_id_type=MESH)
    pl.semaphore_wait(barrier, len(peers))


def send(src, dst, send_sem, recv_sem, peer):
    return pltpu.make_async_remote_copy(src_ref=src, dst_ref=dst, send_sem=send_sem, recv_sem=recv_sem, device_id={'kv': peer}, device_id_type=MESH)


VMEM = pl.BlockSpec(memory_space=pltpu.VMEM)
SMEM = pl.BlockSpec(memory_space=pltpu.SMEM)
ANY = pl.BlockSpec(memory_space=pl.ANY)
DMA = pltpu.SemaphoreType.DMA


WINDOW = 3


def qkv_kernel(layer, first, *refs):
    if first:
        emb, wq, wk, wv, q_all, kv, h, wbuf, wsem, psend, precv, xsend, xrecv, fsend, frecv, hsend, hrecv = refs
    else:
        h, wq, wk, wv, q_all, kv, wbuf, wsem, psend, precv, xsend, xrecv, fsend, frecv = refs
    me, chip, core, partner, across, diag = places()

    def fetch(j):
        if j < 4:
            src = wq.at[layer, :, pl.ds(pl.multiple_of(core * 2048 + j * TN, TN), TN)]
        else:
            src = (wk, wv)[j - 4].at[layer, :, pl.ds(pl.multiple_of(core * TN, TN), TN)]
        return pltpu.make_async_copy(src, wbuf.at[j], wsem.at[j])

    for j in range(WINDOW):
        fetch(j).start()
    meet((partner, across))
    if first:
        copies = []
        for t in range(2):
            rows = pl.ds(pl.multiple_of(t * 32 + core * 16, 16), 16)
            h[rows, :] = emb[t]
            copies.append(send(emb.at[t], h.at[rows, :], hsend.at[t], hrecv.at[t], partner))
        for copy in copies:
            copy.start()
        for copy in copies:
            copy.wait()

    def to_partner(j):
        ref = q_all.at[chip, core * 4 + j]
        return send(ref, ref, psend.at[j], precv.at[j], partner)

    def to_across(j):
        ref = q_all.at[chip, core * 4 + j]
        return send(ref, ref, xsend.at[j], xrecv.at[j], across)

    def forward(j):
        ref = q_all.at[1 - chip, core * 4 + j]
        return send(ref, ref, fsend.at[j], frecv.at[j], partner)

    def tile(j, carry):
        pltpu.make_async_copy(wq.at[layer, :, pl.ds(0, TN)], wbuf.at[j], wsem.at[j]).wait()
        q_all[chip, core * 4 + j] = dot(h[...], wbuf[j]).astype(BF16)
        for i in range(4):
            if i + WINDOW < 6:
                pl.when(j == i)(lambda i=i: fetch(i + WINDOW).start())

        @pl.when(j > 0)
        def _():
            to_across(j - 1).start()
            to_partner(j - 1).start()
        return carry

    lax.fori_loop(0, 4, tile, 0)
    for j in range(4, 6):
        fetch(j).wait()
        kv[:, (j - 4) * TN:(j - 3) * TN] = dot(h[...], wbuf[j]).astype(BF16)
        if j == 4:
            to_across(3).start()
            to_partner(3).start()
    for j in range(4):
        to_across(j).wait_recv()
        forward(j).start()
    for j in range(4):
        to_across(j).wait_send()
        to_partner(j).wait()
        forward(j).wait()


def run_qkv(layer, h, weights, first):
    wq, wk, wv = weights[:3]
    out_shape = [jax.ShapeDtypeStruct((2, 8, TOK, TN), BF16), jax.ShapeDtypeStruct((TOK, 2 * TN), BF16)]
    if first:
        out_shape.append(jax.ShapeDtypeStruct((TOK, D), BF16))
    scratch = [pltpu.VMEM((6, D, TN), BF16), DMA((6,))] + [DMA((4,))] * 6
    if first:
        scratch += [DMA((2,))] * 2
    return pl.pallas_call(
        functools.partial(qkv_kernel, layer, first),
        name=f'qkv{layer}',
        out_shape=out_shape,
        in_specs=[VMEM, ANY, ANY, ANY],
        out_specs=[VMEM] * len(out_shape),
        scratch_shapes=scratch,
        cost_estimate=pl.CostEstimate(flops=2 * TOK * D * 6 * TN * 8, bytes_accessed=D * 6 * TN * 2, transcendentals=0),
        compiler_params=pltpu.CompilerParams(collective_id=layer, has_side_effects=True, vmem_limit_bytes=VMEM_LIMIT),
    )(h, wq, wk, wv)


def plan_kernel(new_table, seq_lens, mig_src, mig_dst, meta, items, slots, gone, moved, rows, source, place_of, counts):
    me = lax.axis_index('kv')
    base = me * SLOTS

    def home(slot):
        return sum((slot >= i * SLOTS).astype(jnp.int32) for i in range(1, 4))

    def clear(i, carry):
        source[i] = -1
        place_of[i] = -1
        return carry

    lax.fori_loop(0, 4 * SLOTS, clear, 0, unroll=16)
    for i in range(16):
        counts[i] = 0

    def keep(i, carry):
        slots[i] = 0
        return carry

    lax.fori_loop(0, SLOTS, keep, 0, unroll=16)

    def entry(e, carry):
        n, m, even, odd = carry
        s, d = mig_src[e], mig_dst[e]
        hs, hd = home(s), home(d)
        pair = hs * 4 + hd
        rank = counts[pair]
        counts[pair] = rank + 1
        channel = (hs ^ hd) - 1
        place = channel * MIG + rank
        source[d] = s
        place_of[d] = place
        misfit = ((channel == 1) | (rank >= FAST_PAGES)).astype(jnp.int32)
        even = even | misfit | (hs & 1)
        odd = odd | misfit | (1 - (hs & 1))

        slots[jnp.where(hs == me, s - base, SLOTS)] = 1
        slots[jnp.where(hd == me, d - base, SLOTS)] = 1
        gone[m] = s - base
        moved[0, n] = d - base
        moved[1, n] = place
        return n + (hd == me).astype(jnp.int32), m + (hs == me).astype(jnp.int32), even, odd

    zero = jnp.int32(0)
    n_moved, n_gone, even, odd = lax.fori_loop(0, MIG, entry, (zero, zero, zero, zero), unroll=8)

    def sequence(b, carry):
        n, m = carry
        length = seq_lens[b]
        local, own, place = [], [], []
        for j in range(2):
            slot = new_table[j, b]
            src = source[slot]
            old = jnp.where(src >= 0, src, slot) - base
            mine = (old >= 0) & (old < SLOTS)
            local.append(old)
            own.append(mine)
            place.append(jnp.where(mine, place_of[slot], -1))
        items[0, n] = b
        items[1, n] = jnp.where(own[0], local[0], -1)
        items[2, n] = jnp.where(own[1], local[1], -1)
        items[3, n] = jnp.where(own[0], jnp.minimum(length, PAGE), 0)
        items[4, n] = jnp.where(own[1], jnp.maximum(length - PAGE, 0), 0)
        items[5, n] = place[0]
        items[6, n] = place[1]
        for t in range(2):
            pos = length + t
            second = pos >= PAGE
            here = jnp.where(second, new_table[1, b], new_table[0, b]) - base
            rows[0, m] = here
            rows[1, m] = jnp.where(second, pos - PAGE, pos)
            rows[2, m] = (b // 32) * TOK + t * 32 + b % 32
            m = m + ((here >= 0) & (here < SLOTS)).astype(jnp.int32)
        return n + (own[0] | own[1]).astype(jnp.int32), m

    n_items, n_rows = lax.fori_loop(0, SEQS, sequence, (zero, zero), unroll=8)

    @pl.when(n_items > 0)
    def _():
        for i in range(UNROLL - 1):
            for f in range(5):
                items[f, n_items + i] = items[f, n_items - 1]
            for f in range(5, 7):
                items[f, n_items + i] = -1
    meta[0] = n_items
    meta[1] = jnp.where(even == 0, 0, jnp.where(odd == 0, 1, 2))
    meta[2] = n_moved
    meta[3] = n_rows
    meta[4] = n_gone


def run_plan(new_table, seq_lens, mig_src, mig_dst):
    shapes = [(5,), (7, SEQS + UNROLL), (SLOTS + 1,), (MIG + 1,), (2, MIG + 1), (3, 2 * SEQS + 1)]
    return pl.pallas_call(
        plan_kernel,
        name='plan',
        out_shape=[jax.ShapeDtypeStruct(shape, jnp.int32) for shape in shapes],
        in_specs=[SMEM] * 4,
        out_specs=[SMEM] * len(shapes),
        scratch_shapes=[pltpu.SMEM((4 * SLOTS,), jnp.int32), pltpu.SMEM((4 * SLOTS,), jnp.int32), pltpu.SMEM((16,), jnp.int32)],
    )(new_table.T, seq_lens, mig_src, mig_dst)


NBUF = 6
AFTER = 2
DIST = NBUF - AFTER
STEPS = SEQS // UNROLL
SLOTS_STEP = SLOTS // STEPS


def attend_kernel(layer, meta, table, slots, q_all, k_pool, v_pool, *refs):
    if layer == 0:
        part_o, part_l, outbox, pool_out, *refs = refs
    else:
        moved, inbox, spare, _, part_o, part_l, outbox, pool_out, k_out, *refs, pages, page_in, page_out = refs
    q_rows, kbuf, vbuf, ring, sems, out_sems, ring_in, ring_out = refs
    pool = (k_pool, v_pool)[layer]
    groups = (meta[0] + UNROLL - 1) // UNROLL

    def copies(g, start):
        slot = lax.rem(g, NBUF)
        for u in range(UNROLL):
            for j in range(2):
                page = table[1 + j, g * UNROLL + u]

                @pl.when(page >= 0)
                def _():
                    for ref, buf in ((k_pool, kbuf), (v_pool, vbuf)):
                        copy = pltpu.make_async_copy(ref.at[page, layer], buf.at[slot, u, j], sems.at[slot])
                        copy.start() if start else copy.wait()

    def packs(g, start):
        slot = lax.rem(g, NBUF)
        for u in range(UNROLL):
            for j in range(2):
                place = table[5 + j, g * UNROLL + u]

                @pl.when(place >= 0)
                def _():
                    for p, buf in enumerate((kbuf, vbuf)):
                        copy = pltpu.make_async_copy(buf.at[slot, u, j], outbox.at[place, p], out_sems.at[slot])
                        copy.start() if start else copy.wait()

    def keep(s, phase):
        place = lax.rem(s, NBUF)
        for i in range(SLOTS_STEP):
            slot = s * SLOTS_STEP + i

            @pl.when(slots[slot] == 0)
            def _():
                if phase < 2:
                    load = pltpu.make_async_copy(pool.at[slot], ring.at[place, i], ring_in.at[place, i])
                    load.wait() if phase else load.start()
                if phase > 0:
                    store = pltpu.make_async_copy(ring.at[place, i], pool_out.at[slot], ring_out.at[place, i])
                    store.start() if phase == 1 else store.wait()

    def settle(phase):
        def one(i, carry):
            def move(box):
                for p, dst in enumerate((k_out, pool_out)):
                    if phase < 2:
                        copy = pltpu.make_async_copy(box.at[moved[1, i], p], pages.at[i, p], page_in)
                    else:
                        copy = pltpu.make_async_copy(pages.at[i, p], dst.at[moved[0, i], 0], page_out)
                    copy.wait() if phase % 2 else copy.start()

            if phase:
                move(inbox)
            else:
                pl.when(meta[1] < 2)(lambda: move(inbox))
                pl.when(meta[1] == 2)(lambda: move(spare))
            return carry

        lax.fori_loop(0, meta[2], one, 0)

    if layer == 1:
        settle(0)
    vbuf[...] = jnp.zeros_like(vbuf)
    for g in range(DIST):
        @pl.when(g < groups)
        def _():
            copies(g, True)
        keep(g, 0)
    part_o[...] = jnp.zeros_like(part_o)
    part_l[...] = jnp.full_like(part_l, NEG)

    for chip in range(2):
        for tile in range(8):
            for i in range(4):
                rows = q_all[chip, tile, :, i * HEAD:(i + 1) * HEAD].astype(F32)
                q_rows[pl.ds(chip * TOK * HEADS + tile * 4 + i, TOK, stride=HEADS), :] = rows

    row = lax.broadcasted_iota(jnp.int32, (2 * HEADS, 256), 0)
    col = lax.broadcasted_iota(jnp.int32, (2 * HEADS, 256), 1)
    pos = jnp.where((row % HEADS) // 4 == col % KV_HEADS, col // KV_HEADS, PAGE)

    def attend(g):
        slot = lax.rem(g, NBUF)
        outs = []
        for u in range(UNROLL):
            item = g * UNROLL + u
            seq = table[0, item]
            base = (seq // 32) * TOK * HEADS + (seq % 32) * HEADS
            q0 = q_rows[pl.ds(pl.multiple_of(base, HEADS), HEADS), :]
            q1 = q_rows[pl.ds(pl.multiple_of(base + 32 * HEADS, HEADS), HEADS), :]
            q = jnp.concatenate([q0, q1], axis=0).astype(BF16)
            scores = []
            for j in range(2):
                s = lax.dot_general(q, kbuf[slot, u, j], (((1,), (1,)), ((), ())), preferred_element_type=F32)
                scores.append(jnp.where(pos < table[3 + j, item], s, NEG))
            top = jnp.max(jnp.maximum(scores[0], scores[1]), axis=1, keepdims=True)
            probs = [jnp.exp2((s - top) * (SCALE * LOG2E)) for s in scores]
            total = jnp.sum(probs[0] + probs[1], axis=1, keepdims=True)
            out = sum(dot(p.astype(BF16), vbuf[slot, u, j]) for j, p in enumerate(probs))
            live = top > NEG
            lse = jnp.where(live, top * SCALE + jnp.log(total), NEG)
            outs.append((seq, jnp.where(live, out / total, 0.0), jnp.broadcast_to(lse, (2 * HEADS, HEAD))))
        for seq, out, lse in outs:
            for t in range(2):
                for half in range(2):
                    rows = slice(t * HEADS + half * HALF_HEADS, t * HEADS + (half + 1) * HALF_HEADS)
                    part_o[seq // 32, half, t * 32 + seq % 32] = out[rows]
                    part_l[seq // 32, half, t * 32 + seq % 32] = lse[rows]

    def step(g, carry):
        keep(g, 1)
        if layer == 1:
            @pl.when(g == STEPS // 2)
            def _():
                settle(1)
                settle(2)

        @pl.when(g < groups)
        def _():
            copies(g, False)
            packs(g, True)

        @pl.when(g >= AFTER)
        def _():
            keep(g - AFTER, 2)

        @pl.when((g >= AFTER) & (g - AFTER < groups))
        def _():
            packs(g - AFTER, False)

        @pl.when(g + DIST < STEPS)
        def _():
            keep(g + DIST, 0)

        @pl.when(g + DIST < groups)
        def _():
            copies(g + DIST, True)

        @pl.when(g < groups)
        def _():
            attend(g)
        return carry

    lax.fori_loop(0, STEPS, step, 0)
    for g in range(STEPS - AFTER, STEPS):
        keep(g, 2)

        @pl.when(g < groups)
        def _():
            packs(g, False)
    if layer == 1:
        settle(3)


def run_attend(layer, meta, table, slots, q_all, k_flat, v_flat, extra=()):
    shape = jax.ShapeDtypeStruct((2, 2, TOK, HALF_HEADS, HEAD), F32)
    page = (UNROLL, 2, PAGE * KV_HEADS, HEAD)
    return pl.pallas_call(
        functools.partial(attend_kernel, layer),
        name=f'attend{layer}',
        out_shape=[shape, shape, BOX] + [jax.ShapeDtypeStruct(k_flat.shape, BF16)] * (layer + 1),
        in_specs=[SMEM, SMEM, SMEM, VMEM, ANY, ANY] + [SMEM, ANY, ANY, ANY] * layer,
        out_specs=[VMEM, VMEM, ANY, ANY] + [ANY] * layer,
        input_output_aliases={9: 4} if layer else {},
        scratch_shapes=[
            pltpu.VMEM((2 * TOK * HEADS, HEAD), F32),
            pltpu.VMEM((NBUF,) + page, BF16),
            pltpu.VMEM((NBUF,) + page, BF16),
            pltpu.VMEM((NBUF, SLOTS_STEP) + k_flat.shape[1:], BF16),
            DMA((NBUF,)),
            DMA((NBUF,)),
            DMA((NBUF, SLOTS_STEP)),
            DMA((NBUF, SLOTS_STEP)),
        ] + [pltpu.VMEM((MIG, 2, PAGE * KV_HEADS, HEAD), BF16), DMA, DMA] * layer,
        cost_estimate=pl.CostEstimate(flops=2 * 10 ** 10, bytes_accessed=16 * 2 ** 20, transcendentals=0),
        compiler_params=pltpu.CompilerParams(vmem_limit_bytes=VMEM_LIMIT),
    )(meta, table, slots, q_all, k_flat, v_flat, *extra)


def merge(parts):
    top = functools.reduce(jnp.maximum, [l for _, l in parts])
    weights = [jnp.exp(l - top) for _, l in parts]
    total = functools.reduce(jnp.add, weights)
    out = functools.reduce(jnp.add, [w * o for w, (o, _) in zip(weights, parts)]) / total
    return out, top + jnp.log(total)


LANES = ([((0,), 2, FAST_PAGES), ((0,), 0, FAST_PAGES)], [((1,), 2, FAST_PAGES), ((1,), 0, FAST_PAGES)])
EVERYTHING = [((0, 1), i, MIG) for i in range(3)]
CHUNK = 2


class Boxes:
    def __init__(self, moves, outbox, inbox, send_sems, recv_sems):
        me, chip, self.core, partner, across, diag = places()
        self.peers = (partner, across, diag)
        self.moves, self.outbox, self.inbox, self.send_sems, self.recv_sems = moves, outbox, inbox, send_sems, recv_sems

    def each(self, sending, act):
        for cores, channel, pages in self.moves:
            def run(channel=channel, pages=pages):
                def one(i, carry):
                    rows = pl.ds(channel * MIG + i * CHUNK, CHUNK)
                    act(send(self.outbox.at[rows], self.inbox.at[rows], self.send_sems.at[channel, i], self.recv_sems.at[channel, i], self.peers[channel]))
                    return carry

                lax.fori_loop(0, pages // CHUNK, one, 0)

            if len(cores) == 2:
                run()
            else:
                cross = 0 if channel == 1 else 1
                at = cores[0] if sending else (cores[0] + cross) % 2
                pl.when(self.core == at)(run)

    def start(self):
        self.each(True, lambda copy: copy.start())

    def wait(self):
        self.each(True, lambda copy: copy.wait_send())
        self.each(False, lambda copy: copy.wait_recv())


RING_W = 18
TK = 2048
UP_TILES = FF // 2 // TN
TD = FF // 8
OUT_END = D // TN
UP_END = OUT_END + 2 * UP_TILES
DOWN_END = UP_END + 4 * (D // TN)
QKV_END = DOWN_END + 12
PART = TOK // 2


def rest_kernel(layer, lane_core, h_in, q_all, kv, part_o, part_l, wo, w_up, w_down, outbox, *refs):
    last = layer == LAYERS - 1
    if last:
        out, kv_all, inbox, *refs = refs
    else:
        wq, wk, wv, out, kv_all, inbox, q_next, kv_next, *refs = refs
        *refs, qp_send, qp_recv, qx_send, qx_recv, qf_send, qf_recv = refs
    (ring, ring_sem, own_o, own_l, own_sem, got_o, got_l, mine_o, mine_l, give_o, give_l, far_o, far_l, q_rows, k_rows, v_rows, attn, act, h,
     psend, precv, dsend, drecv, xsend, xrecv, ssem, rsem, ksend, krecv, bsend, brecv) = refs
    me, chip, core, partner, across, diag = places()
    boxes = Boxes(LANES[lane_core], outbox, inbox, bsend, brecv)
    end = DOWN_END if last else QKV_END

    def tile_copy(t, kind):
        slot = lax.rem(t, RING_W)
        if kind == 0:
            src = wo.at[layer, pl.ds(pl.multiple_of(core * TK, TK), TK), pl.ds(pl.multiple_of(t * TN, TN), TN)]
        elif kind == 1:
            i = t - OUT_END
            src = w_up.at[layer, pl.ds(pl.multiple_of(lax.rem(i, 2) * TK, TK), TK), pl.ds(pl.multiple_of(core * (FF // 2) + (i // 2) * TN, TN), TN)]
        elif kind >= 3:
            i = t - DOWN_END
            rows = pl.ds(pl.multiple_of(lax.rem(i, 2) * TK, TK), TK)
            if kind == 3:
                src = wq.at[layer + 1, rows, pl.ds(pl.multiple_of(core * 2048 + (i // 2) * TN, TN), TN)]
            else:
                src = (wk, wv)[kind - 4].at[layer + 1, rows, pl.ds(pl.multiple_of(core * TN, TN), TN)]
        else:
            i = t - UP_END
            src = w_down.at[layer, pl.ds(pl.multiple_of(core * (FF // 2) + lax.rem(i, 4) * TD, TD), TD), pl.ds(pl.multiple_of((i // 4) * TN, TN), TN)]
        dst = ring.at[slot, pl.ds(0, TD)] if kind == 2 else ring.at[slot]
        return pltpu.make_async_copy(src, dst, ring_sem.at[slot])

    def fetch(t):
        pl.when(t < OUT_END)(lambda: tile_copy(t, 0).start())
        pl.when((t >= OUT_END) & (t < UP_END))(lambda: tile_copy(t, 1).start())
        pl.when((t >= UP_END) & (t < DOWN_END))(lambda: tile_copy(t, 2).start())
        if not last:
            pl.when((t >= DOWN_END) & (t < DOWN_END + 8))(lambda: tile_copy(t, 3).start())
            pl.when((t >= DOWN_END + 8) & (t < DOWN_END + 10))(lambda: tile_copy(t, 4).start())
            pl.when((t >= DOWN_END + 10) & (t < QKV_END))(lambda: tile_copy(t, 5).start())

    own, near = [], []
    for which, (owner, first, size) in enumerate(((1 - chip, 0, PART), (1 - chip, PART, PART), (chip, 0, TOK))):
        at = pl.ds(which * PART, size)
        rows = pl.ds(first, size)
        for i, (src, dst) in enumerate(((part_o, own_o), (part_l, own_l))):
            copy = pltpu.make_async_copy(src.at[owner, core, rows], dst.at[at], own_sem.at[which, i])
            copy.start()
            own.append(copy)
        near.append([
            send(part_o.at[owner, 1 - core, rows], got_o.at[at], dsend.at[which, 0], drecv.at[which, 0], partner),
            send(part_l.at[owner, 1 - core, rows], got_l.at[at], dsend.at[which, 1], drecv.at[which, 1], partner),
        ])
    meet((partner, across, diag))
    for pair in near:
        for copy in pair:
            copy.start()
    lax.fori_loop(0, RING_W, lambda t, carry: (fetch(t), carry)[1], 0)

    lane = lax.broadcasted_iota(jnp.int32, (8, HEAD), 1)
    far = []
    for part in range(2):
        for copy in own[2 * part:2 * part + 2]:
            copy.wait()
        for copy in near[part]:
            copy.wait_recv()

        def chip_merge(i, compact, part=part):
            j = part * PART + i
            o, l = merge([(own_o[j], own_l[j]), (got_o[j], got_l[j])])
            give_o[j] = o
            compact = jnp.where(lane == 2 * i, l[:8], compact)
            return jnp.where(lane == 2 * i + 1, l[8:], compact)

        give_l[part] = lax.fori_loop(0, PART, chip_merge, jnp.zeros((8, HEAD), F32), unroll=8)
        rows = pl.ds(part * PART, PART)
        pair = [
            send(give_l.at[part], far_l.at[part], xsend.at[part, 0], xrecv.at[part, 0], across),
            send(give_o.at[rows], far_o.at[rows], xsend.at[part, 1], xrecv.at[part, 1], across),
        ]
        for copy in pair:
            copy.start()
        far.append(pair)

    kv_all[me] = kv[...]
    new_rows = [send(kv, kv_all.at[me], ksend.at[i], krecv.at[i], peer) for i, peer in enumerate((partner, across))]
    new_rows.append(send(kv_all.at[across], kv_all.at[across], ksend.at[2], krecv.at[2], partner))

    for head in range(HALF_HEADS):
        tile = core * 4 + head // 4
        rows = pl.ds(head, TOK, stride=HALF_HEADS)
        q_rows[rows, :] = q_all[chip, tile, :, (head % 4) * HEAD:(head % 4 + 1) * HEAD].astype(F32)
        k_rows[rows, :] = kv[:, (head // 4) * HEAD:(head // 4 + 1) * HEAD].astype(F32)
        v_rows[rows, :] = kv[:, TN + (head // 4) * HEAD:TN + (head // 4 + 1) * HEAD].astype(F32)
    for copy in own[4:]:
        copy.wait()
    for copy in near[2]:
        copy.wait_recv()

    half = ROWS // 2

    def score(q, k):
        s = jnp.sum(q * k, axis=1, keepdims=True) * SCALE
        return jnp.broadcast_to(s, q.shape)

    def own_merge(i, carry):
        a = pl.ds(pl.multiple_of(i * HALF_HEADS, HALF_HEADS), HALF_HEADS)
        b = pl.ds(pl.multiple_of(half + i * HALF_HEADS, HALF_HEADS), HALF_HEADS)
        k0, v0, k1, v1 = k_rows[a, :], v_rows[a, :], k_rows[b, :], v_rows[b, :]
        q0, q1 = q_rows[a, :], q_rows[b, :]
        j = i + PART
        m, n = TOK + i, TOK + j
        o, l = merge([(own_o[m], own_l[m]), (got_o[m], got_l[m]), (v0, score(q0, k0))])
        mine_o[i] = o
        mine_l[i] = l
        o, l = merge([(own_o[n], own_l[n]), (got_o[n], got_l[n]), (v0, score(q1, k0)), (v1, score(q1, k1))])
        mine_o[j] = o
        mine_l[j] = l
        return carry

    lax.fori_loop(0, PART, own_merge, 0, unroll=4)

    for part in range(2):
        for copy in far[part]:
            copy.wait_recv()
        if part == 1:
            for copy in new_rows[:2]:
                copy.start()
            boxes.start()
        spread = far_l[part]

        def last_merge(i, carry, part=part, spread=spread):
            l = jnp.concatenate([
                jnp.broadcast_to(jnp.sum(jnp.where(lane == 2 * i + k, spread, 0.0), axis=1, keepdims=True), (8, HEAD)) for k in range(2)
            ], axis=0)
            j = part * PART + i
            o, _ = merge([(mine_o[j], mine_l[j]), (far_o[j], l)])
            q_rows[pl.ds(pl.multiple_of(j * HALF_HEADS, HALF_HEADS), HALF_HEADS), :] = o
            return carry

        lax.fori_loop(0, PART, last_merge, 0, unroll=8)
    for head in range(HALF_HEADS):
        attn[:, head * HEAD:(head + 1) * HEAD] = q_rows[pl.ds(head, TOK, stride=HALF_HEADS), :].astype(BF16)

    def reduce(j):
        return send(psend.at[j], precv.at[j], ssem.at[j], rsem.at[j], partner)

    def finish_sum(first, res, target):
        reduce(first + 7).start()
        for j in range(8):
            reduce(first + j).wait_recv()
            cols = slice(j * TN, (j + 1) * TN)
            target[:, cols] = (res[:, cols].astype(F32) + (psend[first + j] + precv[first + j])).astype(BF16)

    def project(j, carry):
        tile_copy(j, 0).wait()
        psend[j] = dot(attn[...], ring[lax.rem(j, RING_W)])
        fetch(j + RING_W)

        @pl.when(j > 0)
        def _():
            reduce(j - 1).start()
        return carry

    lax.fori_loop(0, OUT_END, project, 0)
    finish_sum(0, h_in, h)

    def up(s, carry):
        u = None
        for k in range(2):
            t = OUT_END + 2 * s + k
            tile_copy(t, 1).wait()
            part = dot(h[:, k * TK:(k + 1) * TK], ring[lax.rem(t, RING_W)])
            u = part if u is None else u + part
            fetch(t + RING_W)
        a = jax.nn.gelu(u.astype(BF16).astype(F32), approximate=True).astype(BF16)
        act[:, pl.ds(pl.multiple_of(s * TN, TN), TN)] = a
        return carry

    lax.fori_loop(0, UP_TILES, up, 0)
    new_rows[1].wait_recv()
    new_rows[2].start()

    def down(j, carry):
        total = None
        for k in range(4):
            t = UP_END + 4 * j + k
            tile_copy(t, 2).wait()
            part = dot(act[:, k * TD:(k + 1) * TD], ring[lax.rem(t, RING_W), :TD])
            total = part if total is None else total + part
            fetch(t + RING_W)
        psend[8 + j] = total

        @pl.when(j > 0)
        def _():
            reduce(8 + j - 1).start()
        return carry

    lax.fori_loop(0, D // TN, down, 0)
    finish_sum(8, h, out)

    if not last:
        def to_partner(j):
            ref = q_next.at[chip, core * 4 + j]
            return send(ref, ref, qp_send.at[j], qp_recv.at[j], partner)

        def to_across(j):
            ref = q_next.at[chip, core * 4 + j]
            return send(ref, ref, qx_send.at[j], qx_recv.at[j], across)

        def forward(j):
            ref = q_next.at[1 - chip, core * 4 + j]
            return send(ref, ref, qf_send.at[j], qf_recv.at[j], partner)

        def project_next(j, kind):
            total = None
            for k in range(2):
                t = DOWN_END + 2 * j + k
                tile_copy(t, kind).wait()
                part = dot(out[:, k * TK:(k + 1) * TK], ring[lax.rem(t, RING_W)])
                total = part if total is None else total + part
            return total.astype(BF16)

        def query(j, carry):
            q_next[chip, core * 4 + j] = project_next(j, 3)

            @pl.when(j > 0)
            def _():
                to_across(j - 1).start()
                to_partner(j - 1).start()
            return carry

        lax.fori_loop(0, 4, query, 0)
        to_across(3).start()
        to_partner(3).start()

        def key_value(j, carry):
            kv_next[:, pl.ds(pl.multiple_of(j * TN, TN), TN)] = project_next(j + 4, 4)
            return carry

        lax.fori_loop(0, 2, key_value, 0)
        for j in range(4):
            to_across(j).wait_recv()
            forward(j).start()
        for j in range(4):
            to_across(j).wait_send()
            to_partner(j).wait()
            forward(j).wait()
    for j in range(16):
        reduce(j).wait_send()
    for pair in near + far:
        for copy in pair:
            copy.wait_send()
    new_rows[0].wait()
    new_rows[1].wait_send()
    new_rows[2].wait()
    boxes.wait()


def run_rest(layer, lane_core, h, q_all, kv, part_o, part_l, outbox, w_out, w_up, w_down, *weights):
    more = [jax.ShapeDtypeStruct((2, 8, TOK, TN), BF16), jax.ShapeDtypeStruct((TOK, 2 * TN), BF16)] if weights else []
    token = (HALF_HEADS, HEAD)
    return pl.pallas_call(
        functools.partial(rest_kernel, layer, lane_core),
        name=f'rest{layer}_{lane_core}',
        out_shape=[jax.ShapeDtypeStruct((TOK, D), BF16), jax.ShapeDtypeStruct((4, TOK, 2 * TN), BF16), BOX] + more,
        in_specs=[VMEM] * 3 + [ANY] * (6 + len(weights)),
        out_specs=[VMEM, VMEM, ANY] + [VMEM] * len(more),
        scratch_shapes=[
            pltpu.VMEM((RING_W, TK, TN), BF16),
            DMA((RING_W,)),
            pltpu.VMEM((2 * TOK,) + token, F32),
            pltpu.VMEM((2 * TOK,) + token, F32),
            DMA((3, 2)),
            pltpu.VMEM((2 * TOK,) + token, F32),
            pltpu.VMEM((2 * TOK,) + token, F32),
            pltpu.VMEM((TOK,) + token, F32),
            pltpu.VMEM((TOK,) + token, F32),
            pltpu.VMEM((TOK,) + token, F32),
            pltpu.VMEM((2, 8, HEAD), F32),
            pltpu.VMEM((TOK,) + token, F32),
            pltpu.VMEM((2, 8, HEAD), F32),
            pltpu.VMEM((ROWS, HEAD), F32),
            pltpu.VMEM((ROWS, HEAD), F32),
            pltpu.VMEM((ROWS, HEAD), F32),
            pltpu.VMEM((TOK, 2048), BF16),
            pltpu.VMEM((TOK, FF // 2), BF16),
            pltpu.VMEM((TOK, D), BF16),
            pltpu.VMEM((16, TOK, TN), F32),
            pltpu.VMEM((16, TOK, TN), F32),
            DMA((3, 2)),
            DMA((3, 2)),
            DMA((2, 2)),
            DMA((2, 2)),
            DMA((16,)),
            DMA((16,)),
            DMA((3,)),
            DMA((3,)),
            DMA((3, MIG // CHUNK)),
            DMA((3, MIG // CHUNK)),
        ] + [DMA((4,))] * (6 if weights else 0),
        cost_estimate=pl.CostEstimate(flops=2 * TOK * D * FF * 8, bytes_accessed=D * FF * 2, transcendentals=0),
        compiler_params=pltpu.CompilerParams(collective_id=2 + layer * 2 + lane_core, has_side_effects=True, vmem_limit_bytes=67043328),
    )(h, q_all, kv, part_o, part_l, w_out, w_up, w_down, outbox, *weights)


def move_kernel(outbox, inbox, send_sems, recv_sems):
    me, chip, core, partner, across, diag = places()
    meet((partner, across, diag))
    boxes = Boxes(EVERYTHING, outbox, inbox, send_sems, recv_sems)
    boxes.start()
    boxes.wait()


def run_move(layer, outbox):
    return pl.pallas_call(
        move_kernel,
        name=f'move{layer}',
        out_shape=BOX,
        in_specs=[ANY],
        out_specs=ANY,
        scratch_shapes=[DMA((3, MIG // CHUNK)), DMA((3, MIG // CHUNK))],
        compiler_params=pltpu.CompilerParams(collective_id=6 + layer, has_side_effects=True),
    )(outbox)


def run_blank(layer):
    return pl.pallas_call(lambda box: None, name=f'blank{layer}', out_shape=BOX, out_specs=ANY)()


RING = 32
AHEAD = RING // 2


def finish_kernel(meta, moved, gone, rows, inbox, spare, kv0, kv1, k_in, v_in, k_out, v_out, wide, row_buf, zeros, buf, in_sem, out_sem, zero_sem, row_sem):
    del k_in, v_in
    outs = (k_out, v_out)
    count = meta[2]

    def loop(first, last, body):
        lax.fori_loop(first, last, lambda i, carry: (body(i), carry)[1], 0)

    def clear(i):
        return [pltpu.make_async_copy(zeros, out.at[gone[i]], zero_sem) for out in outs]

    def load(i, box):
        slot = lax.rem(i, RING)
        return [pltpu.make_async_copy(box.at[moved[1, i], p], buf.at[slot, p], in_sem.at[slot, p]) for p in range(2)]

    def store(i):
        slot = lax.rem(i, RING)
        return [pltpu.make_async_copy(buf.at[slot, p], outs[p].at[moved[0, i], 1], out_sem.at[slot, p]) for p in range(2)]

    def begin(group):
        for copy in group:
            copy.start()

    def end(group):
        for copy in group:
            copy.wait()

    def begin_load(i):
        pl.when(meta[1] < 2)(lambda: begin(load(i, inbox)))
        pl.when(meta[1] == 2)(lambda: begin(load(i, spare)))

    loop(0, jnp.minimum(count, AHEAD), begin_load)
    zeros[...] = jnp.zeros_like(zeros)
    loop(0, meta[4], lambda i: begin(clear(i)))

    for l, kv in enumerate((kv0, kv1)):
        for p in range(2):
            for dev in range(4):
                for i in range(4):
                    at = pl.ds((dev // 2) * TOK * KV_HEADS + (dev % 2) * 4 + i, TOK, stride=KV_HEADS)
                    wide[at, :] = kv[dev, :, (p * 4 + i) * HEAD:(p * 4 + i + 1) * HEAD].astype(F32)
            row_buf[p, l] = wide[...].astype(BF16)

    def page(i):
        end(load(i, inbox))
        begin(store(i))

        @pl.when(i + AHEAD < count)
        def _():
            @pl.when(i >= AHEAD)
            def _():
                end(store(i - AHEAD))
            begin_load(i + AHEAD)

    loop(0, count, page)
    loop(jnp.maximum(count - RING, 0), count, lambda i: end(store(i)))

    def row(i):
        at = pl.ds(pl.multiple_of(rows[1, i] * KV_HEADS, KV_HEADS), KV_HEADS)
        src = pl.ds(pl.multiple_of(rows[2, i] * KV_HEADS, KV_HEADS), KV_HEADS)
        return [pltpu.make_async_copy(row_buf.at[p, l, src, :], outs[p].at[rows[0, i], l, at, :], row_sem.at[p, l]) for p in range(2) for l in range(LAYERS)]

    loop(0, meta[3], lambda i: begin(row(i)))
    loop(0, meta[3], lambda i: end(row(i)))
    loop(0, meta[4], lambda i: end(clear(i)))


def run_finish(meta, moved, gone, rows, boxes, kvs, k_part, v_part):
    shape = jax.ShapeDtypeStruct(k_part.shape, BF16)
    return pl.pallas_call(
        finish_kernel,
        name='finish',
        out_shape=[shape, shape],
        in_specs=[SMEM] * 4 + [ANY, ANY, VMEM, VMEM, ANY, ANY],
        out_specs=[ANY, ANY],
        scratch_shapes=[
            pltpu.VMEM((2 * TOK * KV_HEADS, HEAD), F32),
            pltpu.VMEM((2, LAYERS, 2 * TOK * KV_HEADS, HEAD), BF16),
            pltpu.VMEM(k_part.shape[1:], BF16),
            pltpu.VMEM((RING, 2) + k_part.shape[2:], BF16),
            DMA((RING, 2)),
            DMA((RING, 2)),
            DMA,
            DMA((2, LAYERS)),
        ],
        input_output_aliases={8: 0, 9: 1},
        cost_estimate=pl.CostEstimate(flops=10 ** 10, bytes_accessed=16 * 2 ** 20, transcendentals=0),
        compiler_params=pltpu.CompilerParams(vmem_limit_bytes=VMEM_LIMIT),
    )(meta, moved, gone, rows, *boxes, *kvs, k_part, v_part)


def solution(mesh):
    pool_spec = P(('rep', 'kv'))
    tok_spec = P(None, ('rep', 'kv'), None)

    def device_fn(embeds, w_query, w_key, w_value, w_out, w_up, w_down, k_pool, v_pool, new_table, seq_lens, mig_src, mig_dst):
        me = lax.axis_index('kv')
        weights = (w_query, w_key, w_value)
        k_flat, v_flat = flat_pool(k_pool), flat_pool(v_pool)
        meta, items, slots, gone, moved, where = run_plan(new_table, seq_lens, mig_src, mig_dst)
        lane_core = jnp.minimum(meta[1], 1)
        q_all, kv, h = run_qkv(0, embeds, weights, True)
        kvs, boxes, pools = [], (), ()
        for layer in range(LAYERS):
            extra = (moved, *boxes, *pools) if layer else ()
            part_o, part_l, outbox, *pools = run_attend(layer, meta, items, slots, q_all, k_flat, v_flat, extra)
            forms = [functools.partial(run_rest, layer, core) for core in range(2)]
            more = weights if layer == 0 else ()
            h, kv_all, inbox, *more = lax.switch(lane_core, forms, h, q_all, kv, part_o, part_l, outbox, w_out, w_up, w_down, *more)
            kvs.append(kv_all)
            if more:
                q_all, kv = more
            boxes = inbox, lax.cond(meta[1] == 2, functools.partial(run_move, layer), lambda box: run_blank(layer), outbox)
        k_out, v_out = run_finish(meta, moved, gone, where, boxes, kvs, pools[1], pools[0])
        k_out, v_out = k_out.reshape(k_pool.shape), v_out.reshape(v_pool.shape)
        y = lax.dynamic_slice_in_dim(h.reshape(2, 32, D), (me % 2) * 16, 16, axis=1)
        return y, k_out, v_out

    return jax.shard_map(device_fn, mesh=mesh, in_specs=(tok_spec, P(), P(), P(), P(), P(), P(), pool_spec, pool_spec, P('rep', None), P('rep'), P('rep'), P('rep')), out_specs=(tok_spec, pool_spec, pool_spec), check_vma=False)
```

```python
import functools

import jax
import jax.numpy as jnp
from jax import lax
from jax.experimental import pallas as pl
from jax.experimental.pallas import tpu as pltpu
from jax.sharding import PartitionSpec as P

BF16 = jnp.bfloat16
F32 = jnp.float32
MESH = pl.DeviceIdType.MESH
NEG = -3.0e38
VMEM_LIMIT = 60 * 1024 * 1024

D = 4096
HEADS = 32
KV_HEADS = 8
HEAD = 128
FF = 14336
PAGE = 32
LAYERS = 2
SEQS = 64
MIG = 64
TOK = 64
HALF_HEADS = HEADS // 2
ROWS = TOK * HALF_HEADS
TN = 512
SCALE = HEAD ** -0.5
LOG2E = 1.4426950408889634
SLOTS = 96
UNROLL = 4
FAST_PAGES = 32
LATE = 23
LATES = FAST_PAGES - LATE
BOX = jax.ShapeDtypeStruct((3 * MIG, 2, PAGE * KV_HEADS, HEAD), BF16)


def flat_pool(pool):
    return pool.reshape(pool.shape[0], LAYERS, PAGE * KV_HEADS, HEAD)


def dot(a, b):
    return jnp.dot(a, b, preferred_element_type=F32)


def places():
    me = lax.axis_index('kv')
    core = lax.rem(me, 2)
    chip = me // 2
    partner = me + 1 - 2 * core
    across = lax.rem(me + 2, 4)
    diag = lax.rem(partner + 2, 4)
    return me, chip, core, partner, across, diag


def meet(peers):
    barrier = pltpu.get_barrier_semaphore()
    for peer in peers:
        pl.semaphore_signal(barrier, inc=1, device_id={'kv': peer}, device_id_type=MESH)
    pl.semaphore_wait(barrier, len(peers))


def send(src, dst, send_sem, recv_sem, peer):
    return pltpu.make_async_remote_copy(src_ref=src, dst_ref=dst, send_sem=send_sem, recv_sem=recv_sem, device_id={'kv': peer}, device_id_type=MESH)


VMEM = pl.BlockSpec(memory_space=pltpu.VMEM)
SMEM = pl.BlockSpec(memory_space=pltpu.SMEM)
ANY = pl.BlockSpec(memory_space=pl.ANY)
DMA = pltpu.SemaphoreType.DMA


WINDOW = 3


def qkv_kernel(layer, first, *refs):
    if first:
        emb, wq, wk, wv, q_all, kv, h, wbuf, wsem, psend, precv, xsend, xrecv, fsend, frecv, hsend, hrecv = refs
    else:
        h, wq, wk, wv, q_all, kv, wbuf, wsem, psend, precv, xsend, xrecv, fsend, frecv = refs
    me, chip, core, partner, across, diag = places()

    def fetch(j):
        if j < 4:
            src = wq.at[layer, :, pl.ds(pl.multiple_of(core * 2048 + j * TN, TN), TN)]
        else:
            src = (wk, wv)[j - 4].at[layer, :, pl.ds(pl.multiple_of(core * TN, TN), TN)]
        return pltpu.make_async_copy(src, wbuf.at[j], wsem.at[j])

    for j in range(WINDOW):
        fetch(j).start()
    meet((partner, across))
    if first:
        copies = []
        for t in range(2):
            rows = pl.ds(pl.multiple_of(t * 32 + core * 16, 16), 16)
            h[rows, :] = emb[t]
            copies.append(send(emb.at[t], h.at[rows, :], hsend.at[t], hrecv.at[t], partner))
        for copy in copies:
            copy.start()
        for copy in copies:
            copy.wait()

    def to_partner(j):
        ref = q_all.at[chip, core * 4 + j]
        return send(ref, ref, psend.at[j], precv.at[j], partner)

    def to_across(j):
        ref = q_all.at[chip, core * 4 + j]
        return send(ref, ref, xsend.at[j], xrecv.at[j], across)

    def forward(j):
        ref = q_all.at[1 - chip, core * 4 + j]
        return send(ref, ref, fsend.at[j], frecv.at[j], partner)

    def tile(j, carry):
        pltpu.make_async_copy(wq.at[layer, :, pl.ds(0, TN)], wbuf.at[j], wsem.at[j]).wait()
        q_all[chip, core * 4 + j] = dot(h[...], wbuf[j]).astype(BF16)
        for i in range(4):
            if i + WINDOW < 6:
                pl.when(j == i)(lambda i=i: fetch(i + WINDOW).start())

        @pl.when(j > 0)
        def _():
            to_across(j - 1).start()
            to_partner(j - 1).start()
        return carry

    lax.fori_loop(0, 4, tile, 0)
    for j in range(4, 6):
        fetch(j).wait()
        kv[:, (j - 4) * TN:(j - 3) * TN] = dot(h[...], wbuf[j]).astype(BF16)
        if j == 4:
            to_across(3).start()
            to_partner(3).start()
    for j in range(4):
        to_across(j).wait_recv()
        forward(j).start()
    for j in range(4):
        to_across(j).wait_send()
        to_partner(j).wait()
        forward(j).wait()


def run_qkv(layer, h, weights, first):
    wq, wk, wv = weights[:3]
    out_shape = [jax.ShapeDtypeStruct((2, 8, TOK, TN), BF16), jax.ShapeDtypeStruct((TOK, 2 * TN), BF16)]
    if first:
        out_shape.append(jax.ShapeDtypeStruct((TOK, D), BF16))
    scratch = [pltpu.VMEM((6, D, TN), BF16), DMA((6,))] + [DMA((4,))] * 6
    if first:
        scratch += [DMA((2,))] * 2
    return pl.pallas_call(
        functools.partial(qkv_kernel, layer, first),
        name=f'qkv{layer}',
        out_shape=out_shape,
        in_specs=[VMEM, ANY, ANY, ANY],
        out_specs=[VMEM] * len(out_shape),
        scratch_shapes=scratch,
        cost_estimate=pl.CostEstimate(flops=2 * TOK * D * 6 * TN * 8, bytes_accessed=D * 6 * TN * 2, transcendentals=0),
        compiler_params=pltpu.CompilerParams(collective_id=layer, has_side_effects=True, vmem_limit_bytes=VMEM_LIMIT),
    )(h, wq, wk, wv)


def plan_kernel(new_table, seq_lens, mig_src, mig_dst, meta, items, slots, gone, moved, rows, lates, source, place_of, counts):
    me = lax.axis_index('kv')
    base = me * SLOTS

    def home(slot):
        return sum((slot >= i * SLOTS).astype(jnp.int32) for i in range(1, 4))

    def clear(i, carry):
        source[i] = -1
        place_of[i] = -1
        return carry

    lax.fori_loop(0, 4 * SLOTS, clear, 0, unroll=16)
    for i in range(16):
        counts[i] = 0
    for i in range(LATES):
        lates[i] = -1

    def keep(i, carry):
        slots[i] = 0
        return carry

    lax.fori_loop(0, SLOTS, keep, 0, unroll=16)

    def entry(e, carry):
        n, m, even, odd = carry
        s, d = mig_src[e], mig_dst[e]
        hs, hd = home(s), home(d)
        pair = hs * 4 + hd
        rank = counts[pair]
        counts[pair] = rank + 1
        channel = (hs ^ hd) - 1
        place = channel * MIG + rank
        source[d] = s
        place_of[d] = place
        misfit = ((channel == 1) | (rank >= FAST_PAGES)).astype(jnp.int32)
        even = even | misfit | (hs & 1)
        odd = odd | misfit | (1 - (hs & 1))

        slots[jnp.where(hs == me, s - base, SLOTS)] = 1
        slots[jnp.where(hd == me, d - base, SLOTS)] = 1
        gone[m] = s - base
        is_late = (hs == me) & (channel == 2) & (rank >= LATE) & (rank < FAST_PAGES)
        lates[jnp.where(is_late, rank - LATE, LATES)] = s - base
        moved[0, n] = d - base
        moved[1, n] = place
        return n + (hd == me).astype(jnp.int32), m + (hs == me).astype(jnp.int32), even, odd

    zero = jnp.int32(0)
    n_moved, n_gone, even, odd = lax.fori_loop(0, MIG, entry, (zero, zero, zero, zero), unroll=8)

    def sequence(b, carry):
        n, m = carry
        length = seq_lens[b]
        local, own, place = [], [], []
        for j in range(2):
            slot = new_table[j, b]
            src = source[slot]
            old = jnp.where(src >= 0, src, slot) - base
            mine = (old >= 0) & (old < SLOTS)
            local.append(old)
            own.append(mine)
            place.append(jnp.where(mine, place_of[slot], -1))
        items[0, n] = b
        items[1, n] = jnp.where(own[0], local[0], -1)
        items[2, n] = jnp.where(own[1], local[1], -1)
        items[3, n] = jnp.where(own[0], jnp.minimum(length, PAGE), 0)
        items[4, n] = jnp.where(own[1], jnp.maximum(length - PAGE, 0), 0)
        items[5, n] = place[0]
        items[6, n] = place[1]
        for t in range(2):
            pos = length + t
            second = pos >= PAGE
            here = jnp.where(second, new_table[1, b], new_table[0, b]) - base
            rows[0, m] = here
            rows[1, m] = jnp.where(second, pos - PAGE, pos)
            rows[2, m] = (b // 32) * TOK + t * 32 + b % 32
            m = m + ((here >= 0) & (here < SLOTS)).astype(jnp.int32)
        return n + (own[0] | own[1]).astype(jnp.int32), m

    n_items, n_rows = lax.fori_loop(0, SEQS, sequence, (zero, zero), unroll=8)

    @pl.when(n_items > 0)
    def _():
        for i in range(UNROLL - 1):
            for f in range(5):
                items[f, n_items + i] = items[f, n_items - 1]
            for f in range(5, 7):
                items[f, n_items + i] = -1
    meta[0] = n_items
    meta[1] = jnp.where(even == 0, 0, jnp.where(odd == 0, 1, 2))
    meta[2] = n_moved
    meta[3] = n_rows
    meta[4] = n_gone


def run_plan(new_table, seq_lens, mig_src, mig_dst):
    shapes = [(5,), (7, SEQS + UNROLL), (SLOTS + 1,), (MIG + 1,), (2, MIG + 1), (3, 2 * SEQS + 1), (LATES + 1,)]
    return pl.pallas_call(
        plan_kernel,
        name='plan',
        out_shape=[jax.ShapeDtypeStruct(shape, jnp.int32) for shape in shapes],
        in_specs=[SMEM] * 4,
        out_specs=[SMEM] * len(shapes),
        scratch_shapes=[pltpu.SMEM((4 * SLOTS,), jnp.int32), pltpu.SMEM((4 * SLOTS,), jnp.int32), pltpu.SMEM((16,), jnp.int32)],
    )(new_table.T, seq_lens, mig_src, mig_dst)


NBUF = 6
AFTER = 2
DIST = NBUF - AFTER
STEPS = SEQS // UNROLL
SLOTS_STEP = SLOTS // STEPS


def attend_kernel(layer, meta, table, slots, q_all, k_pool, v_pool, *refs):
    if layer == 0:
        lates, part_o, part_l, outbox, pool_out, late_box, *refs, late_buf, late_in, late_out = refs
    else:
        moved, inbox, spare, _, part_o, part_l, outbox, pool_out, k_out, *refs, pages, page_in, page_out = refs
    q_rows, kvbuf, ring, sems, out_sems, ring_in, ring_out = refs
    pool = (k_pool, v_pool)[layer]
    groups = (meta[0] + UNROLL - 1) // UNROLL

    def copies(g, start):
        slot = lax.rem(g, NBUF)
        for u in range(UNROLL):
            for j in range(2):
                page = table[1 + j, g * UNROLL + u]

                @pl.when(page >= 0)
                def _():
                    if start:
                        for p, ref in enumerate((k_pool, v_pool)):
                            pltpu.make_async_copy(ref.at[page, layer], kvbuf.at[slot, u, j, p], sems.at[slot]).start()
                    else:
                        pltpu.make_async_copy(outbox.at[0], kvbuf.at[slot, u, j], sems.at[slot]).wait()

    def packs(g, start):
        slot = lax.rem(g, NBUF)
        for u in range(UNROLL):
            for j in range(2):
                place = table[5 + j, g * UNROLL + u]

                @pl.when(place >= 0)
                def _():
                    copy = pltpu.make_async_copy(kvbuf.at[slot, u, j], outbox.at[place], out_sems.at[slot])
                    copy.start() if start else copy.wait()

    def keep(s, phase):
        place = lax.rem(s, NBUF)
        for i in range(SLOTS_STEP):
            slot = s * SLOTS_STEP + i

            @pl.when(slots[slot] == 0)
            def _():
                if phase < 2:
                    load = pltpu.make_async_copy(pool.at[slot], ring.at[place, i], ring_in.at[place, i])
                    load.wait() if phase else load.start()
                if phase > 0:
                    store = pltpu.make_async_copy(ring.at[place, i], pool_out.at[slot], ring_out.at[place, i])
                    store.start() if phase == 1 else store.wait()

    def settle(phase):
        def one(i, carry):
            place = moved[1, i]
            here = (place < 2 * MIG + LATE) | (meta[1] == 2)

            def move(box):
                for p, dst in enumerate((k_out, pool_out)):
                    if phase < 2:
                        copy = pltpu.make_async_copy(box.at[moved[1, i], p], pages.at[i, p], page_in)
                    else:
                        copy = pltpu.make_async_copy(pages.at[i, p], dst.at[moved[0, i], 0], page_out)
                    copy.wait() if phase % 2 else copy.start()

            if phase:
                pl.when(here)(lambda: move(inbox))
            else:
                pl.when(here & (meta[1] < 2))(lambda: move(inbox))
                pl.when(meta[1] == 2)(lambda: move(spare))
            return carry

        lax.fori_loop(0, meta[2], one, 0)

    def late(phase):
        def one(i, carry):
            @pl.when(lates[i] >= 0)
            def _():
                for l in range(LAYERS):
                    for p, ref in enumerate((k_pool, v_pool)):
                        if phase < 2:
                            copy = pltpu.make_async_copy(ref.at[lates[i], l], late_buf.at[l, i, p], late_in)
                        else:
                            copy = pltpu.make_async_copy(late_buf.at[l, i, p], late_box.at[l, i, p], late_out)
                        copy.wait() if phase % 2 else copy.start()
            return carry

        lax.fori_loop(0, LATES, one, 0)

    if layer == 1:
        settle(0)
    else:
        late(0)
    kvbuf[...] = jnp.zeros_like(kvbuf)
    for g in range(DIST):
        @pl.when(g < groups)
        def _():
            copies(g, True)
        keep(g, 0)
    part_o[...] = jnp.zeros_like(part_o)
    part_l[...] = jnp.full_like(part_l, NEG)

    for chip in range(2):
        for tile in range(8):
            for i in range(4):
                rows = q_all[chip, tile, :, i * HEAD:(i + 1) * HEAD].astype(F32)
                q_rows[pl.ds(chip * TOK * HEADS + tile * 4 + i, TOK, stride=HEADS), :] = rows

    row = lax.broadcasted_iota(jnp.int32, (2 * HEADS, 256), 0)
    col = lax.broadcasted_iota(jnp.int32, (2 * HEADS, 256), 1)
    pos = jnp.where((row % HEADS) // 4 == col % KV_HEADS, col // KV_HEADS, PAGE)

    def attend(g):
        slot = lax.rem(g, NBUF)
        outs = []
        for u in range(UNROLL):
            item = g * UNROLL + u
            seq = table[0, item]
            base = (seq // 32) * TOK * HEADS + (seq % 32) * HEADS
            q0 = q_rows[pl.ds(pl.multiple_of(base, HEADS), HEADS), :]
            q1 = q_rows[pl.ds(pl.multiple_of(base + 32 * HEADS, HEADS), HEADS), :]
            q = jnp.concatenate([q0, q1], axis=0).astype(BF16)
            scores = []
            for j in range(2):
                s = lax.dot_general(q, kvbuf[slot, u, j, 0], (((1,), (1,)), ((), ())), preferred_element_type=F32)
                scores.append(jnp.where(pos < table[3 + j, item], s, NEG))
            top = jnp.max(jnp.maximum(scores[0], scores[1]), axis=1, keepdims=True)
            probs = [jnp.exp2((s - top) * (SCALE * LOG2E)) for s in scores]
            total = jnp.sum(probs[0] + probs[1], axis=1, keepdims=True)
            out = sum(dot(p.astype(BF16), kvbuf[slot, u, j, 1]) for j, p in enumerate(probs))
            live = top > NEG
            lse = jnp.where(live, top * SCALE + jnp.log(total), NEG)
            outs.append((seq, jnp.where(live, out / total, 0.0), jnp.broadcast_to(lse, (2 * HEADS, HEAD))))
        for seq, out, lse in outs:
            for t in range(2):
                for half in range(2):
                    rows = slice(t * HEADS + half * HALF_HEADS, t * HEADS + (half + 1) * HALF_HEADS)
                    part_o[seq // 32, half, t * 32 + seq % 32] = out[rows]
                    part_l[seq // 32, half, t * 32 + seq % 32] = lse[rows]

    def step(g, carry):
        keep(g, 1)

        @pl.when(g == STEPS // 2)
        def _():
            for phase in (1, 2):
                settle(phase) if layer == 1 else late(phase)

        @pl.when(g < groups)
        def _():
            copies(g, False)
            packs(g, True)

        @pl.when(g >= AFTER)
        def _():
            keep(g - AFTER, 2)

        @pl.when((g >= AFTER) & (g - AFTER < groups))
        def _():
            packs(g - AFTER, False)

        @pl.when(g + DIST < STEPS)
        def _():
            keep(g + DIST, 0)

        @pl.when(g + DIST < groups)
        def _():
            copies(g + DIST, True)

        @pl.when(g < groups)
        def _():
            attend(g)
        return carry

    lax.fori_loop(0, STEPS, step, 0)
    for g in range(STEPS - AFTER, STEPS):
        keep(g, 2)

        @pl.when(g < groups)
        def _():
            packs(g, False)
    settle(3) if layer == 1 else late(3)


def run_attend(layer, meta, table, slots, q_all, k_flat, v_flat, *extra):
    shape = jax.ShapeDtypeStruct((2, 2, TOK, HALF_HEADS, HEAD), F32)
    page = (PAGE * KV_HEADS, HEAD)
    late = (LAYERS, LATES, 2) + page
    more = [jax.ShapeDtypeStruct(k_flat.shape if layer else late, BF16)]
    return pl.pallas_call(
        functools.partial(attend_kernel, layer),
        name=f'attend{layer}',
        out_shape=[shape, shape, BOX, jax.ShapeDtypeStruct(k_flat.shape, BF16)] + more,
        in_specs=[SMEM, SMEM, SMEM, VMEM, ANY, ANY, SMEM] + [ANY, ANY, ANY] * layer,
        out_specs=[VMEM, VMEM, ANY, ANY, ANY],
        input_output_aliases={9: 4} if layer else {},
        scratch_shapes=[
            pltpu.VMEM((2 * TOK * HEADS, HEAD), F32),
            pltpu.VMEM((NBUF, UNROLL, 2, 2) + page, BF16),
            pltpu.VMEM((NBUF, SLOTS_STEP) + k_flat.shape[1:], BF16),
            DMA((NBUF,)),
            DMA((NBUF,)),
            DMA((NBUF, SLOTS_STEP)),
            DMA((NBUF, SLOTS_STEP)),
            pltpu.VMEM(((MIG, 2) + page) if layer else late, BF16),
            DMA,
            DMA,
        ],
        cost_estimate=pl.CostEstimate(flops=2 * 10 ** 10, bytes_accessed=16 * 2 ** 20, transcendentals=0),
        compiler_params=pltpu.CompilerParams(vmem_limit_bytes=VMEM_LIMIT),
    )(meta, table, slots, q_all, k_flat, v_flat, *extra)


def merge(parts):
    top = functools.reduce(jnp.maximum, [l for _, l in parts])
    weights = [jnp.exp(l - top) for _, l in parts]
    total = functools.reduce(jnp.add, weights)
    out = functools.reduce(jnp.add, [w * o for w, (o, _) in zip(weights, parts)]) / total
    return out, top + jnp.log(total)


LANES = ([((0,), 2, LATE), ((0,), 0, FAST_PAGES)], [((1,), 2, LATE), ((1,), 0, FAST_PAGES)])
EVERYTHING = [((0, 1), i, MIG) for i in range(3)]
CHUNK = 1


class Boxes:
    def __init__(self, moves, outbox, inbox, send_sems, recv_sems):
        me, chip, self.core, partner, across, diag = places()
        self.peers = (partner, across, diag)
        self.moves, self.outbox, self.inbox, self.send_sems, self.recv_sems = moves, outbox, inbox, send_sems, recv_sems

    def each(self, sending, act):
        for cores, channel, pages in self.moves:
            def run(channel=channel, pages=pages):
                def one(i, carry):
                    rows = pl.ds(channel * MIG + i * CHUNK, CHUNK)
                    act(send(self.outbox.at[rows], self.inbox.at[rows], self.send_sems.at[channel, i], self.recv_sems.at[channel, i], self.peers[channel]))
                    return carry

                lax.fori_loop(0, pages // CHUNK, one, 0)

            if len(cores) == 2:
                run()
            else:
                cross = 0 if channel == 1 else 1
                at = cores[0] if sending else (cores[0] + cross) % 2
                pl.when(self.core == at)(run)

    def start(self):
        self.each(True, lambda copy: copy.start())

    def wait(self):
        self.each(True, lambda copy: copy.wait_send())
        self.each(False, lambda copy: copy.wait_recv())


RING_W = 18
TK = 2048
UP_TILES = FF // 2 // TN
TD = FF // 8
OUT_END = D // TN
UP_END = OUT_END + 2 * UP_TILES
DOWN_END = UP_END + 4 * (D // TN)
QKV_END = DOWN_END + 12
PART = TOK // 2


def rest_kernel(layer, lane_core, h_in, q_all, kv, part_o, part_l, wo, w_up, w_down, outbox, *refs):
    last = layer == LAYERS - 1
    if last:
        out, kv_all, inbox, *refs = refs
    else:
        wq, wk, wv, out, kv_all, inbox, q_next, kv_next, *refs = refs
        *refs, qp_send, qp_recv, qx_send, qx_recv, qf_send, qf_recv = refs
    (ring, ring_sem, own_o, own_l, own_sem, got_o, got_l, mine_o, mine_l, give_o, give_l, far_o, far_l, q_rows, k_rows, v_rows, attn, act, h,
     psend, precv, dsend, drecv, xsend, xrecv, ssem, rsem, ksend, krecv, bsend, brecv) = refs
    me, chip, core, partner, across, diag = places()
    boxes = Boxes(LANES[lane_core], outbox, inbox, bsend, brecv)
    end = DOWN_END if last else QKV_END

    def tile_copy(t, kind):
        slot = lax.rem(t, RING_W)
        if kind == 0:
            src = wo.at[layer, pl.ds(pl.multiple_of(core * TK, TK), TK), pl.ds(pl.multiple_of(t * TN, TN), TN)]
        elif kind == 1:
            i = t - OUT_END
            src = w_up.at[layer, pl.ds(pl.multiple_of(lax.rem(i, 2) * TK, TK), TK), pl.ds(pl.multiple_of(core * (FF // 2) + (i // 2) * TN, TN), TN)]
        elif kind >= 3:
            i = t - DOWN_END
            rows = pl.ds(pl.multiple_of(lax.rem(i, 2) * TK, TK), TK)
            if kind == 3:
                src = wq.at[layer + 1, rows, pl.ds(pl.multiple_of(core * 2048 + (i // 2) * TN, TN), TN)]
            else:
                src = (wk, wv)[kind - 4].at[layer + 1, rows, pl.ds(pl.multiple_of(core * TN, TN), TN)]
        else:
            i = t - UP_END
            src = w_down.at[layer, pl.ds(pl.multiple_of(core * (FF // 2) + lax.rem(i, 4) * TD, TD), TD), pl.ds(pl.multiple_of((i // 4) * TN, TN), TN)]
        dst = ring.at[slot, pl.ds(0, TD)] if kind == 2 else ring.at[slot]
        return pltpu.make_async_copy(src, dst, ring_sem.at[slot])

    def fetch(t):
        pl.when(t < OUT_END)(lambda: tile_copy(t, 0).start())
        pl.when((t >= OUT_END) & (t < UP_END))(lambda: tile_copy(t, 1).start())
        pl.when((t >= UP_END) & (t < DOWN_END))(lambda: tile_copy(t, 2).start())
        if not last:
            pl.when((t >= DOWN_END) & (t < DOWN_END + 8))(lambda: tile_copy(t, 3).start())
            pl.when((t >= DOWN_END + 8) & (t < DOWN_END + 10))(lambda: tile_copy(t, 4).start())
            pl.when((t >= DOWN_END + 10) & (t < QKV_END))(lambda: tile_copy(t, 5).start())

    own, near = [], []
    for which, (owner, first, size) in enumerate(((1 - chip, 0, PART), (1 - chip, PART, PART), (chip, 0, TOK))):
        at = pl.ds(which * PART, size)
        rows = pl.ds(first, size)
        for i, (src, dst) in enumerate(((part_o, own_o), (part_l, own_l))):
            copy = pltpu.make_async_copy(src.at[owner, core, rows], dst.at[at], own_sem.at[which, i])
            copy.start()
            own.append(copy)
        near.append([
            send(part_o.at[owner, 1 - core, rows], got_o.at[at], dsend.at[which, 0], drecv.at[which, 0], partner),
            send(part_l.at[owner, 1 - core, rows], got_l.at[at], dsend.at[which, 1], drecv.at[which, 1], partner),
        ])
    meet((partner, across, diag))
    for pair in near:
        for copy in pair:
            copy.start()
    lax.fori_loop(0, RING_W, lambda t, carry: (fetch(t), carry)[1], 0)

    lane = lax.broadcasted_iota(jnp.int32, (8, HEAD), 1)
    far = []
    for part in range(2):
        for copy in own[2 * part:2 * part + 2]:
            copy.wait()
        for copy in near[part]:
            copy.wait_recv()

        def chip_merge(i, compact, part=part):
            j = part * PART + i
            o, l = merge([(own_o[j], own_l[j]), (got_o[j], got_l[j])])
            give_o[j] = o
            compact = jnp.where(lane == 2 * i, l[:8], compact)
            return jnp.where(lane == 2 * i + 1, l[8:], compact)

        give_l[part] = lax.fori_loop(0, PART, chip_merge, jnp.zeros((8, HEAD), F32), unroll=4)
        rows = pl.ds(part * PART, PART)
        pair = [
            send(give_l.at[part], far_l.at[part], xsend.at[part, 0], xrecv.at[part, 0], across),
            send(give_o.at[rows], far_o.at[rows], xsend.at[part, 1], xrecv.at[part, 1], across),
        ]
        for copy in pair:
            copy.start()
        far.append(pair)

    kv_all[me] = kv[...]
    new_rows = [send(kv, kv_all.at[me], ksend.at[i], krecv.at[i], peer) for i, peer in enumerate((partner, across))]
    new_rows.append(send(kv_all.at[across], kv_all.at[across], ksend.at[2], krecv.at[2], partner))

    for head in range(HALF_HEADS):
        tile = core * 4 + head // 4
        rows = pl.ds(head, TOK, stride=HALF_HEADS)
        q_rows[rows, :] = q_all[chip, tile, :, (head % 4) * HEAD:(head % 4 + 1) * HEAD].astype(F32)
        k_rows[rows, :] = kv[:, (head // 4) * HEAD:(head // 4 + 1) * HEAD].astype(F32)
        v_rows[rows, :] = kv[:, TN + (head // 4) * HEAD:TN + (head // 4 + 1) * HEAD].astype(F32)
    for copy in own[4:]:
        copy.wait()
    for copy in near[2]:
        copy.wait_recv()

    half = ROWS // 2

    def score(q, k):
        s = jnp.sum(q * k, axis=1, keepdims=True) * SCALE
        return jnp.broadcast_to(s, q.shape)

    def own_merge(i, carry):
        a = pl.ds(pl.multiple_of(i * HALF_HEADS, HALF_HEADS), HALF_HEADS)
        b = pl.ds(pl.multiple_of(half + i * HALF_HEADS, HALF_HEADS), HALF_HEADS)
        k0, v0, k1, v1 = k_rows[a, :], v_rows[a, :], k_rows[b, :], v_rows[b, :]
        q0, q1 = q_rows[a, :], q_rows[b, :]
        j = i + PART
        m, n = TOK + i, TOK + j
        o, l = merge([(own_o[m], own_l[m]), (got_o[m], got_l[m]), (v0, score(q0, k0))])
        mine_o[i] = o
        mine_l[i] = l
        o, l = merge([(own_o[n], own_l[n]), (got_o[n], got_l[n]), (v0, score(q1, k0)), (v1, score(q1, k1))])
        mine_o[j] = o
        mine_l[j] = l
        return carry

    lax.fori_loop(0, PART, own_merge, 0, unroll=2)

    for part in range(2):
        for copy in far[part]:
            copy.wait_recv()
        if part == 1:
            for copy in new_rows[:2]:
                copy.start()
            boxes.start()
        spread = far_l[part]

        def last_merge(i, carry, part=part, spread=spread):
            l = jnp.concatenate([
                jnp.broadcast_to(jnp.sum(jnp.where(lane == 2 * i + k, spread, 0.0), axis=1, keepdims=True), (8, HEAD)) for k in range(2)
            ], axis=0)
            j = part * PART + i
            o, _ = merge([(mine_o[j], mine_l[j]), (far_o[j], l)])
            q_rows[pl.ds(pl.multiple_of(j * HALF_HEADS, HALF_HEADS), HALF_HEADS), :] = o
            return carry

        lax.fori_loop(0, PART, last_merge, 0, unroll=4)
    for head in range(HALF_HEADS):
        attn[:, head * HEAD:(head + 1) * HEAD] = q_rows[pl.ds(head, TOK, stride=HALF_HEADS), :].astype(BF16)

    def reduce(j):
        return send(psend.at[j], precv.at[j], ssem.at[j], rsem.at[j], partner)

    def finish_sum(first, res, target):
        reduce(first + 7).start()
        for j in range(8):
            reduce(first + j).wait_recv()
            cols = slice(j * TN, (j + 1) * TN)
            target[:, cols] = (res[:, cols].astype(F32) + (psend[first + j] + precv[first + j])).astype(BF16)

    def project(j, carry):
        tile_copy(j, 0).wait()
        psend[j] = dot(attn[...], ring[lax.rem(j, RING_W)])
        fetch(j + RING_W)

        @pl.when(j > 0)
        def _():
            reduce(j - 1).start()
        return carry

    lax.fori_loop(0, OUT_END, project, 0)
    finish_sum(0, h_in, h)

    def up(s, carry):
        u = None
        for k in range(2):
            t = OUT_END + 2 * s + k
            tile_copy(t, 1).wait()
            part = dot(h[:, k * TK:(k + 1) * TK], ring[lax.rem(t, RING_W)])
            u = part if u is None else u + part
            fetch(t + RING_W)
        a = jax.nn.gelu(u.astype(BF16).astype(F32), approximate=True).astype(BF16)
        act[:, pl.ds(pl.multiple_of(s * TN, TN), TN)] = a
        return carry

    lax.fori_loop(0, UP_TILES, up, 0)
    new_rows[1].wait_recv()
    new_rows[2].start()

    def down(j, carry):
        total = None
        for k in range(4):
            t = UP_END + 4 * j + k
            tile_copy(t, 2).wait()
            part = dot(act[:, k * TD:(k + 1) * TD], ring[lax.rem(t, RING_W), :TD])
            total = part if total is None else total + part
            fetch(t + RING_W)
        psend[8 + j] = total

        @pl.when(j > 0)
        def _():
            reduce(8 + j - 1).start()
        return carry

    lax.fori_loop(0, D // TN, down, 0)
    finish_sum(8, h, out)

    if not last:
        def to_partner(j):
            ref = q_next.at[chip, core * 4 + j]
            return send(ref, ref, qp_send.at[j], qp_recv.at[j], partner)

        def to_across(j):
            ref = q_next.at[chip, core * 4 + j]
            return send(ref, ref, qx_send.at[j], qx_recv.at[j], across)

        def forward(j):
            ref = q_next.at[1 - chip, core * 4 + j]
            return send(ref, ref, qf_send.at[j], qf_recv.at[j], partner)

        def project_next(j, carry):
            total = None
            for k in range(2):
                t = DOWN_END + 2 * j + k
                tile_copy(t, 4).wait()
                part = dot(out[:, k * TK:(k + 1) * TK], ring[lax.rem(t, RING_W)])
                total = part if total is None else total + part
            tile = total.astype(BF16)

            @pl.when(j < 4)
            def _():
                q_next[chip, core * 4 + j] = tile

            @pl.when(j >= 4)
            def _():
                kv_next[:, pl.ds(pl.multiple_of((j - 4) * TN, TN), TN)] = tile

            @pl.when((j > 0) & (j < 5))
            def _():
                to_across(j - 1).start()
                to_partner(j - 1).start()
            return carry

        lax.fori_loop(0, 6, project_next, 0)
        for j in range(4):
            to_across(j).wait_recv()
            forward(j).start()
        for j in range(4):
            to_across(j).wait_send()
            to_partner(j).wait()
            forward(j).wait()
    for j in range(16):
        reduce(j).wait_send()
    for pair in near + far:
        for copy in pair:
            copy.wait_send()
    new_rows[0].wait()
    new_rows[1].wait_send()
    new_rows[2].wait()
    boxes.wait()


def run_rest(layer, lane_core, h, q_all, kv, part_o, part_l, outbox, w_out, w_up, w_down, *weights):
    more = [jax.ShapeDtypeStruct((2, 8, TOK, TN), BF16), jax.ShapeDtypeStruct((TOK, 2 * TN), BF16)] if weights else []
    token = (HALF_HEADS, HEAD)
    return pl.pallas_call(
        functools.partial(rest_kernel, layer, lane_core),
        name=f'rest{layer}_{lane_core}',
        out_shape=[jax.ShapeDtypeStruct((TOK, D), BF16), jax.ShapeDtypeStruct((4, TOK, 2 * TN), BF16), BOX] + more,
        in_specs=[VMEM] * 3 + [ANY] * (6 + len(weights)),
        out_specs=[VMEM, VMEM, ANY] + [VMEM] * len(more),
        scratch_shapes=[
            pltpu.VMEM((RING_W, TK, TN), BF16),
            DMA((RING_W,)),
            pltpu.VMEM((2 * TOK,) + token, F32),
            pltpu.VMEM((2 * TOK,) + token, F32),
            DMA((3, 2)),
            pltpu.VMEM((2 * TOK,) + token, F32),
            pltpu.VMEM((2 * TOK,) + token, F32),
            pltpu.VMEM((TOK,) + token, F32),
            pltpu.VMEM((TOK,) + token, F32),
            pltpu.VMEM((TOK,) + token, F32),
            pltpu.VMEM((2, 8, HEAD), F32),
            pltpu.VMEM((TOK,) + token, F32),
            pltpu.VMEM((2, 8, HEAD), F32),
            pltpu.VMEM((ROWS, HEAD), F32),
            pltpu.VMEM((ROWS, HEAD), F32),
            pltpu.VMEM((ROWS, HEAD), F32),
            pltpu.VMEM((TOK, 2048), BF16),
            pltpu.VMEM((TOK, FF // 2), BF16),
            pltpu.VMEM((TOK, D), BF16),
            pltpu.VMEM((16, TOK, TN), F32),
            pltpu.VMEM((16, TOK, TN), F32),
            DMA((3, 2)),
            DMA((3, 2)),
            DMA((2, 2)),
            DMA((2, 2)),
            DMA((16,)),
            DMA((16,)),
            DMA((3,)),
            DMA((3,)),
            DMA((3, MIG // CHUNK)),
            DMA((3, MIG // CHUNK)),
        ] + [DMA((4,))] * (6 if weights else 0),
        cost_estimate=pl.CostEstimate(flops=2 * TOK * D * FF * 8, bytes_accessed=D * FF * 2, transcendentals=0),
        compiler_params=pltpu.CompilerParams(collective_id=2 + layer * 2 + lane_core, has_side_effects=True, vmem_limit_bytes=67043328),
    )(h, q_all, kv, part_o, part_l, w_out, w_up, w_down, outbox, *weights)


def move_kernel(outbox, inbox, send_sems, recv_sems):
    me, chip, core, partner, across, diag = places()
    meet((partner, across, diag))
    boxes = Boxes(EVERYTHING, outbox, inbox, send_sems, recv_sems)
    boxes.start()
    boxes.wait()


def run_move(layer, outbox):
    return pl.pallas_call(
        move_kernel,
        name=f'move{layer}',
        out_shape=BOX,
        in_specs=[ANY],
        out_specs=ANY,
        scratch_shapes=[DMA((3, MIG // CHUNK)), DMA((3, MIG // CHUNK))],
        compiler_params=pltpu.CompilerParams(collective_id=6 + layer, has_side_effects=True),
    )(outbox)


def run_blank(layer):
    return pl.pallas_call(lambda box: None, name=f'blank{layer}', out_shape=BOX, out_specs=ANY)()


RING = 32
AHEAD = RING // 2


def finish_kernel(meta, moved, gone, rows, inbox, spare, late, kv0, kv1, k_in, v_in, k_out, v_out, wide, row_buf, zeros, buf, in_sem, out_sem, zero_sem, row_sem):
    del k_in, v_in
    outs = (k_out, v_out)
    count = meta[2]

    def loop(first, last, body):
        lax.fori_loop(first, last, lambda i, carry: (body(i), carry)[1], 0)

    def clear(i):
        return [pltpu.make_async_copy(zeros, out.at[gone[i]], zero_sem) for out in outs]

    def is_late(i):
        return (moved[1, i] >= 2 * MIG + LATE) & (meta[1] < 2)

    def load(i, box):
        slot = lax.rem(i, RING)
        return [pltpu.make_async_copy(box.at[moved[1, i], p], buf.at[slot, 1, p], in_sem.at[slot, 1, p]) for p in range(2)]

    def load_late(i):
        slot = lax.rem(i, RING)
        rank = moved[1, i] - (2 * MIG + LATE)
        return [pltpu.make_async_copy(late.at[l, rank, p], buf.at[slot, l, p], in_sem.at[slot, l, p]) for l in range(LAYERS) for p in range(2)]

    def store(i, layers):
        slot = lax.rem(i, RING)
        return [pltpu.make_async_copy(buf.at[slot, l, p], outs[p].at[moved[0, i], l], out_sem.at[slot, l, p]) for l in layers for p in range(2)]

    def begin(group):
        for copy in group:
            copy.start()

    def end(group):
        for copy in group:
            copy.wait()

    def begin_load(i):
        pl.when((meta[1] < 2) & jnp.logical_not(is_late(i)))(lambda: begin(load(i, inbox)))
        pl.when(is_late(i))(lambda: begin(load_late(i)))
        pl.when(meta[1] == 2)(lambda: begin(load(i, spare)))

    def begin_store(i):
        @pl.when(is_late(i))
        def _():
            end(load_late(i))
            begin(store(i, (0, 1)))

        @pl.when(jnp.logical_not(is_late(i)))
        def _():
            end(load(i, inbox))
            begin(store(i, (1,)))

    def end_store(i):
        pl.when(is_late(i))(lambda: end(store(i, (0, 1))))
        pl.when(jnp.logical_not(is_late(i)))(lambda: end(store(i, (1,))))

    loop(0, jnp.minimum(count, AHEAD), begin_load)
    zeros[...] = jnp.zeros_like(zeros)
    loop(0, meta[4], lambda i: begin(clear(i)))

    for l, kv in enumerate((kv0, kv1)):
        for p in range(2):
            for dev in range(4):
                for i in range(4):
                    at = pl.ds((dev // 2) * TOK * KV_HEADS + (dev % 2) * 4 + i, TOK, stride=KV_HEADS)
                    wide[at, :] = kv[dev, :, (p * 4 + i) * HEAD:(p * 4 + i + 1) * HEAD].astype(F32)
            row_buf[p, l] = wide[...].astype(BF16)

    def page(i):
        begin_store(i)

        @pl.when(i + AHEAD < count)
        def _():
            pl.when(i >= AHEAD)(lambda: end_store(i - AHEAD))
            begin_load(i + AHEAD)

    loop(0, count, page)
    loop(jnp.maximum(count - RING, 0), count, end_store)

    def row(i):
        at = pl.ds(pl.multiple_of(rows[1, i] * KV_HEADS, KV_HEADS), KV_HEADS)
        src = pl.ds(pl.multiple_of(rows[2, i] * KV_HEADS, KV_HEADS), KV_HEADS)
        return [pltpu.make_async_copy(row_buf.at[p, l, src, :], outs[p].at[rows[0, i], l, at, :], row_sem.at[p, l]) for p in range(2) for l in range(LAYERS)]

    loop(0, meta[3], lambda i: begin(row(i)))
    loop(0, meta[3], lambda i: end(row(i)))
    loop(0, meta[4], lambda i: end(clear(i)))


def run_finish(meta, moved, gone, rows, boxes, kvs, k_part, v_part):
    shape = jax.ShapeDtypeStruct(k_part.shape, BF16)
    return pl.pallas_call(
        finish_kernel,
        name='finish',
        out_shape=[shape, shape],
        in_specs=[SMEM] * 4 + [ANY, ANY, ANY, VMEM, VMEM, ANY, ANY],
        out_specs=[ANY, ANY],
        scratch_shapes=[
            pltpu.VMEM((2 * TOK * KV_HEADS, HEAD), F32),
            pltpu.VMEM((2, LAYERS, 2 * TOK * KV_HEADS, HEAD), BF16),
            pltpu.VMEM(k_part.shape[1:], BF16),
            pltpu.VMEM((RING,) + (LAYERS, 2) + k_part.shape[2:], BF16),
            DMA((RING, LAYERS, 2)),
            DMA((RING, LAYERS, 2)),
            DMA,
            DMA((2, LAYERS)),
        ],
        input_output_aliases={9: 0, 10: 1},
        cost_estimate=pl.CostEstimate(flops=10 ** 10, bytes_accessed=16 * 2 ** 20, transcendentals=0),
        compiler_params=pltpu.CompilerParams(vmem_limit_bytes=VMEM_LIMIT),
    )(meta, moved, gone, rows, *boxes, *kvs, k_part, v_part)


def solution(mesh):
    pool_spec = P(('rep', 'kv'))
    tok_spec = P(None, ('rep', 'kv'), None)

    def device_fn(embeds, w_query, w_key, w_value, w_out, w_up, w_down, k_pool, v_pool, new_table, seq_lens, mig_src, mig_dst):
        me = lax.axis_index('kv')
        weights = (w_query, w_key, w_value)
        k_flat, v_flat = flat_pool(k_pool), flat_pool(v_pool)
        meta, items, slots, gone, moved, where, lates = run_plan(new_table, seq_lens, mig_src, mig_dst)
        q_all, kv, h = run_qkv(0, embeds, weights, True)
        part_o, part_l, outbox, k_kept, late_box = run_attend(0, meta, items, slots, q_all, k_flat, v_flat, lates)

        def extra_boxes(layer, outbox):
            return lax.cond(meta[1] == 2, functools.partial(run_move, layer), lambda box: run_blank(layer), outbox)

        def layers(core, h, q_all, kv, part_o, part_l, outbox, late_box, k_kept):
            h, kv_all0, inbox, q_all, kv = run_rest(0, core, h, q_all, kv, part_o, part_l, outbox, w_out, w_up, w_down, *weights)
            spare = extra_boxes(0, outbox)
            late_box, q_all = lax.optimization_barrier((late_box, q_all))
            late = lax.ppermute(late_box, 'kv', [(core, 3 - core), (2 + core, 1 - core)])
            part_o, part_l, outbox, v_kept, k_kept = run_attend(1, meta, items, slots, q_all, k_flat, v_flat, moved, inbox, spare, k_kept)
            h, kv_all1, inbox = run_rest(1, core, h, q_all, kv, part_o, part_l, outbox, w_out, w_up, w_down)
            return h, kv_all0, kv_all1, inbox, extra_boxes(1, outbox), late, k_kept, v_kept

        forms = [functools.partial(layers, core) for core in range(2)]
        h, kv_all0, kv_all1, inbox, spare, late, k_kept, v_kept = lax.switch(jnp.minimum(meta[1], 1), forms, h, q_all, kv, part_o, part_l, outbox, late_box, k_kept)
        k_out, v_out = run_finish(meta, moved, gone, where, (inbox, spare, late), (kv_all0, kv_all1), k_kept, v_kept)
        k_out, v_out = k_out.reshape(k_pool.shape), v_out.reshape(v_pool.shape)
        y = lax.dynamic_slice_in_dim(h.reshape(2, 32, D), (me % 2) * 16, 16, axis=1)
        return y, k_out, v_out

    return jax.shard_map(device_fn, mesh=mesh, in_specs=(tok_spec, P(), P(), P(), P(), P(), P(), pool_spec, pool_spec, P('rep', None), P('rep'), P('rep'), P('rep')), out_specs=(tok_spec, pool_spec, pool_spec), check_vma=False)
```

```python
import functools

import jax
import jax.numpy as jnp
from jax import lax
from jax.experimental import pallas as pl
from jax.experimental.pallas import tpu as pltpu
from jax.sharding import PartitionSpec as P

BF16 = jnp.bfloat16
F32 = jnp.float32
MESH = pl.DeviceIdType.MESH
NEG = -3.0e38
VMEM_LIMIT = 60 * 1024 * 1024

D = 4096
HEADS = 32
KV_HEADS = 8
HEAD = 128
FF = 14336
PAGE = 32
LAYERS = 2
SEQS = 64
MIG = 64
TOK = 64
HALF_HEADS = HEADS // 2
ROWS = TOK * HALF_HEADS
TN = 512
SCALE = HEAD ** -0.5
LOG2E = 1.4426950408889634
SLOTS = 96
UNROLL = 4
FAST_PAGES = 32
LATE = 23
LATES = FAST_PAGES - LATE
BOX = jax.ShapeDtypeStruct((3 * MIG, 2, PAGE * KV_HEADS, HEAD), BF16)


def flat_pool(pool):
    return pool.reshape(pool.shape[0], LAYERS, PAGE * KV_HEADS, HEAD)


def dot(a, b):
    return jnp.dot(a, b, preferred_element_type=F32)


def places():
    me = lax.axis_index('kv')
    core = lax.rem(me, 2)
    chip = me // 2
    partner = me + 1 - 2 * core
    across = lax.rem(me + 2, 4)
    diag = lax.rem(partner + 2, 4)
    return me, chip, core, partner, across, diag


def meet(peers):
    barrier = pltpu.get_barrier_semaphore()
    for peer in peers:
        pl.semaphore_signal(barrier, inc=1, device_id={'kv': peer}, device_id_type=MESH)
    pl.semaphore_wait(barrier, len(peers))


def send(src, dst, send_sem, recv_sem, peer):
    return pltpu.make_async_remote_copy(src_ref=src, dst_ref=dst, send_sem=send_sem, recv_sem=recv_sem, device_id={'kv': peer}, device_id_type=MESH)


VMEM = pl.BlockSpec(memory_space=pltpu.VMEM)
SMEM = pl.BlockSpec(memory_space=pltpu.SMEM)
ANY = pl.BlockSpec(memory_space=pl.ANY)
DMA = pltpu.SemaphoreType.DMA


WINDOW = 3


def qkv_kernel(layer, first, *refs):
    if first:
        emb, wq, wk, wv, q_all, kv, h, wbuf, wsem, psend, precv, xsend, xrecv, fsend, frecv, hsend, hrecv = refs
    else:
        h, wq, wk, wv, q_all, kv, wbuf, wsem, psend, precv, xsend, xrecv, fsend, frecv = refs
    me, chip, core, partner, across, diag = places()

    def fetch(j):
        if j < 4:
            src = wq.at[layer, :, pl.ds(pl.multiple_of(core * 2048 + j * TN, TN), TN)]
        else:
            src = (wk, wv)[j - 4].at[layer, :, pl.ds(pl.multiple_of(core * TN, TN), TN)]
        return pltpu.make_async_copy(src, wbuf.at[j], wsem.at[j])

    for j in range(WINDOW):
        fetch(j).start()
    meet((partner, across))
    if first:
        copies = []
        for t in range(2):
            rows = pl.ds(pl.multiple_of(t * 32 + core * 16, 16), 16)
            h[rows, :] = emb[t]
            copies.append(send(emb.at[t], h.at[rows, :], hsend.at[t], hrecv.at[t], partner))
        for copy in copies:
            copy.start()
        for copy in copies:
            copy.wait()

    def to_partner(j):
        ref = q_all.at[chip, core * 4 + j]
        return send(ref, ref, psend.at[j], precv.at[j], partner)

    def to_across(j):
        ref = q_all.at[chip, core * 4 + j]
        return send(ref, ref, xsend.at[j], xrecv.at[j], across)

    def forward(j):
        ref = q_all.at[1 - chip, core * 4 + j]
        return send(ref, ref, fsend.at[j], frecv.at[j], partner)

    def tile(j, carry):
        pltpu.make_async_copy(wq.at[layer, :, pl.ds(0, TN)], wbuf.at[j], wsem.at[j]).wait()
        q_all[chip, core * 4 + j] = dot(h[...], wbuf[j]).astype(BF16)
        for i in range(4):
            if i + WINDOW < 6:
                pl.when(j == i)(lambda i=i: fetch(i + WINDOW).start())

        @pl.when(j > 0)
        def _():
            to_across(j - 1).start()
            to_partner(j - 1).start()
        return carry

    lax.fori_loop(0, 4, tile, 0)
    for j in range(4, 6):
        fetch(j).wait()
        kv[:, (j - 4) * TN:(j - 3) * TN] = dot(h[...], wbuf[j]).astype(BF16)
        if j == 4:
            to_across(3).start()
            to_partner(3).start()
    for j in range(4):
        to_across(j).wait_recv()
        forward(j).start()
    for j in range(4):
        to_across(j).wait_send()
        to_partner(j).wait()
        forward(j).wait()


def run_qkv(layer, h, weights, first):
    wq, wk, wv = weights[:3]
    out_shape = [jax.ShapeDtypeStruct((2, 8, TOK, TN), BF16), jax.ShapeDtypeStruct((TOK, 2 * TN), BF16)]
    if first:
        out_shape.append(jax.ShapeDtypeStruct((TOK, D), BF16))
    scratch = [pltpu.VMEM((6, D, TN), BF16), DMA((6,))] + [DMA((4,))] * 6
    if first:
        scratch += [DMA((2,))] * 2
    return pl.pallas_call(
        functools.partial(qkv_kernel, layer, first),
        name=f'qkv{layer}',
        out_shape=out_shape,
        in_specs=[VMEM, ANY, ANY, ANY],
        out_specs=[VMEM] * len(out_shape),
        scratch_shapes=scratch,
        cost_estimate=pl.CostEstimate(flops=2 * TOK * D * 6 * TN * 8, bytes_accessed=D * 6 * TN * 2, transcendentals=0),
        compiler_params=pltpu.CompilerParams(collective_id=layer, has_side_effects=True, vmem_limit_bytes=VMEM_LIMIT),
    )(h, wq, wk, wv)


def plan_kernel(new_table, seq_lens, mig_src, mig_dst, meta, items, slots, gone, moved, rows, lates, lane, general, source, place_of, counts):
    me = lax.axis_index('kv')
    base = me * SLOTS

    def home(slot):
        return sum((slot >= i * SLOTS).astype(jnp.int32) for i in range(1, 4))

    def clear(i, carry):
        source[i] = -1
        place_of[i] = -1
        return carry

    lax.fori_loop(0, 4 * SLOTS, clear, 0, unroll=16)
    for i in range(16):
        counts[i] = 0
    for i in range(LATES):
        lates[i] = -1

    def keep(i, carry):
        slots[i] = 0
        return carry

    lax.fori_loop(0, SLOTS, keep, 0, unroll=16)

    def entry(e, carry):
        n, m, even, odd = carry
        s, d = mig_src[e], mig_dst[e]
        hs, hd = home(s), home(d)
        pair = hs * 4 + hd
        rank = counts[pair]
        counts[pair] = rank + 1
        channel = (hs ^ hd) - 1
        place = channel * MIG + rank
        source[d] = s
        place_of[d] = place
        misfit = ((channel == 1) | (rank >= FAST_PAGES)).astype(jnp.int32)
        even = even | misfit | (hs & 1)
        odd = odd | misfit | (1 - (hs & 1))

        slots[jnp.where(hs == me, s - base, SLOTS)] = 1
        slots[jnp.where(hd == me, d - base, SLOTS)] = 1
        gone[m] = s - base
        is_late = (hs == me) & (channel == 2) & (rank >= LATE) & (rank < FAST_PAGES)
        lates[jnp.where(is_late, rank - LATE, LATES)] = s - base
        moved[0, n] = d - base
        moved[1, n] = place
        return n + (hd == me).astype(jnp.int32), m + (hs == me).astype(jnp.int32), even, odd

    zero = jnp.int32(0)
    n_moved, n_gone, even, odd = lax.fori_loop(0, MIG, entry, (zero, zero, zero, zero), unroll=8)

    def sequence(b, carry):
        n, m = carry
        length = seq_lens[b]
        local, own, place = [], [], []
        for j in range(2):
            slot = new_table[j, b]
            src = source[slot]
            old = jnp.where(src >= 0, src, slot) - base
            mine = (old >= 0) & (old < SLOTS)
            local.append(old)
            own.append(mine)
            place.append(jnp.where(mine, place_of[slot], -1))
        items[0, n] = b
        items[1, n] = jnp.where(own[0], local[0], -1)
        items[2, n] = jnp.where(own[1], local[1], -1)
        items[3, n] = jnp.where(own[0], jnp.minimum(length, PAGE), 0)
        items[4, n] = jnp.where(own[1], jnp.maximum(length - PAGE, 0), 0)
        items[5, n] = place[0]
        items[6, n] = place[1]
        here = new_table[1, b] - base
        rows[0, m] = here
        rows[1, m] = length - PAGE
        rows[2, m] = b
        m = m + ((here >= 0) & (here < SLOTS)).astype(jnp.int32)
        return n + (own[0] | own[1]).astype(jnp.int32), m

    n_items, n_rows = lax.fori_loop(0, SEQS, sequence, (zero, zero), unroll=8)

    @pl.when(n_items > 0)
    def _():
        for i in range(UNROLL - 1):
            for f in range(5):
                items[f, n_items + i] = items[f, n_items - 1]
            for f in range(5, 7):
                items[f, n_items + i] = -1
    meta[0] = n_items
    meta[1] = jnp.where(even == 0, 0, jnp.where(odd == 0, 1, 2))
    lane[0] = jnp.where(even == 0, 0, 1)
    general[0] = jnp.where((even == 0) | (odd == 0), 0, 1)
    meta[2] = n_moved
    meta[3] = n_rows
    meta[4] = n_gone


def run_plan(new_table, seq_lens, mig_src, mig_dst):
    shapes = [(5,), (7, SEQS + UNROLL), (SLOTS + 1,), (MIG + 1,), (2, MIG + 1), (3, SEQS + 1), (LATES + 1,), (1,), (1,)]
    return pl.pallas_call(
        plan_kernel,
        name='plan',
        out_shape=[jax.ShapeDtypeStruct(shape, jnp.int32) for shape in shapes],
        in_specs=[SMEM] * 4,
        out_specs=[SMEM] * len(shapes),
        scratch_shapes=[pltpu.SMEM((4 * SLOTS,), jnp.int32), pltpu.SMEM((4 * SLOTS,), jnp.int32), pltpu.SMEM((16,), jnp.int32)],
    )(new_table.T, seq_lens, mig_src, mig_dst)


NBUF = 6
AFTER = 2
DIST = NBUF - AFTER
STEPS = SEQS // UNROLL
SLOTS_STEP = SLOTS // STEPS


def attend_kernel(layer, meta, table, slots, q_all, k_pool, v_pool, *refs):
    if layer == 0:
        lates, part_o, part_l, outbox, pool_out, late_box, *refs, late_buf, late_in, late_out = refs
    else:
        moved, inbox, spare, _, part_o, part_l, outbox, pool_out, k_out, *refs, pages, page_in, page_out = refs
    q_rows, kvbuf, ring, sems, out_sems, ring_in, ring_out = refs
    pool = (k_pool, v_pool)[layer]
    groups = (meta[0] + UNROLL - 1) // UNROLL

    def copies(g, start):
        slot = lax.rem(g, NBUF)
        for u in range(UNROLL):
            for j in range(2):
                page = table[1 + j, g * UNROLL + u]

                @pl.when(page >= 0)
                def _():
                    if start:
                        for p, ref in enumerate((k_pool, v_pool)):
                            pltpu.make_async_copy(ref.at[page, layer], kvbuf.at[slot, u, j, p], sems.at[slot]).start()
                    else:
                        pltpu.make_async_copy(outbox.at[0], kvbuf.at[slot, u, j], sems.at[slot]).wait()

    def packs(g, start):
        slot = lax.rem(g, NBUF)
        for u in range(UNROLL):
            for j in range(2):
                place = table[5 + j, g * UNROLL + u]

                @pl.when(place >= 0)
                def _():
                    copy = pltpu.make_async_copy(kvbuf.at[slot, u, j], outbox.at[place], out_sems.at[slot])
                    copy.start() if start else copy.wait()

    def keep(s, phase):
        place = lax.rem(s, NBUF)
        for i in range(SLOTS_STEP):
            slot = s * SLOTS_STEP + i

            @pl.when(slots[slot] == 0)
            def _():
                if phase < 2:
                    load = pltpu.make_async_copy(pool.at[slot], ring.at[place, i], ring_in.at[place, i])
                    load.wait() if phase else load.start()
                if phase > 0:
                    store = pltpu.make_async_copy(ring.at[place, i], pool_out.at[slot], ring_out.at[place, i])
                    store.start() if phase == 1 else store.wait()

    def settle(phase):
        def one(i, carry):
            place = moved[1, i]
            here = (place < 2 * MIG + LATE) | (meta[1] == 2)

            def move(box):
                for p, dst in enumerate((k_out, pool_out)):
                    if phase < 2:
                        copy = pltpu.make_async_copy(box.at[moved[1, i], p], pages.at[i, p], page_in)
                    else:
                        copy = pltpu.make_async_copy(pages.at[i, p], dst.at[moved[0, i], 0], page_out)
                    copy.wait() if phase % 2 else copy.start()

            if phase:
                pl.when(here)(lambda: move(inbox))
            else:
                pl.when(here & (meta[1] < 2))(lambda: move(inbox))
                pl.when(meta[1] == 2)(lambda: move(spare))
            return carry

        lax.fori_loop(0, meta[2], one, 0)

    def late(phase):
        def one(i, carry):
            @pl.when(lates[i] >= 0)
            def _():
                if phase == 0:
                    for p, ref in enumerate((k_pool, v_pool)):
                        pltpu.make_async_copy(ref.at[lates[i]], late_buf.at[i, p], late_in).start()
                elif phase == 1:
                    pltpu.make_async_copy(late_box.at[i], late_buf.at[i], late_in).wait()
                else:
                    copy = pltpu.make_async_copy(late_buf.at[i], late_box.at[i], late_out)
                    copy.wait() if phase == 3 else copy.start()
            return carry

        lax.fori_loop(0, LATES, one, 0)

    if layer == 1:
        settle(0)
    else:
        late(0)
    kvbuf[...] = jnp.zeros_like(kvbuf)
    for g in range(DIST):
        @pl.when(g < groups)
        def _():
            copies(g, True)
        keep(g, 0)
    part_o[...] = jnp.zeros_like(part_o)
    part_l[...] = jnp.full_like(part_l, NEG)

    for chip in range(2):
        for tile in range(8):
            for i in range(4):
                rows = q_all[chip, tile, :, i * HEAD:(i + 1) * HEAD].astype(F32)
                q_rows[pl.ds(chip * TOK * HEADS + tile * 4 + i, TOK, stride=HEADS), :] = rows

    row = lax.broadcasted_iota(jnp.int32, (2 * HEADS, 256), 0)
    col = lax.broadcasted_iota(jnp.int32, (2 * HEADS, 256), 1)
    pos = jnp.where((row % HEADS) // 4 == col % KV_HEADS, col // KV_HEADS, PAGE)

    def attend(g):
        slot = lax.rem(g, NBUF)
        outs = []
        for u in range(UNROLL):
            item = g * UNROLL + u
            seq = table[0, item]
            base = (seq // 32) * TOK * HEADS + (seq % 32) * HEADS
            q0 = q_rows[pl.ds(pl.multiple_of(base, HEADS), HEADS), :]
            q1 = q_rows[pl.ds(pl.multiple_of(base + 32 * HEADS, HEADS), HEADS), :]
            q = jnp.concatenate([q0, q1], axis=0).astype(BF16)
            scores = []
            for j in range(2):
                s = lax.dot_general(q, kvbuf[slot, u, j, 0], (((1,), (1,)), ((), ())), preferred_element_type=F32)
                scores.append(jnp.where(pos < table[3 + j, item], s, NEG))
            top = jnp.max(jnp.maximum(scores[0], scores[1]), axis=1, keepdims=True)
            probs = [jnp.exp2((s - top) * (SCALE * LOG2E)) for s in scores]
            total = jnp.sum(probs[0] + probs[1], axis=1, keepdims=True)
            out = sum(dot(p.astype(BF16), kvbuf[slot, u, j, 1]) for j, p in enumerate(probs))
            live = top > NEG
            lse = jnp.where(live, top * SCALE + jnp.log(total), NEG)
            outs.append((seq, jnp.where(live, out / total, 0.0), jnp.broadcast_to(lse, (2 * HEADS, HEAD))))
        for seq, out, lse in outs:
            for t in range(2):
                for half in range(2):
                    rows = slice(t * HEADS + half * HALF_HEADS, t * HEADS + (half + 1) * HALF_HEADS)
                    part_o[seq // 32, half, t * 32 + seq % 32] = out[rows]
                    part_l[seq // 32, half, t * 32 + seq % 32] = lse[rows]

    def step(g, carry):
        keep(g, 1)

        @pl.when(g == STEPS // 2)
        def _():
            for phase in (1, 2):
                settle(phase) if layer == 1 else late(phase)

        @pl.when(g < groups)
        def _():
            copies(g, False)
            packs(g, True)

        @pl.when(g >= AFTER)
        def _():
            keep(g - AFTER, 2)

        @pl.when((g >= AFTER) & (g - AFTER < groups))
        def _():
            packs(g - AFTER, False)

        @pl.when(g + DIST < STEPS)
        def _():
            keep(g + DIST, 0)

        @pl.when(g + DIST < groups)
        def _():
            copies(g + DIST, True)

        @pl.when(g < groups)
        def _():
            attend(g)
        return carry

    lax.fori_loop(0, STEPS, step, 0)
    for g in range(STEPS - AFTER, STEPS):
        keep(g, 2)

        @pl.when(g < groups)
        def _():
            packs(g, False)
    settle(3) if layer == 1 else late(3)


def run_attend(layer, meta, table, slots, q_all, k_flat, v_flat, *extra):
    shape = jax.ShapeDtypeStruct((2, 2, TOK, HALF_HEADS, HEAD), F32)
    page = (PAGE * KV_HEADS, HEAD)
    late = (LATES, 2, LAYERS) + page
    more = [jax.ShapeDtypeStruct(k_flat.shape if layer else late, BF16)]
    return pl.pallas_call(
        functools.partial(attend_kernel, layer),
        name=f'attend{layer}',
        out_shape=[shape, shape, BOX, jax.ShapeDtypeStruct(k_flat.shape, BF16)] + more,
        in_specs=[SMEM, SMEM, SMEM, VMEM, ANY, ANY, SMEM] + [ANY, ANY, ANY] * layer,
        out_specs=[VMEM, VMEM, ANY, ANY, ANY],
        input_output_aliases={9: 4} if layer else {},
        scratch_shapes=[
            pltpu.VMEM((2 * TOK * HEADS, HEAD), F32),
            pltpu.VMEM((NBUF, UNROLL, 2, 2) + page, BF16),
            pltpu.VMEM((NBUF, SLOTS_STEP) + k_flat.shape[1:], BF16),
            DMA((NBUF,)),
            DMA((NBUF,)),
            DMA((NBUF, SLOTS_STEP)),
            DMA((NBUF, SLOTS_STEP)),
            pltpu.VMEM(((MIG, 2) + page) if layer else late, BF16),
            DMA,
            DMA,
        ],
        cost_estimate=pl.CostEstimate(flops=2 * 10 ** 10, bytes_accessed=16 * 2 ** 20, transcendentals=0),
        compiler_params=pltpu.CompilerParams(vmem_limit_bytes=VMEM_LIMIT),
    )(meta, table, slots, q_all, k_flat, v_flat, *extra)


def merge(parts):
    top = functools.reduce(jnp.maximum, [l for _, l in parts])
    weights = [jnp.exp(l - top) for _, l in parts]
    total = functools.reduce(jnp.add, weights)
    out = functools.reduce(jnp.add, [w * o for w, (o, _) in zip(weights, parts)]) / total
    return out, top + jnp.log(total)


LANES = ([((0,), 2, LATE), ((0,), 0, FAST_PAGES)], [((1,), 2, LATE), ((1,), 0, FAST_PAGES)])
EVERYTHING = [((0, 1), i, MIG) for i in range(3)]
CHUNK = 1


class Boxes:
    def __init__(self, moves, outbox, inbox, send_sems, recv_sems):
        me, chip, self.core, partner, across, diag = places()
        self.peers = (partner, across, diag)
        self.moves, self.outbox, self.inbox, self.send_sems, self.recv_sems = moves, outbox, inbox, send_sems, recv_sems

    def each(self, sending, act):
        for cores, channel, pages in self.moves:
            def run(channel=channel, pages=pages):
                def one(i, carry):
                    rows = pl.ds(channel * MIG + i * CHUNK, CHUNK)
                    act(send(self.outbox.at[rows], self.inbox.at[rows], self.send_sems.at[channel, i], self.recv_sems.at[channel, i], self.peers[channel]))
                    return carry

                lax.fori_loop(0, pages // CHUNK, one, 0)

            if len(cores) == 2:
                run()
            else:
                cross = 0 if channel == 1 else 1
                at = cores[0] if sending else (cores[0] + cross) % 2
                pl.when(self.core == at)(run)

    def start(self):
        self.each(True, lambda copy: copy.start())

    def wait(self):
        self.each(True, lambda copy: copy.wait_send())
        self.each(False, lambda copy: copy.wait_recv())


RING_W = 20
SOON = 4
TK = 2048
UP_TILES = FF // 2 // TN
TD = FF // 8
OUT_END = D // TN
UP_END = OUT_END + 2 * UP_TILES
DOWN_END = UP_END + 4 * (D // TN)
QKV_END = DOWN_END + 12
PART = TOK // 2


def rest_kernel(layer, lane_core, h_in, q_all, kv, part_o, part_l, wo, w_up, w_down, outbox, *refs):
    last = layer == LAYERS - 1
    if last:
        out, kv_all, inbox, *refs = refs
    else:
        wq, wk, wv, out, kv_all, inbox, q_next, kv_next, *refs = refs
        *refs, qp_send, qp_recv, qx_send, qx_recv, qf_send, qf_recv = refs
    (ring, ring_sem, own_o, own_l, own_sem, got_o, got_l, mine_o, mine_l, give_o, give_l, far_o, far_l, q_rows, k_rows, v_rows, attn, act, h,
     psend, precv, dsend, drecv, xsend, xrecv, ssem, rsem, ksend, krecv, bsend, brecv) = refs
    me, chip, core, partner, across, diag = places()
    boxes = Boxes(LANES[lane_core], outbox, inbox, bsend, brecv)
    end = DOWN_END if last else QKV_END

    def tile_copy(t, kind):
        slot = lax.rem(t, RING_W)
        if kind == 0:
            src = wo.at[layer, pl.ds(pl.multiple_of(core * TK, TK), TK), pl.ds(pl.multiple_of(t * TN, TN), TN)]
        elif kind == 1:
            i = t - OUT_END
            src = w_up.at[layer, pl.ds(pl.multiple_of(lax.rem(i, 2) * TK, TK), TK), pl.ds(pl.multiple_of(core * (FF // 2) + (i // 2) * TN, TN), TN)]
        elif kind >= 3:
            i = t - DOWN_END
            rows = pl.ds(pl.multiple_of(lax.rem(i, 2) * TK, TK), TK)
            if kind == 3:
                src = wq.at[layer + 1, rows, pl.ds(pl.multiple_of(core * 2048 + (i // 2) * TN, TN), TN)]
            else:
                src = (wk, wv)[kind - 4].at[layer + 1, rows, pl.ds(pl.multiple_of(core * TN, TN), TN)]
        else:
            i = t - UP_END
            src = w_down.at[layer, pl.ds(pl.multiple_of(core * (FF // 2) + lax.rem(i, 4) * TD, TD), TD), pl.ds(pl.multiple_of((i // 4) * TN, TN), TN)]
        dst = ring.at[slot, pl.ds(0, TD)] if kind == 2 else ring.at[slot]
        return pltpu.make_async_copy(src, dst, ring_sem.at[slot])

    def fetch(t):
        pl.when(t < OUT_END)(lambda: tile_copy(t, 0).start())
        pl.when((t >= OUT_END) & (t < UP_END))(lambda: tile_copy(t, 1).start())
        pl.when((t >= UP_END) & (t < DOWN_END))(lambda: tile_copy(t, 2).start())
        if not last:
            pl.when((t >= DOWN_END) & (t < DOWN_END + 8))(lambda: tile_copy(t, 3).start())
            pl.when((t >= DOWN_END + 8) & (t < DOWN_END + 10))(lambda: tile_copy(t, 4).start())
            pl.when((t >= DOWN_END + 10) & (t < QKV_END))(lambda: tile_copy(t, 5).start())

    own, near = [], []
    for which, (owner, first, size) in enumerate(((1 - chip, 0, PART), (1 - chip, PART, PART), (chip, 0, TOK))):
        at = pl.ds(which * PART, size)
        rows = pl.ds(first, size)
        for i, (src, dst) in enumerate(((part_o, own_o), (part_l, own_l))):
            copy = pltpu.make_async_copy(src.at[owner, core, rows], dst.at[at], own_sem.at[which, i])
            copy.start()
            own.append(copy)
        near.append([
            send(part_o.at[owner, 1 - core, rows], got_o.at[at], dsend.at[which, 0], drecv.at[which, 0], partner),
            send(part_l.at[owner, 1 - core, rows], got_l.at[at], dsend.at[which, 1], drecv.at[which, 1], partner),
        ])
    lax.fori_loop(0, SOON, lambda t, carry: (fetch(t), carry)[1], 0)
    meet((partner, across, diag))
    for pair in near:
        for copy in pair:
            copy.start()
    lax.fori_loop(SOON, RING_W, lambda t, carry: (fetch(t), carry)[1], 0)

    lane = lax.broadcasted_iota(jnp.int32, (8, HEAD), 1)
    far = []
    for part in range(2):
        for copy in own[2 * part:2 * part + 2]:
            copy.wait()
        for copy in near[part]:
            copy.wait_recv()

        def chip_merge(i, compact, part=part):
            j = part * PART + i
            o, l = merge([(own_o[j], own_l[j]), (got_o[j], got_l[j])])
            give_o[j] = o
            compact = jnp.where(lane == 2 * i, l[:8], compact)
            return jnp.where(lane == 2 * i + 1, l[8:], compact)

        give_l[part] = lax.fori_loop(0, PART, chip_merge, jnp.zeros((8, HEAD), F32), unroll=4)
        rows = pl.ds(part * PART, PART)
        pair = [
            send(give_l.at[part], far_l.at[part], xsend.at[part, 0], xrecv.at[part, 0], across),
            send(give_o.at[rows], far_o.at[rows], xsend.at[part, 1], xrecv.at[part, 1], across),
        ]
        for copy in pair:
            copy.start()
        far.append(pair)

    kv_all[me] = kv[...]
    new_rows = [send(kv, kv_all.at[me], ksend.at[i], krecv.at[i], peer) for i, peer in enumerate((partner, across))]
    new_rows.append(send(kv_all.at[across], kv_all.at[across], ksend.at[2], krecv.at[2], partner))

    for head in range(HALF_HEADS):
        tile = core * 4 + head // 4
        rows = pl.ds(head, TOK, stride=HALF_HEADS)
        q_rows[rows, :] = q_all[chip, tile, :, (head % 4) * HEAD:(head % 4 + 1) * HEAD].astype(F32)
        k_rows[rows, :] = kv[:, (head // 4) * HEAD:(head // 4 + 1) * HEAD].astype(F32)
        v_rows[rows, :] = kv[:, TN + (head // 4) * HEAD:TN + (head // 4 + 1) * HEAD].astype(F32)
    for copy in own[4:]:
        copy.wait()
    for copy in near[2]:
        copy.wait_recv()

    half = ROWS // 2

    def score(q, k):
        s = jnp.sum(q * k, axis=1, keepdims=True) * SCALE
        return jnp.broadcast_to(s, q.shape)

    def own_merge(i, carry):
        a = pl.ds(pl.multiple_of(i * HALF_HEADS, HALF_HEADS), HALF_HEADS)
        b = pl.ds(pl.multiple_of(half + i * HALF_HEADS, HALF_HEADS), HALF_HEADS)
        k0, v0, k1, v1 = k_rows[a, :], v_rows[a, :], k_rows[b, :], v_rows[b, :]
        q0, q1 = q_rows[a, :], q_rows[b, :]
        j = i + PART
        m, n = TOK + i, TOK + j
        o, l = merge([(own_o[m], own_l[m]), (got_o[m], got_l[m]), (v0, score(q0, k0))])
        mine_o[i] = o
        mine_l[i] = l
        o, l = merge([(own_o[n], own_l[n]), (got_o[n], got_l[n]), (v0, score(q1, k0)), (v1, score(q1, k1))])
        mine_o[j] = o
        mine_l[j] = l
        return carry

    lax.fori_loop(0, PART, own_merge, 0, unroll=2)

    for part in range(2):
        for copy in far[part]:
            copy.wait_recv()
        if part == 1:
            for copy in new_rows[:2]:
                copy.start()
            boxes.start()
        spread = far_l[part]

        def last_merge(i, carry, part=part, spread=spread):
            l = jnp.concatenate([
                jnp.broadcast_to(jnp.sum(jnp.where(lane == 2 * i + k, spread, 0.0), axis=1, keepdims=True), (8, HEAD)) for k in range(2)
            ], axis=0)
            j = part * PART + i
            o, _ = merge([(mine_o[j], mine_l[j]), (far_o[j], l)])
            q_rows[pl.ds(pl.multiple_of(j * HALF_HEADS, HALF_HEADS), HALF_HEADS), :] = o
            return carry

        lax.fori_loop(0, PART, last_merge, 0, unroll=4)
    for head in range(HALF_HEADS):
        attn[:, head * HEAD:(head + 1) * HEAD] = q_rows[pl.ds(head, TOK, stride=HALF_HEADS), :].astype(BF16)

    def reduce(j):
        return send(psend.at[j], precv.at[j], ssem.at[j], rsem.at[j], partner)

    def finish_sum(first, res, target):
        reduce(first + 7).start()
        for j in range(8):
            reduce(first + j).wait_recv()
            cols = slice(j * TN, (j + 1) * TN)
            target[:, cols] = (res[:, cols].astype(F32) + (psend[first + j] + precv[first + j])).astype(BF16)

    def project(j, carry):
        tile_copy(j, 0).wait()
        psend[j] = dot(attn[...], ring[lax.rem(j, RING_W)])
        fetch(j + RING_W)

        @pl.when(j > 0)
        def _():
            reduce(j - 1).start()
        return carry

    lax.fori_loop(0, OUT_END, project, 0)
    finish_sum(0, h_in, h)

    def up(s, carry):
        u = None
        for k in range(2):
            t = OUT_END + 2 * s + k
            tile_copy(t, 1).wait()
            part = dot(h[:, k * TK:(k + 1) * TK], ring[lax.rem(t, RING_W)])
            u = part if u is None else u + part
            fetch(t + RING_W)
        a = jax.nn.gelu(u.astype(BF16).astype(F32), approximate=True).astype(BF16)
        act[:, pl.ds(pl.multiple_of(s * TN, TN), TN)] = a
        return carry

    lax.fori_loop(0, UP_TILES, up, 0)
    new_rows[1].wait_recv()
    new_rows[2].start()

    def down(j, carry):
        total = None
        for k in range(4):
            t = UP_END + 4 * j + k
            tile_copy(t, 2).wait()
            part = dot(act[:, k * TD:(k + 1) * TD], ring[lax.rem(t, RING_W), :TD])
            total = part if total is None else total + part
            fetch(t + RING_W)
        psend[8 + j] = total

        @pl.when(j > 0)
        def _():
            reduce(8 + j - 1).start()
        return carry

    lax.fori_loop(0, D // TN, down, 0)
    finish_sum(8, h, out)

    if not last:
        def to_partner(j):
            ref = q_next.at[chip, core * 4 + j]
            return send(ref, ref, qp_send.at[j], qp_recv.at[j], partner)

        def to_across(j):
            ref = q_next.at[chip, core * 4 + j]
            return send(ref, ref, qx_send.at[j], qx_recv.at[j], across)

        def forward(j):
            ref = q_next.at[1 - chip, core * 4 + j]
            return send(ref, ref, qf_send.at[j], qf_recv.at[j], partner)

        def project_next(j, carry):
            total = None
            for k in range(2):
                t = DOWN_END + 2 * j + k
                tile_copy(t, 4).wait()
                part = dot(out[:, k * TK:(k + 1) * TK], ring[lax.rem(t, RING_W)])
                total = part if total is None else total + part
            tile = total.astype(BF16)

            @pl.when(j < 4)
            def _():
                q_next[chip, core * 4 + j] = tile

            @pl.when(j >= 4)
            def _():
                kv_next[:, pl.ds(pl.multiple_of((j - 4) * TN, TN), TN)] = tile

            @pl.when((j > 0) & (j < 5))
            def _():
                to_across(j - 1).start()
                to_partner(j - 1).start()
            return carry

        lax.fori_loop(0, 6, project_next, 0)
        for j in range(4):
            to_across(j).wait_recv()
            forward(j).start()
        for j in range(4):
            to_across(j).wait_send()
            to_partner(j).wait()
            forward(j).wait()
    for j in range(16):
        reduce(j).wait_send()
    for pair in near + far:
        for copy in pair:
            copy.wait_send()
    new_rows[0].wait()
    new_rows[1].wait_send()
    new_rows[2].wait()
    boxes.wait()


def run_rest(layer, lane_core, h, q_all, kv, part_o, part_l, outbox, w_out, w_up, w_down, *weights):
    more = [jax.ShapeDtypeStruct((2, 8, TOK, TN), BF16), jax.ShapeDtypeStruct((TOK, 2 * TN), BF16)] if weights else []
    token = (HALF_HEADS, HEAD)
    return pl.pallas_call(
        functools.partial(rest_kernel, layer, lane_core),
        name=f'rest{layer}_{lane_core}',
        out_shape=[jax.ShapeDtypeStruct((TOK, D), BF16), jax.ShapeDtypeStruct((4, TOK, 2 * TN), BF16), BOX] + more,
        in_specs=[VMEM] * 3 + [ANY] * (6 + len(weights)),
        out_specs=[VMEM, VMEM, ANY] + [VMEM] * len(more),
        scratch_shapes=[
            pltpu.VMEM((RING_W, TK, TN), BF16),
            DMA((RING_W,)),
            pltpu.VMEM((2 * TOK,) + token, F32),
            pltpu.VMEM((2 * TOK,) + token, F32),
            DMA((3, 2)),
            pltpu.VMEM((2 * TOK,) + token, F32),
            pltpu.VMEM((2 * TOK,) + token, F32),
            pltpu.VMEM((TOK,) + token, F32),
            pltpu.VMEM((TOK,) + token, F32),
            pltpu.VMEM((TOK,) + token, F32),
            pltpu.VMEM((2, 8, HEAD), F32),
            pltpu.VMEM((TOK,) + token, F32),
            pltpu.VMEM((2, 8, HEAD), F32),
            pltpu.VMEM((ROWS, HEAD), F32),
            pltpu.VMEM((ROWS, HEAD), F32),
            pltpu.VMEM((ROWS, HEAD), F32),
            pltpu.VMEM((TOK, 2048), BF16),
            pltpu.VMEM((TOK, FF // 2), BF16),
            pltpu.VMEM((TOK, D), BF16),
            pltpu.VMEM((16, TOK, TN), F32),
            pltpu.VMEM((16, TOK, TN), F32),
            DMA((3, 2)),
            DMA((3, 2)),
            DMA((2, 2)),
            DMA((2, 2)),
            DMA((16,)),
            DMA((16,)),
            DMA((3,)),
            DMA((3,)),
            DMA((3, MIG // CHUNK)),
            DMA((3, MIG // CHUNK)),
        ] + [DMA((4,))] * (6 if weights else 0),
        cost_estimate=pl.CostEstimate(flops=2 * TOK * D * FF * 8, bytes_accessed=D * FF * 2, transcendentals=0),
        compiler_params=pltpu.CompilerParams(collective_id=2 + layer * 2 + lane_core, has_side_effects=True, vmem_limit_bytes=67043328),
    )(h, q_all, kv, part_o, part_l, w_out, w_up, w_down, outbox, *weights)


def move_kernel(outbox, inbox, send_sems, recv_sems):
    me, chip, core, partner, across, diag = places()
    meet((partner, across, diag))
    boxes = Boxes(EVERYTHING, outbox, inbox, send_sems, recv_sems)
    boxes.start()
    boxes.wait()


def run_move(layer, outbox):
    return pl.pallas_call(
        move_kernel,
        name=f'move{layer}',
        out_shape=BOX,
        in_specs=[ANY],
        out_specs=ANY,
        scratch_shapes=[DMA((3, MIG // CHUNK)), DMA((3, MIG // CHUNK))],
        compiler_params=pltpu.CompilerParams(collective_id=6 + layer, has_side_effects=True),
    )(outbox)


def run_blank(layer):
    return pl.pallas_call(lambda box: None, name=f'blank{layer}', out_shape=BOX, out_specs=ANY)()


RING = 32
AHEAD = RING // 2


def finish_kernel(meta, moved, gone, rows, inbox, spare, late, kv0, kv1, k_in, v_in, k_out, v_out, wide, row_buf, zeros, buf, in_sem, out_sem, zero_sem, row_sem):
    del k_in, v_in
    outs = (k_out, v_out)
    count = meta[2]

    def loop(first, last, body):
        lax.fori_loop(first, last, lambda i, carry: (body(i), carry)[1], 0)

    def clear(i):
        return [pltpu.make_async_copy(zeros, out.at[gone[i]], zero_sem) for out in outs]

    def is_late(i):
        return (moved[1, i] >= 2 * MIG + LATE) & (meta[1] < 2)

    def load(i, box):
        slot = lax.rem(i, RING)
        return [pltpu.make_async_copy(box.at[moved[1, i], p], buf.at[slot, p, 1], in_sem.at[slot, p]) for p in range(2)]

    def load_late(i):
        slot = lax.rem(i, RING)
        return [pltpu.make_async_copy(late.at[moved[1, i] - (2 * MIG + LATE), p], buf.at[slot, p], in_sem.at[slot, p]) for p in range(2)]

    def store(i):
        slot = lax.rem(i, RING)
        return [pltpu.make_async_copy(buf.at[slot, p, 1], outs[p].at[moved[0, i], 1], out_sem.at[slot, p]) for p in range(2)]

    def store_late(i):
        slot = lax.rem(i, RING)
        return [pltpu.make_async_copy(buf.at[slot, p], outs[p].at[moved[0, i]], out_sem.at[slot, p]) for p in range(2)]

    def begin(group):
        for copy in group:
            copy.start()

    def end(group):
        for copy in group:
            copy.wait()

    def begin_load(i):
        pl.when((meta[1] < 2) & jnp.logical_not(is_late(i)))(lambda: begin(load(i, inbox)))
        pl.when(is_late(i))(lambda: begin(load_late(i)))
        pl.when(meta[1] == 2)(lambda: begin(load(i, spare)))

    def begin_store(i):
        @pl.when(is_late(i))
        def _():
            end(load_late(i))
            begin(store_late(i))

        @pl.when(jnp.logical_not(is_late(i)))
        def _():
            end(load(i, inbox))
            begin(store(i))

    def end_store(i):
        pl.when(is_late(i))(lambda: end(store_late(i)))
        pl.when(jnp.logical_not(is_late(i)))(lambda: end(store(i)))

    loop(0, jnp.minimum(count, AHEAD), begin_load)
    zeros[...] = jnp.zeros_like(zeros)
    loop(0, meta[4], lambda i: begin(clear(i)))

    for l, kv in enumerate((kv0, kv1)):
        for p in range(2):
            for dev in range(4):
                for i in range(4):
                    for t in range(2):
                        at = pl.ds((dev // 2) * TOK * KV_HEADS + t * KV_HEADS + (dev % 2) * 4 + i, TOK // 2, stride=2 * KV_HEADS)
                        wide[at, :] = kv[dev, t * 32:(t + 1) * 32, (p * 4 + i) * HEAD:(p * 4 + i + 1) * HEAD].astype(F32)
            row_buf[p, l] = wide[...].astype(BF16)

    def page(i):
        begin_store(i)

        @pl.when(i + AHEAD < count)
        def _():
            pl.when(i >= AHEAD)(lambda: end_store(i - AHEAD))
            begin_load(i + AHEAD)

    loop(0, count, page)
    loop(jnp.maximum(count - RING, 0), count, end_store)

    def row(i):
        at = pl.ds(pl.multiple_of(rows[1, i] * KV_HEADS, KV_HEADS), 2 * KV_HEADS)
        src = pl.ds(pl.multiple_of(rows[2, i] * 2 * KV_HEADS, 2 * KV_HEADS), 2 * KV_HEADS)
        return [pltpu.make_async_copy(row_buf.at[p, :, src, :], outs[p].at[rows[0, i], :, at, :], row_sem.at[p]) for p in range(2)]

    loop(0, meta[3], lambda i: begin(row(i)))
    loop(0, meta[3], lambda i: end(row(i)))
    loop(0, meta[4], lambda i: end(clear(i)))


def run_finish(meta, moved, gone, rows, boxes, kvs, k_part, v_part):
    shape = jax.ShapeDtypeStruct(k_part.shape, BF16)
    return pl.pallas_call(
        finish_kernel,
        name='finish',
        out_shape=[shape, shape],
        in_specs=[SMEM] * 4 + [ANY, ANY, ANY, VMEM, VMEM, ANY, ANY],
        out_specs=[ANY, ANY],
        scratch_shapes=[
            pltpu.VMEM((2 * TOK * KV_HEADS, HEAD), F32),
            pltpu.VMEM((2, LAYERS, 2 * TOK * KV_HEADS, HEAD), BF16),
            pltpu.VMEM(k_part.shape[1:], BF16),
            pltpu.VMEM((RING, 2) + k_part.shape[1:], BF16),
            DMA((RING, 2)),
            DMA((RING, 2)),
            DMA,
            DMA((2,)),
        ],
        input_output_aliases={9: 0, 10: 1},
        cost_estimate=pl.CostEstimate(flops=10 ** 10, bytes_accessed=16 * 2 ** 20, transcendentals=0),
        compiler_params=pltpu.CompilerParams(vmem_limit_bytes=VMEM_LIMIT),
    )(meta, moved, gone, rows, *boxes, *kvs, k_part, v_part)


def solution(mesh):
    pool_spec = P(('rep', 'kv'))
    tok_spec = P(None, ('rep', 'kv'), None)

    def device_fn(embeds, w_query, w_key, w_value, w_out, w_up, w_down, k_pool, v_pool, new_table, seq_lens, mig_src, mig_dst):
        me = lax.axis_index('kv')
        weights = (w_query, w_key, w_value)
        k_flat, v_flat = flat_pool(k_pool), flat_pool(v_pool)
        meta, items, slots, gone, moved, where, lates, lane, general = run_plan(new_table, seq_lens, mig_src, mig_dst)
        q_all, kv, h = run_qkv(0, embeds, weights, True)
        part_o, part_l, outbox, k_kept, late_box = run_attend(0, meta, items, slots, q_all, k_flat, v_flat, lates)

        def extra_boxes(layer, outbox):
            return lax.switch(general.reshape(()), [lambda box: run_blank(layer), functools.partial(run_move, layer)], outbox)

        def layers(core, h, q_all, kv, part_o, part_l, outbox, late_box, k_kept):
            h, kv_all0, inbox, q_all, kv = run_rest(0, core, h, q_all, kv, part_o, part_l, outbox, w_out, w_up, w_down, *weights)
            spare = extra_boxes(0, outbox)
            late_box, q_all = lax.optimization_barrier((late_box, q_all))
            late = lax.ppermute(late_box, 'kv', [(core, 3 - core), (2 + core, 1 - core)])
            part_o, part_l, outbox, v_kept, k_kept = run_attend(1, meta, items, slots, q_all, k_flat, v_flat, moved, inbox, spare, k_kept)
            h, kv_all1, inbox = run_rest(1, core, h, q_all, kv, part_o, part_l, outbox, w_out, w_up, w_down)
            return h, kv_all0, kv_all1, inbox, extra_boxes(1, outbox), late, k_kept, v_kept

        forms = [functools.partial(layers, core) for core in range(2)]
        h, kv_all0, kv_all1, inbox, spare, late, k_kept, v_kept = lax.switch(lane.reshape(()), forms, h, q_all, kv, part_o, part_l, outbox, late_box, k_kept)
        k_out, v_out = run_finish(meta, moved, gone, where, (inbox, spare, late), (kv_all0, kv_all1), k_kept, v_kept)
        k_out, v_out = k_out.reshape(k_pool.shape), v_out.reshape(v_pool.shape)
        y = lax.dynamic_slice_in_dim(h.reshape(2, 32, D), (me % 2) * 16, 16, axis=1)
        return y, k_out, v_out

    return jax.shard_map(device_fn, mesh=mesh, in_specs=(tok_spec, P(), P(), P(), P(), P(), P(), pool_spec, pool_spec, P('rep', None), P('rep'), P('rep'), P('rep')), out_specs=(tok_spec, pool_spec, pool_spec), check_vma=False)
```

```python
import functools

import jax
import jax.numpy as jnp
from jax import lax
from jax.experimental import pallas as pl
from jax.experimental.pallas import tpu as pltpu
from jax.sharding import PartitionSpec as P

BF16 = jnp.bfloat16
F32 = jnp.float32
MESH = pl.DeviceIdType.MESH
NEG = -3.0e38
VMEM_LIMIT = 60 * 1024 * 1024

D = 4096
HEADS = 32
KV_HEADS = 8
HEAD = 128
FF = 14336
PAGE = 32
LAYERS = 2
SEQS = 64
MIG = 64
TOK = 64
HALF_HEADS = HEADS // 2
ROWS = TOK * HALF_HEADS
TN = 512
SCALE = HEAD ** -0.5
LOG2E = 1.4426950408889634
SLOTS = 96
UNROLL = 4
FAST_PAGES = 32
LATE = 21
LATES = FAST_PAGES - LATE
BOX = jax.ShapeDtypeStruct((3 * MIG, 2, PAGE * KV_HEADS, HEAD), BF16)


def flat_pool(pool):
    return pool.reshape(pool.shape[0], LAYERS, PAGE * KV_HEADS, HEAD)


def dot(a, b):
    return jnp.dot(a, b, preferred_element_type=F32)


def places():
    me = lax.axis_index('kv')
    core = lax.rem(me, 2)
    chip = me // 2
    partner = me + 1 - 2 * core
    across = lax.rem(me + 2, 4)
    diag = lax.rem(partner + 2, 4)
    return me, chip, core, partner, across, diag


def meet(peers):
    barrier = pltpu.get_barrier_semaphore()
    for peer in peers:
        pl.semaphore_signal(barrier, inc=1, device_id={'kv': peer}, device_id_type=MESH)
    pl.semaphore_wait(barrier, len(peers))


def send(src, dst, send_sem, recv_sem, peer):
    return pltpu.make_async_remote_copy(src_ref=src, dst_ref=dst, send_sem=send_sem, recv_sem=recv_sem, device_id={'kv': peer}, device_id_type=MESH)


VMEM = pl.BlockSpec(memory_space=pltpu.VMEM)
SMEM = pl.BlockSpec(memory_space=pltpu.SMEM)
ANY = pl.BlockSpec(memory_space=pl.ANY)
DMA = pltpu.SemaphoreType.DMA


WINDOW = 3


def qkv_kernel(layer, first, *refs):
    if first:
        emb, wq, wk, wv, q_all, kv, h, wbuf, wsem, psend, precv, xsend, xrecv, fsend, frecv, hsend, hrecv = refs
    else:
        h, wq, wk, wv, q_all, kv, wbuf, wsem, psend, precv, xsend, xrecv, fsend, frecv = refs
    me, chip, core, partner, across, diag = places()

    def fetch(j):
        if j < 4:
            src = wq.at[layer, :, pl.ds(pl.multiple_of(core * 2048 + j * TN, TN), TN)]
        else:
            src = (wk, wv)[j - 4].at[layer, :, pl.ds(pl.multiple_of(core * TN, TN), TN)]
        return pltpu.make_async_copy(src, wbuf.at[j], wsem.at[j])

    for j in range(WINDOW):
        fetch(j).start()
    meet((partner, across))
    if first:
        copies = []
        for t in range(2):
            rows = pl.ds(pl.multiple_of(t * 32 + core * 16, 16), 16)
            h[rows, :] = emb[t]
            copies.append(send(emb.at[t], h.at[rows, :], hsend.at[t], hrecv.at[t], partner))
        for copy in copies:
            copy.start()
        for copy in copies:
            copy.wait()

    def to_partner(j):
        ref = q_all.at[chip, core * 4 + j]
        return send(ref, ref, psend.at[j], precv.at[j], partner)

    def to_across(j):
        ref = q_all.at[chip, core * 4 + j]
        return send(ref, ref, xsend.at[j], xrecv.at[j], across)

    def forward(j):
        ref = q_all.at[1 - chip, core * 4 + j]
        return send(ref, ref, fsend.at[j], frecv.at[j], partner)

    def tile(j, carry):
        pltpu.make_async_copy(wq.at[layer, :, pl.ds(0, TN)], wbuf.at[j], wsem.at[j]).wait()
        q_all[chip, core * 4 + j] = dot(h[...], wbuf[j]).astype(BF16)
        for i in range(4):
            if i + WINDOW < 6:
                pl.when(j == i)(lambda i=i: fetch(i + WINDOW).start())

        to_across(j).start()
        to_partner(j).start()
        return carry

    lax.fori_loop(0, 4, tile, 0)
    for j in range(4, 6):
        fetch(j).wait()
        kv[:, (j - 4) * TN:(j - 3) * TN] = dot(h[...], wbuf[j]).astype(BF16)
    for j in range(4):
        to_across(j).wait_recv()
        forward(j).start()
    for j in range(4):
        to_across(j).wait_send()
        to_partner(j).wait()
        forward(j).wait()


def run_qkv(layer, h, weights, first):
    wq, wk, wv = weights[:3]
    out_shape = [jax.ShapeDtypeStruct((2, 8, TOK, TN), BF16), jax.ShapeDtypeStruct((TOK, 2 * TN), BF16)]
    if first:
        out_shape.append(jax.ShapeDtypeStruct((TOK, D), BF16))
    scratch = [pltpu.VMEM((6, D, TN), BF16), DMA((6,))] + [DMA((4,))] * 6
    if first:
        scratch += [DMA((2,))] * 2
    return pl.pallas_call(
        functools.partial(qkv_kernel, layer, first),
        name=f'qkv{layer}',
        out_shape=out_shape,
        in_specs=[VMEM, ANY, ANY, ANY],
        out_specs=[VMEM] * len(out_shape),
        scratch_shapes=scratch,
        cost_estimate=pl.CostEstimate(flops=2 * TOK * D * 6 * TN * 8, bytes_accessed=D * 6 * TN * 2, transcendentals=0),
        compiler_params=pltpu.CompilerParams(collective_id=layer, has_side_effects=True, vmem_limit_bytes=VMEM_LIMIT),
    )(h, wq, wk, wv)


def plan_kernel(new_table, seq_lens, mig_src, mig_dst, meta, items, slots, gone, moved, rows, lates, lane, general, source, place_of, counts):
    me = lax.axis_index('kv')
    base = me * SLOTS

    def home(slot):
        return sum((slot >= i * SLOTS).astype(jnp.int32) for i in range(1, 4))

    def clear(i, carry):
        source[i] = -1
        place_of[i] = -1
        return carry

    lax.fori_loop(0, 4 * SLOTS, clear, 0, unroll=16)
    for i in range(16):
        counts[i] = 0
    for i in range(LATES):
        lates[i] = -1

    def keep(i, carry):
        slots[i] = 0
        return carry

    lax.fori_loop(0, SLOTS, keep, 0, unroll=16)

    def entry(e, carry):
        n, m, even, odd = carry
        s, d = mig_src[e], mig_dst[e]
        hs, hd = home(s), home(d)
        pair = hs * 4 + hd
        rank = counts[pair]
        counts[pair] = rank + 1
        channel = (hs ^ hd) - 1
        place = channel * MIG + rank
        source[d] = s
        place_of[d] = place
        misfit = ((channel == 1) | (rank >= FAST_PAGES)).astype(jnp.int32)
        even = even | misfit | (hs & 1)
        odd = odd | misfit | (1 - (hs & 1))

        slots[jnp.where(hs == me, s - base, SLOTS)] = 1
        slots[jnp.where(hd == me, d - base, SLOTS)] = 1
        gone[m] = s - base
        is_late = (hs == me) & (channel == 2) & (rank >= LATE) & (rank < FAST_PAGES)
        lates[jnp.where(is_late, rank - LATE, LATES)] = s - base
        moved[0, n] = d - base
        moved[1, n] = place
        return n + (hd == me).astype(jnp.int32), m + (hs == me).astype(jnp.int32), even, odd

    zero = jnp.int32(0)
    n_moved, n_gone, even, odd = lax.fori_loop(0, MIG, entry, (zero, zero, zero, zero), unroll=8)

    def sequence(b, carry):
        n, m = carry
        length = seq_lens[b]
        local, own, place = [], [], []
        for j in range(2):
            slot = new_table[j, b]
            src = source[slot]
            old = jnp.where(src >= 0, src, slot) - base
            mine = (old >= 0) & (old < SLOTS)
            local.append(old)
            own.append(mine)
            place.append(jnp.where(mine, place_of[slot], -1))
        items[0, n] = b
        items[1, n] = jnp.where(own[0], local[0], -1)
        items[2, n] = jnp.where(own[1], local[1], -1)
        items[3, n] = jnp.where(own[0], jnp.minimum(length, PAGE), 0)
        items[4, n] = jnp.where(own[1], jnp.maximum(length - PAGE, 0), 0)
        items[5, n] = place[0]
        items[6, n] = place[1]
        here = new_table[1, b] - base
        rows[0, m] = here
        rows[1, m] = length - PAGE
        rows[2, m] = b
        m = m + ((here >= 0) & (here < SLOTS)).astype(jnp.int32)
        return n + (own[0] | own[1]).astype(jnp.int32), m

    n_items, n_rows = lax.fori_loop(0, SEQS, sequence, (zero, zero), unroll=8)

    @pl.when(n_items > 0)
    def _():
        for i in range(UNROLL - 1):
            for f in range(5):
                items[f, n_items + i] = items[f, n_items - 1]
            for f in range(5, 7):
                items[f, n_items + i] = -1
    meta[0] = n_items
    meta[1] = jnp.where(even == 0, 0, jnp.where(odd == 0, 1, 2))
    lane[0] = jnp.where(even == 0, 0, 1)
    general[0] = jnp.where((even == 0) | (odd == 0), 0, 1)
    meta[2] = n_moved
    meta[3] = n_rows
    meta[4] = n_gone


def run_plan(new_table, seq_lens, mig_src, mig_dst):
    shapes = [(5,), (7, SEQS + UNROLL), (SLOTS + 1,), (MIG + 1,), (2, MIG + 1), (3, SEQS + 1), (LATES + 1,), (1,), (1,)]
    return pl.pallas_call(
        plan_kernel,
        name='plan',
        out_shape=[jax.ShapeDtypeStruct(shape, jnp.int32) for shape in shapes],
        in_specs=[SMEM] * 4,
        out_specs=[SMEM] * len(shapes),
        scratch_shapes=[pltpu.SMEM((4 * SLOTS,), jnp.int32), pltpu.SMEM((4 * SLOTS,), jnp.int32), pltpu.SMEM((16,), jnp.int32)],
    )(new_table.T, seq_lens, mig_src, mig_dst)


NBUF = 4
AFTER = 1
DIST = NBUF - AFTER
STEPS = SEQS // UNROLL
SLOTS_STEP = SLOTS // STEPS


def attend_kernel(layer, meta, table, slots, q_all, k_pool, v_pool, *refs):
    if layer == 0:
        lates, part_o, part_l, outbox, pool_out, late_box, *refs, late_buf, late_in, late_out = refs
    else:
        moved, inbox, spare, _, part_o, part_l, outbox, pool_out, k_out, *refs, pages, page_in, page_out = refs
    q_rows, kvbuf, ring, sems, out_sems, ring_in, ring_out = refs
    pool = (k_pool, v_pool)[layer]
    groups = (meta[0] + UNROLL - 1) // UNROLL

    def copies(g, start):
        slot = lax.rem(g, NBUF)
        for u in range(UNROLL):
            for j in range(2):
                page = table[1 + j, g * UNROLL + u]

                @pl.when(page >= 0)
                def _():
                    if start:
                        for p, ref in enumerate((k_pool, v_pool)):
                            pltpu.make_async_copy(ref.at[page, layer], kvbuf.at[slot, u, j, p], sems.at[slot]).start()
                    else:
                        pltpu.make_async_copy(outbox.at[0], kvbuf.at[slot, u, j], sems.at[slot]).wait()

    def packs(g, start):
        slot = lax.rem(g, NBUF)
        for u in range(UNROLL):
            for j in range(2):
                place = table[5 + j, g * UNROLL + u]

                @pl.when(place >= 0)
                def _():
                    copy = pltpu.make_async_copy(kvbuf.at[slot, u, j], outbox.at[place], out_sems.at[slot])
                    copy.start() if start else copy.wait()

    def keep(s, phase):
        place = lax.rem(s, NBUF)
        for i in range(SLOTS_STEP):
            slot = s * SLOTS_STEP + i

            @pl.when(slots[slot] == 0)
            def _():
                if phase < 2:
                    load = pltpu.make_async_copy(pool.at[slot], ring.at[place, i], ring_in.at[place, i])
                    load.wait() if phase else load.start()
                if phase > 0:
                    store = pltpu.make_async_copy(ring.at[place, i], pool_out.at[slot], ring_out.at[place, i])
                    store.start() if phase == 1 else store.wait()

    def settle(phase):
        def one(i, carry):
            place = moved[1, i]
            here = (place < 2 * MIG + LATE) | (meta[1] == 2)

            def move(box):
                for p, dst in enumerate((k_out, pool_out)):
                    if phase < 2:
                        copy = pltpu.make_async_copy(box.at[moved[1, i], p], pages.at[i, p], page_in)
                    else:
                        copy = pltpu.make_async_copy(pages.at[i, p], dst.at[moved[0, i], 0], page_out)
                    copy.wait() if phase % 2 else copy.start()

            if phase:
                pl.when(here)(lambda: move(inbox))
            else:
                pl.when(here & (meta[1] < 2))(lambda: move(inbox))
                pl.when(meta[1] == 2)(lambda: move(spare))
            return carry

        lax.fori_loop(0, meta[2], one, 0)

    def late(phase):
        def one(i, carry):
            @pl.when(lates[i] >= 0)
            def _():
                if phase == 0:
                    for p, ref in enumerate((k_pool, v_pool)):
                        pltpu.make_async_copy(ref.at[lates[i]], late_buf.at[i, p], late_in).start()
                elif phase == 1:
                    pltpu.make_async_copy(late_box.at[i], late_buf.at[i], late_in).wait()
                else:
                    copy = pltpu.make_async_copy(late_buf.at[i], late_box.at[i], late_out)
                    copy.wait() if phase == 3 else copy.start()
            return carry

        lax.fori_loop(0, LATES, one, 0)

    if layer == 1:
        settle(0)
    else:
        late(0)
    kvbuf[:, :, :, 1] = jnp.zeros((NBUF, UNROLL, 2) + kvbuf.shape[4:], BF16)
    for g in range(DIST):
        @pl.when(g < groups)
        def _():
            copies(g, True)
        keep(g, 0)
    part_o[...] = jnp.zeros_like(part_o)
    part_l[...] = jnp.full_like(part_l, NEG)

    for chip in range(2):
        for tile in range(8):
            for i in range(4):
                rows = q_all[chip, tile, :, i * HEAD:(i + 1) * HEAD].astype(F32)
                q_rows[pl.ds(chip * TOK * HEADS + tile * 4 + i, TOK, stride=HEADS), :] = rows

    row = lax.broadcasted_iota(jnp.int32, (2 * HEADS, 256), 0)
    col = lax.broadcasted_iota(jnp.int32, (2 * HEADS, 256), 1)
    pos = jnp.where((row % HEADS) // 4 == col % KV_HEADS, col // KV_HEADS, PAGE)

    def attend(g):
        slot = lax.rem(g, NBUF)
        outs = []
        for u in range(UNROLL):
            item = g * UNROLL + u
            seq = table[0, item]
            base = (seq // 32) * TOK * HEADS + (seq % 32) * HEADS
            q0 = q_rows[pl.ds(pl.multiple_of(base, HEADS), HEADS), :]
            q1 = q_rows[pl.ds(pl.multiple_of(base + 32 * HEADS, HEADS), HEADS), :]
            q = jnp.concatenate([q0, q1], axis=0).astype(BF16)
            scores = []
            for j in range(2):
                s = lax.dot_general(q, kvbuf[slot, u, j, 0], (((1,), (1,)), ((), ())), preferred_element_type=F32)
                scores.append(jnp.where(pos < table[3 + j, item], s, NEG))
            top = jnp.max(jnp.maximum(scores[0], scores[1]), axis=1, keepdims=True)
            probs = [jnp.exp2((s - top) * (SCALE * LOG2E)) for s in scores]
            total = jnp.sum(probs[0] + probs[1], axis=1, keepdims=True)
            out = sum(dot(p.astype(BF16), kvbuf[slot, u, j, 1]) for j, p in enumerate(probs))
            live = top > NEG
            lse = jnp.where(live, top * SCALE + jnp.log(total), NEG)
            outs.append((seq, jnp.where(live, out / total, 0.0), jnp.broadcast_to(lse, (2 * HEADS, HEAD))))
        for seq, out, lse in outs:
            for t in range(2):
                for half in range(2):
                    rows = slice(t * HEADS + half * HALF_HEADS, t * HEADS + (half + 1) * HALF_HEADS)
                    part_o[seq // 32, half, t * 32 + seq % 32] = out[rows]
                    part_l[seq // 32, half, t * 32 + seq % 32] = lse[rows]

    def step(g, carry):
        keep(g, 1)

        @pl.when(g == STEPS // 2)
        def _():
            for phase in (1, 2):
                settle(phase) if layer == 1 else late(phase)

        @pl.when(g < groups)
        def _():
            copies(g, False)
            packs(g, True)

        @pl.when(g >= AFTER)
        def _():
            keep(g - AFTER, 2)

        @pl.when((g >= AFTER) & (g - AFTER < groups))
        def _():
            packs(g - AFTER, False)

        @pl.when(g + DIST < STEPS)
        def _():
            keep(g + DIST, 0)

        @pl.when(g + DIST < groups)
        def _():
            copies(g + DIST, True)

        @pl.when(g < groups)
        def _():
            attend(g)
        return carry

    lax.fori_loop(0, STEPS, step, 0)
    for g in range(STEPS - AFTER, STEPS):
        keep(g, 2)

        @pl.when(g < groups)
        def _():
            packs(g, False)
    settle(3) if layer == 1 else late(3)


def run_attend(layer, meta, table, slots, q_all, k_flat, v_flat, *extra):
    shape = jax.ShapeDtypeStruct((2, 2, TOK, HALF_HEADS, HEAD), F32)
    page = (PAGE * KV_HEADS, HEAD)
    late = (LATES, 2, LAYERS) + page
    more = [jax.ShapeDtypeStruct(k_flat.shape if layer else late, BF16)]
    return pl.pallas_call(
        functools.partial(attend_kernel, layer),
        name=f'attend{layer}',
        out_shape=[shape, shape, BOX, jax.ShapeDtypeStruct(k_flat.shape, BF16)] + more,
        in_specs=[SMEM, SMEM, SMEM, VMEM, ANY, ANY, SMEM] + [ANY, ANY, ANY] * layer,
        out_specs=[VMEM, VMEM, ANY, ANY, ANY],
        input_output_aliases={9: 4} if layer else {},
        scratch_shapes=[
            pltpu.VMEM((2 * TOK * HEADS, HEAD), F32),
            pltpu.VMEM((NBUF, UNROLL, 2, 2) + page, BF16),
            pltpu.VMEM((NBUF, SLOTS_STEP) + k_flat.shape[1:], BF16),
            DMA((NBUF,)),
            DMA((NBUF,)),
            DMA((NBUF, SLOTS_STEP)),
            DMA((NBUF, SLOTS_STEP)),
            pltpu.VMEM(((MIG, 2) + page) if layer else late, BF16),
            DMA,
            DMA,
        ],
        cost_estimate=pl.CostEstimate(flops=2 * 10 ** 10, bytes_accessed=16 * 2 ** 20, transcendentals=0),
        compiler_params=pltpu.CompilerParams(vmem_limit_bytes=VMEM_LIMIT),
    )(meta, table, slots, q_all, k_flat, v_flat, *extra)


def merge(parts):
    top = functools.reduce(jnp.maximum, [l for _, l in parts])
    weights = [jnp.exp(l - top) for _, l in parts]
    total = functools.reduce(jnp.add, weights)
    out = functools.reduce(jnp.add, [w * o for w, (o, _) in zip(weights, parts)]) / total
    return out, top + jnp.log(total)


LANES = ([((0,), 2, LATE), ((0,), 0, FAST_PAGES)], [((1,), 2, LATE), ((1,), 0, FAST_PAGES)])
EVERYTHING = [((0, 1), i, MIG) for i in range(3)]
CHUNK = 1


class Boxes:
    def __init__(self, moves, outbox, inbox, send_sems, recv_sems):
        me, chip, self.core, partner, across, diag = places()
        self.peers = (partner, across, diag)
        self.moves, self.outbox, self.inbox, self.send_sems, self.recv_sems = moves, outbox, inbox, send_sems, recv_sems

    def each(self, sending, act):
        for cores, channel, pages in self.moves:
            def run(channel=channel, pages=pages):
                def one(i, carry):
                    rows = pl.ds(channel * MIG + i * CHUNK, CHUNK)
                    act(send(self.outbox.at[rows], self.inbox.at[rows], self.send_sems.at[channel, i], self.recv_sems.at[channel, i], self.peers[channel]))
                    return carry

                lax.fori_loop(0, pages // CHUNK, one, 0)

            if len(cores) == 2:
                run()
            else:
                cross = 0 if channel == 1 else 1
                at = cores[0] if sending else (cores[0] + cross) % 2
                pl.when(self.core == at)(run)

    def start(self):
        self.each(True, lambda copy: copy.start())

    def wait(self):
        self.each(True, lambda copy: copy.wait_send())
        self.each(False, lambda copy: copy.wait_recv())


RING_W = 20
SOON = 4
TK = 2048
UP_TILES = FF // 2 // TN
TD = FF // 8
OUT_END = D // TN
UP_END = OUT_END + 2 * UP_TILES
DOWN_END = UP_END + 4 * (D // TN)
QKV_END = DOWN_END + 12
PART = TOK // 2


def rest_kernel(layer, lane_core, h_in, q_all, kv, part_o, part_l, wo, w_up, w_down, outbox, *refs):
    last = layer == LAYERS - 1
    if last:
        out, kv_all, inbox, *refs = refs
    else:
        wq, wk, wv, out, kv_all, inbox, q_next, kv_next, *refs = refs
        *refs, qp_send, qp_recv, qx_send, qx_recv, qf_send, qf_recv = refs
    (ring, ring_sem, own_o, own_l, own_sem, got_o, got_l, mine_o, mine_l, give_o, give_l, far_o, far_l, q_rows, k_rows, v_rows, attn, act, h,
     psend, precv, dsend, drecv, xsend, xrecv, ssem, rsem, ksend, krecv, bsend, brecv) = refs
    me, chip, core, partner, across, diag = places()
    boxes = Boxes(LANES[lane_core], outbox, inbox, bsend, brecv)
    end = DOWN_END if last else QKV_END

    def tile_copy(t, kind):
        slot = lax.rem(t, RING_W)
        if kind == 0:
            src = wo.at[layer, pl.ds(pl.multiple_of(core * TK, TK), TK), pl.ds(pl.multiple_of(t * TN, TN), TN)]
        elif kind == 1:
            i = t - OUT_END
            src = w_up.at[layer, pl.ds(pl.multiple_of(lax.rem(i, 2) * TK, TK), TK), pl.ds(pl.multiple_of(core * (FF // 2) + (i // 2) * TN, TN), TN)]
        elif kind >= 3:
            i = t - DOWN_END
            rows = pl.ds(pl.multiple_of(lax.rem(i, 2) * TK, TK), TK)
            if kind == 3:
                src = wq.at[layer + 1, rows, pl.ds(pl.multiple_of(core * 2048 + (i // 2) * TN, TN), TN)]
            else:
                src = (wk, wv)[kind - 4].at[layer + 1, rows, pl.ds(pl.multiple_of(core * TN, TN), TN)]
        else:
            i = t - UP_END
            src = w_down.at[layer, pl.ds(pl.multiple_of(core * (FF // 2) + lax.rem(i, 4) * TD, TD), TD), pl.ds(pl.multiple_of((i // 4) * TN, TN), TN)]
        dst = ring.at[slot, pl.ds(0, TD)] if kind == 2 else ring.at[slot]
        return pltpu.make_async_copy(src, dst, ring_sem.at[slot])

    def fetch(t):
        pl.when(t < OUT_END)(lambda: tile_copy(t, 0).start())
        pl.when((t >= OUT_END) & (t < UP_END))(lambda: tile_copy(t, 1).start())
        pl.when((t >= UP_END) & (t < DOWN_END))(lambda: tile_copy(t, 2).start())
        if not last:
            pl.when((t >= DOWN_END) & (t < DOWN_END + 8))(lambda: tile_copy(t, 3).start())
            pl.when((t >= DOWN_END + 8) & (t < DOWN_END + 10))(lambda: tile_copy(t, 4).start())
            pl.when((t >= DOWN_END + 10) & (t < QKV_END))(lambda: tile_copy(t, 5).start())

    own, near = [], []
    for which, (owner, first, size) in enumerate(((1 - chip, 0, PART), (1 - chip, PART, PART), (chip, 0, TOK))):
        at = pl.ds(which * PART, size)
        rows = pl.ds(first, size)
        for i, (src, dst) in enumerate(((part_o, own_o), (part_l, own_l))):
            copy = pltpu.make_async_copy(src.at[owner, core, rows], dst.at[at], own_sem.at[which, i])
            copy.start()
            own.append(copy)
        near.append([
            send(part_o.at[owner, 1 - core, rows], got_o.at[at], dsend.at[which, 0], drecv.at[which, 0], partner),
            send(part_l.at[owner, 1 - core, rows], got_l.at[at], dsend.at[which, 1], drecv.at[which, 1], partner),
        ])
    lax.fori_loop(0, SOON, lambda t, carry: (fetch(t), carry)[1], 0)
    meet((partner, across, diag))
    for pair in near:
        for copy in pair:
            copy.start()
    lax.fori_loop(SOON, RING_W, lambda t, carry: (fetch(t), carry)[1], 0)

    lane = lax.broadcasted_iota(jnp.int32, (8, HEAD), 1)
    far = []
    for part in range(2):
        for copy in own[2 * part:2 * part + 2]:
            copy.wait()
        for copy in near[part]:
            copy.wait_recv()

        def chip_merge(i, compact, part=part):
            j = part * PART + i
            o, l = merge([(own_o[j], own_l[j]), (got_o[j], got_l[j])])
            give_o[j] = o
            compact = jnp.where(lane == 2 * i, l[:8], compact)
            return jnp.where(lane == 2 * i + 1, l[8:], compact)

        give_l[part] = lax.fori_loop(0, PART, chip_merge, jnp.zeros((8, HEAD), F32), unroll=4)
        rows = pl.ds(part * PART, PART)
        pair = [
            send(give_l.at[part], far_l.at[part], xsend.at[part, 0], xrecv.at[part, 0], across),
            send(give_o.at[rows], far_o.at[rows], xsend.at[part, 1], xrecv.at[part, 1], across),
        ]
        for copy in pair:
            copy.start()
        far.append(pair)

    kv_all[me] = kv[...]
    new_rows = [send(kv, kv_all.at[me], ksend.at[i], krecv.at[i], peer) for i, peer in enumerate((partner, across))]
    new_rows.append(send(kv_all.at[across], kv_all.at[across], ksend.at[2], krecv.at[2], partner))

    for head in range(HALF_HEADS):
        tile = core * 4 + head // 4
        rows = pl.ds(head, TOK, stride=HALF_HEADS)
        q_rows[rows, :] = q_all[chip, tile, :, (head % 4) * HEAD:(head % 4 + 1) * HEAD].astype(F32)
        k_rows[rows, :] = kv[:, (head // 4) * HEAD:(head // 4 + 1) * HEAD].astype(F32)
        v_rows[rows, :] = kv[:, TN + (head // 4) * HEAD:TN + (head // 4 + 1) * HEAD].astype(F32)
    for copy in own[4:]:
        copy.wait()
    for copy in near[2]:
        copy.wait_recv()

    half = ROWS // 2

    def score(q, k):
        s = jnp.sum(q * k, axis=1, keepdims=True) * SCALE
        return jnp.broadcast_to(s, q.shape)

    def own_merge(i, carry):
        a = pl.ds(pl.multiple_of(i * HALF_HEADS, HALF_HEADS), HALF_HEADS)
        b = pl.ds(pl.multiple_of(half + i * HALF_HEADS, HALF_HEADS), HALF_HEADS)
        k0, v0, k1, v1 = k_rows[a, :], v_rows[a, :], k_rows[b, :], v_rows[b, :]
        q0, q1 = q_rows[a, :], q_rows[b, :]
        j = i + PART
        m, n = TOK + i, TOK + j
        o, l = merge([(own_o[m], own_l[m]), (got_o[m], got_l[m]), (v0, score(q0, k0))])
        mine_o[i] = o
        mine_l[i] = l
        o, l = merge([(own_o[n], own_l[n]), (got_o[n], got_l[n]), (v0, score(q1, k0)), (v1, score(q1, k1))])
        mine_o[j] = o
        mine_l[j] = l
        return carry

    lax.fori_loop(0, PART, own_merge, 0, unroll=2)

    for part in range(2):
        for copy in far[part]:
            copy.wait_recv()
        if part == 1:
            for copy in new_rows[:2]:
                copy.start()
            boxes.start()
        spread = far_l[part]

        def last_merge(i, carry, part=part, spread=spread):
            l = jnp.concatenate([
                jnp.broadcast_to(jnp.sum(jnp.where(lane == 2 * i + k, spread, 0.0), axis=1, keepdims=True), (8, HEAD)) for k in range(2)
            ], axis=0)
            j = part * PART + i
            o, _ = merge([(mine_o[j], mine_l[j]), (far_o[j], l)])
            q_rows[pl.ds(pl.multiple_of(j * HALF_HEADS, HALF_HEADS), HALF_HEADS), :] = o
            return carry

        lax.fori_loop(0, PART, last_merge, 0, unroll=4)
    for head in range(HALF_HEADS):
        attn[:, head * HEAD:(head + 1) * HEAD] = q_rows[pl.ds(head, TOK, stride=HALF_HEADS), :].astype(BF16)

    def reduce(j):
        return send(psend.at[j], precv.at[j], ssem.at[j], rsem.at[j], partner)

    def finish_sum(first, res, target):
        reduce(first + 7).start()
        for j in range(8):
            reduce(first + j).wait_recv()
            cols = slice(j * TN, (j + 1) * TN)
            target[:, cols] = (res[:, cols].astype(F32) + (psend[first + j] + precv[first + j])).astype(BF16)

    def project(j, carry):
        tile_copy(j, 0).wait()
        psend[j] = dot(attn[...], ring[lax.rem(j, RING_W)])
        fetch(j + RING_W)

        @pl.when(j > 0)
        def _():
            reduce(j - 1).start()
        return carry

    lax.fori_loop(0, OUT_END, project, 0)
    finish_sum(0, h_in, h)

    def up(s, carry):
        u = None
        for k in range(2):
            t = OUT_END + 2 * s + k
            tile_copy(t, 1).wait()
            part = dot(h[:, k * TK:(k + 1) * TK], ring[lax.rem(t, RING_W)])
            u = part if u is None else u + part
            fetch(t + RING_W)
        a = jax.nn.gelu(u.astype(BF16).astype(F32), approximate=True).astype(BF16)
        act[:, pl.ds(pl.multiple_of(s * TN, TN), TN)] = a
        return carry

    lax.fori_loop(0, UP_TILES, up, 0)
    new_rows[1].wait_recv()
    new_rows[2].start()

    def down(j, carry):
        total = None
        for k in range(4):
            t = UP_END + 4 * j + k
            tile_copy(t, 2).wait()
            part = dot(act[:, k * TD:(k + 1) * TD], ring[lax.rem(t, RING_W), :TD])
            total = part if total is None else total + part
            fetch(t + RING_W)
        psend[8 + j] = total

        @pl.when(j > 0)
        def _():
            reduce(8 + j - 1).start()
        return carry

    lax.fori_loop(0, D // TN, down, 0)
    finish_sum(8, h, out)

    if not last:
        def to_partner(j):
            ref = q_next.at[chip, core * 4 + j]
            return send(ref, ref, qp_send.at[j], qp_recv.at[j], partner)

        def to_across(j):
            ref = q_next.at[chip, core * 4 + j]
            return send(ref, ref, qx_send.at[j], qx_recv.at[j], across)

        def forward(j):
            ref = q_next.at[1 - chip, core * 4 + j]
            return send(ref, ref, qf_send.at[j], qf_recv.at[j], partner)

        def project_next(j, carry):
            total = None
            for k in range(2):
                t = DOWN_END + 2 * j + k
                tile_copy(t, 4).wait()
                part = dot(out[:, k * TK:(k + 1) * TK], ring[lax.rem(t, RING_W)])
                total = part if total is None else total + part
            tile = total.astype(BF16)

            @pl.when(j < 4)
            def _():
                q_next[chip, core * 4 + j] = tile

            @pl.when(j >= 4)
            def _():
                kv_next[:, pl.ds(pl.multiple_of((j - 4) * TN, TN), TN)] = tile

            @pl.when(j < 4)
            def _():
                to_across(j).start()
                to_partner(j).start()
            return carry

        lax.fori_loop(0, 6, project_next, 0)
        for j in range(4):
            to_across(j).wait_recv()
            forward(j).start()
        for j in range(4):
            to_across(j).wait_send()
            to_partner(j).wait()
            forward(j).wait()
    for j in range(16):
        reduce(j).wait_send()
    for pair in near + far:
        for copy in pair:
            copy.wait_send()
    new_rows[0].wait()
    new_rows[1].wait_send()
    new_rows[2].wait()
    boxes.wait()


def run_rest(layer, lane_core, h, q_all, kv, part_o, part_l, outbox, w_out, w_up, w_down, *weights):
    more = [jax.ShapeDtypeStruct((2, 8, TOK, TN), BF16), jax.ShapeDtypeStruct((TOK, 2 * TN), BF16)] if weights else []
    token = (HALF_HEADS, HEAD)
    return pl.pallas_call(
        functools.partial(rest_kernel, layer, lane_core),
        name=f'rest{layer}_{lane_core}',
        out_shape=[jax.ShapeDtypeStruct((TOK, D), BF16), jax.ShapeDtypeStruct((4, TOK, 2 * TN), BF16), BOX] + more,
        in_specs=[VMEM] * 3 + [ANY] * (6 + len(weights)),
        out_specs=[VMEM, VMEM, ANY] + [VMEM] * len(more),
        scratch_shapes=[
            pltpu.VMEM((RING_W, TK, TN), BF16),
            DMA((RING_W,)),
            pltpu.VMEM((2 * TOK,) + token, F32),
            pltpu.VMEM((2 * TOK,) + token, F32),
            DMA((3, 2)),
            pltpu.VMEM((2 * TOK,) + token, F32),
            pltpu.VMEM((2 * TOK,) + token, F32),
            pltpu.VMEM((TOK,) + token, F32),
            pltpu.VMEM((TOK,) + token, F32),
            pltpu.VMEM((TOK,) + token, F32),
            pltpu.VMEM((2, 8, HEAD), F32),
            pltpu.VMEM((TOK,) + token, F32),
            pltpu.VMEM((2, 8, HEAD), F32),
            pltpu.VMEM((ROWS, HEAD), F32),
            pltpu.VMEM((ROWS, HEAD), F32),
            pltpu.VMEM((ROWS, HEAD), F32),
            pltpu.VMEM((TOK, 2048), BF16),
            pltpu.VMEM((TOK, FF // 2), BF16),
            pltpu.VMEM((TOK, D), BF16),
            pltpu.VMEM((16, TOK, TN), F32),
            pltpu.VMEM((16, TOK, TN), F32),
            DMA((3, 2)),
            DMA((3, 2)),
            DMA((2, 2)),
            DMA((2, 2)),
            DMA((16,)),
            DMA((16,)),
            DMA((3,)),
            DMA((3,)),
            DMA((3, MIG // CHUNK)),
            DMA((3, MIG // CHUNK)),
        ] + [DMA((4,))] * (6 if weights else 0),
        cost_estimate=pl.CostEstimate(flops=2 * TOK * D * FF * 8, bytes_accessed=D * FF * 2, transcendentals=0),
        compiler_params=pltpu.CompilerParams(collective_id=2 + layer * 2 + lane_core, has_side_effects=True, vmem_limit_bytes=67043328),
    )(h, q_all, kv, part_o, part_l, w_out, w_up, w_down, outbox, *weights)


def move_kernel(outbox, inbox, send_sems, recv_sems):
    me, chip, core, partner, across, diag = places()
    meet((partner, across, diag))
    boxes = Boxes(EVERYTHING, outbox, inbox, send_sems, recv_sems)
    boxes.start()
    boxes.wait()


def run_move(layer, outbox):
    return pl.pallas_call(
        move_kernel,
        name=f'move{layer}',
        out_shape=BOX,
        in_specs=[ANY],
        out_specs=ANY,
        scratch_shapes=[DMA((3, MIG // CHUNK)), DMA((3, MIG // CHUNK))],
        compiler_params=pltpu.CompilerParams(collective_id=6 + layer, has_side_effects=True),
    )(outbox)


def run_blank(layer):
    return pl.pallas_call(lambda box: None, name=f'blank{layer}', out_shape=BOX, out_specs=ANY)()


RING = 32
AHEAD = RING // 2


def finish_kernel(meta, moved, gone, rows, inbox, spare, late, kv0, kv1, k_in, v_in, k_out, v_out, wide, row_buf, zeros, buf, in_sem, out_sem, zero_sem, row_sem):
    del k_in, v_in
    outs = (k_out, v_out)
    count = meta[2]

    def loop(first, last, body):
        lax.fori_loop(first, last, lambda i, carry: (body(i), carry)[1], 0)

    def clear(i):
        return [pltpu.make_async_copy(zeros, out.at[gone[i]], zero_sem) for out in outs]

    def is_late(i):
        return (moved[1, i] >= 2 * MIG + LATE) & (meta[1] < 2)

    def load(i, box):
        slot = lax.rem(i, RING)
        return [pltpu.make_async_copy(box.at[moved[1, i], p], buf.at[slot, p, 1], in_sem.at[slot, p]) for p in range(2)]

    def load_late(i):
        slot = lax.rem(i, RING)
        return [pltpu.make_async_copy(late.at[moved[1, i] - (2 * MIG + LATE), p], buf.at[slot, p], in_sem.at[slot, p]) for p in range(2)]

    def store(i):
        slot = lax.rem(i, RING)
        return [pltpu.make_async_copy(buf.at[slot, p, 1], outs[p].at[moved[0, i], 1], out_sem.at[slot, p]) for p in range(2)]

    def store_late(i):
        slot = lax.rem(i, RING)
        return [pltpu.make_async_copy(buf.at[slot, p], outs[p].at[moved[0, i]], out_sem.at[slot, p]) for p in range(2)]

    def begin(group):
        for copy in group:
            copy.start()

    def end(group):
        for copy in group:
            copy.wait()

    def begin_load(i):
        pl.when((meta[1] < 2) & jnp.logical_not(is_late(i)))(lambda: begin(load(i, inbox)))
        pl.when(is_late(i))(lambda: begin(load_late(i)))
        pl.when(meta[1] == 2)(lambda: begin(load(i, spare)))

    def begin_store(i):
        @pl.when(is_late(i))
        def _():
            end(load_late(i))
            begin(store_late(i))

        @pl.when(jnp.logical_not(is_late(i)))
        def _():
            end(load(i, inbox))
            begin(store(i))

    def end_store(i):
        pl.when(is_late(i))(lambda: end(store_late(i)))
        pl.when(jnp.logical_not(is_late(i)))(lambda: end(store(i)))

    loop(0, jnp.minimum(count, AHEAD), begin_load)
    zeros[...] = jnp.zeros_like(zeros)
    loop(0, meta[4], lambda i: begin(clear(i)))

    for l, kv in enumerate((kv0, kv1)):
        for p in range(2):
            for dev in range(4):
                for i in range(4):
                    for t in range(2):
                        at = pl.ds((dev // 2) * TOK * KV_HEADS + t * KV_HEADS + (dev % 2) * 4 + i, TOK // 2, stride=2 * KV_HEADS)
                        wide[at, :] = kv[dev, t * 32:(t + 1) * 32, (p * 4 + i) * HEAD:(p * 4 + i + 1) * HEAD].astype(F32)
            row_buf[p, l] = wide[...].astype(BF16)

    def page(i):
        begin_store(i)

        @pl.when(i + AHEAD < count)
        def _():
            pl.when(i >= AHEAD)(lambda: end_store(i - AHEAD))
            begin_load(i + AHEAD)

    loop(0, count, page)
    loop(jnp.maximum(count - RING, 0), count, end_store)

    def row(i):
        at = pl.ds(pl.multiple_of(rows[1, i] * KV_HEADS, KV_HEADS), 2 * KV_HEADS)
        src = pl.ds(pl.multiple_of(rows[2, i] * 2 * KV_HEADS, 2 * KV_HEADS), 2 * KV_HEADS)
        return [pltpu.make_async_copy(row_buf.at[p, :, src, :], outs[p].at[rows[0, i], :, at, :], row_sem.at[p]) for p in range(2)]

    loop(0, meta[3], lambda i: begin(row(i)))
    loop(0, meta[3], lambda i: end(row(i)))
    loop(0, meta[4], lambda i: end(clear(i)))


def run_finish(meta, moved, gone, rows, boxes, kvs, k_part, v_part):
    shape = jax.ShapeDtypeStruct(k_part.shape, BF16)
    return pl.pallas_call(
        finish_kernel,
        name='finish',
        out_shape=[shape, shape],
        in_specs=[SMEM] * 4 + [ANY, ANY, ANY, VMEM, VMEM, ANY, ANY],
        out_specs=[ANY, ANY],
        scratch_shapes=[
            pltpu.VMEM((2 * TOK * KV_HEADS, HEAD), F32),
            pltpu.VMEM((2, LAYERS, 2 * TOK * KV_HEADS, HEAD), BF16),
            pltpu.VMEM(k_part.shape[1:], BF16),
            pltpu.VMEM((RING, 2) + k_part.shape[1:], BF16),
            DMA((RING, 2)),
            DMA((RING, 2)),
            DMA,
            DMA((2,)),
        ],
        input_output_aliases={9: 0, 10: 1},
        cost_estimate=pl.CostEstimate(flops=10 ** 10, bytes_accessed=16 * 2 ** 20, transcendentals=0),
        compiler_params=pltpu.CompilerParams(vmem_limit_bytes=VMEM_LIMIT),
    )(meta, moved, gone, rows, *boxes, *kvs, k_part, v_part)


def solution(mesh):
    pool_spec = P(('rep', 'kv'))
    tok_spec = P(None, ('rep', 'kv'), None)

    def device_fn(embeds, w_query, w_key, w_value, w_out, w_up, w_down, k_pool, v_pool, new_table, seq_lens, mig_src, mig_dst):
        me = lax.axis_index('kv')
        weights = (w_query, w_key, w_value)
        k_flat, v_flat = flat_pool(k_pool), flat_pool(v_pool)
        meta, items, slots, gone, moved, where, lates, lane, general = run_plan(new_table, seq_lens, mig_src, mig_dst)
        q_all, kv, h = run_qkv(0, embeds, weights, True)
        part_o, part_l, outbox, k_kept, late_box = run_attend(0, meta, items, slots, q_all, k_flat, v_flat, lates)

        def extra_boxes(layer, outbox):
            return lax.switch(general.reshape(()), [lambda box: run_blank(layer), functools.partial(run_move, layer)], outbox)

        def layers(core, h, q_all, kv, part_o, part_l, outbox, late_box, k_kept):
            h, kv_all0, inbox, q_all, kv = run_rest(0, core, h, q_all, kv, part_o, part_l, outbox, w_out, w_up, w_down, *weights)
            spare = extra_boxes(0, outbox)
            late_box, q_all = lax.optimization_barrier((late_box, q_all))
            late = lax.ppermute(late_box, 'kv', [(core, 3 - core), (2 + core, 1 - core)])
            part_o, part_l, outbox, v_kept, k_kept = run_attend(1, meta, items, slots, q_all, k_flat, v_flat, moved, inbox, spare, k_kept)
            h, kv_all1, inbox = run_rest(1, core, h, q_all, kv, part_o, part_l, outbox, w_out, w_up, w_down)
            return h, kv_all0, kv_all1, inbox, extra_boxes(1, outbox), late, k_kept, v_kept

        forms = [functools.partial(layers, core) for core in range(2)]
        h, kv_all0, kv_all1, inbox, spare, late, k_kept, v_kept = lax.switch(lane.reshape(()), forms, h, q_all, kv, part_o, part_l, outbox, late_box, k_kept)
        k_out, v_out = run_finish(meta, moved, gone, where, (inbox, spare, late), (kv_all0, kv_all1), k_kept, v_kept)
        k_out, v_out = k_out.reshape(k_pool.shape), v_out.reshape(v_pool.shape)
        y = lax.dynamic_slice_in_dim(h.reshape(2, 32, D), (me % 2) * 16, 16, axis=1)
        return y, k_out, v_out

    return jax.shard_map(device_fn, mesh=mesh, in_specs=(tok_spec, P(), P(), P(), P(), P(), P(), pool_spec, pool_spec, P('rep', None), P('rep'), P('rep'), P('rep')), out_specs=(tok_spec, pool_spec, pool_spec), check_vma=False)
```

```python
import functools

import jax
import jax.numpy as jnp
from jax import lax
from jax.experimental import pallas as pl
from jax.experimental.pallas import tpu as pltpu
from jax.sharding import PartitionSpec as P

BF16 = jnp.bfloat16
F32 = jnp.float32
MESH = pl.DeviceIdType.MESH
NEG = -3.0e38
VMEM_LIMIT = 60 * 1024 * 1024

D = 4096
HEADS = 32
KV_HEADS = 8
HEAD = 128
FF = 14336
PAGE = 32
LAYERS = 2
SEQS = 64
MIG = 64
TOK = 64
HALF_HEADS = HEADS // 2
ROWS = TOK * HALF_HEADS
TN = 512
SCALE = HEAD ** -0.5
LOG2E = 1.4426950408889634
SLOTS = 96
UNROLL = 4
FAST_PAGES = 32
LATE = 20
LATES = FAST_PAGES - LATE
BOX = jax.ShapeDtypeStruct((3 * MIG, 2, PAGE * KV_HEADS, HEAD), BF16)


def flat_pool(pool):
    return pool.reshape(pool.shape[0], LAYERS, PAGE * KV_HEADS, HEAD)


def dot(a, b):
    return jnp.dot(a, b, preferred_element_type=F32)


def places():
    me = lax.axis_index('kv')
    core = lax.rem(me, 2)
    chip = me // 2
    partner = me + 1 - 2 * core
    across = lax.rem(me + 2, 4)
    diag = lax.rem(partner + 2, 4)
    return me, chip, core, partner, across, diag


def meet(peers):
    barrier = pltpu.get_barrier_semaphore()
    for peer in peers:
        pl.semaphore_signal(barrier, inc=1, device_id={'kv': peer}, device_id_type=MESH)
    pl.semaphore_wait(barrier, len(peers))


def send(src, dst, send_sem, recv_sem, peer):
    return pltpu.make_async_remote_copy(src_ref=src, dst_ref=dst, send_sem=send_sem, recv_sem=recv_sem, device_id={'kv': peer}, device_id_type=MESH)


VMEM = pl.BlockSpec(memory_space=pltpu.VMEM)
SMEM = pl.BlockSpec(memory_space=pltpu.SMEM)
ANY = pl.BlockSpec(memory_space=pl.ANY)
DMA = pltpu.SemaphoreType.DMA


WINDOW = 3


def qkv_kernel(layer, first, *refs):
    if first:
        emb, wq, wk, wv, q_all, kv, h, wbuf, wsem, psend, precv, xsend, xrecv, fsend, frecv, hsend, hrecv = refs
    else:
        h, wq, wk, wv, q_all, kv, wbuf, wsem, psend, precv, xsend, xrecv, fsend, frecv = refs
    me, chip, core, partner, across, diag = places()

    def fetch(j):
        if j < 4:
            src = wq.at[layer, :, pl.ds(pl.multiple_of(core * 2048 + j * TN, TN), TN)]
        else:
            src = (wk, wv)[j - 4].at[layer, :, pl.ds(pl.multiple_of(core * TN, TN), TN)]
        return pltpu.make_async_copy(src, wbuf.at[j], wsem.at[j])

    for j in range(WINDOW):
        fetch(j).start()
    meet((partner, across))
    if first:
        copies = []
        for t in range(2):
            rows = pl.ds(pl.multiple_of(t * 32 + core * 16, 16), 16)
            h[rows, :] = emb[t]
            copies.append(send(emb.at[t], h.at[rows, :], hsend.at[t], hrecv.at[t], partner))
        for copy in copies:
            copy.start()
        for copy in copies:
            copy.wait()

    def to_partner(j):
        ref = q_all.at[chip, core * 4 + j]
        return send(ref, ref, psend.at[j], precv.at[j], partner)

    def to_across(j):
        ref = q_all.at[chip, core * 4 + j]
        return send(ref, ref, xsend.at[j], xrecv.at[j], across)

    def forward(j):
        ref = q_all.at[1 - chip, core * 4 + j]
        return send(ref, ref, fsend.at[j], frecv.at[j], partner)

    def tile(j, carry):
        pltpu.make_async_copy(wq.at[layer, :, pl.ds(0, TN)], wbuf.at[j], wsem.at[j]).wait()
        q_all[chip, core * 4 + j] = dot(h[...], wbuf[j]).astype(BF16)
        for i in range(4):
            if i + WINDOW < 6:
                pl.when(j == i)(lambda i=i: fetch(i + WINDOW).start())

        to_across(j).start()
        to_partner(j).start()
        return carry

    lax.fori_loop(0, 4, tile, 0)
    for j in range(4, 6):
        fetch(j).wait()
        kv[:, (j - 4) * TN:(j - 3) * TN] = dot(h[...], wbuf[j]).astype(BF16)
    for j in range(4):
        to_across(j).wait_recv()
        forward(j).start()
    for j in range(4):
        to_across(j).wait_send()
        to_partner(j).wait()
        forward(j).wait()


def run_qkv(layer, h, weights, first):
    wq, wk, wv = weights[:3]
    out_shape = [jax.ShapeDtypeStruct((2, 8, TOK, TN), BF16), jax.ShapeDtypeStruct((TOK, 2 * TN), BF16)]
    if first:
        out_shape.append(jax.ShapeDtypeStruct((TOK, D), BF16))
    scratch = [pltpu.VMEM((6, D, TN), BF16), DMA((6,))] + [DMA((4,))] * 6
    if first:
        scratch += [DMA((2,))] * 2
    return pl.pallas_call(
        functools.partial(qkv_kernel, layer, first),
        name=f'qkv{layer}',
        out_shape=out_shape,
        in_specs=[VMEM, ANY, ANY, ANY],
        out_specs=[VMEM] * len(out_shape),
        scratch_shapes=scratch,
        cost_estimate=pl.CostEstimate(flops=2 * TOK * D * 6 * TN * 8, bytes_accessed=D * 6 * TN * 2, transcendentals=0),
        compiler_params=pltpu.CompilerParams(collective_id=layer, has_side_effects=True, vmem_limit_bytes=VMEM_LIMIT),
    )(h, wq, wk, wv)


def plan_kernel(new_table, seq_lens, mig_src, mig_dst, meta, items, slots, gone, moved, rows, lates, lane, general, source, place_of, counts):
    me = lax.axis_index('kv')
    base = me * SLOTS

    def home(slot):
        return sum((slot >= i * SLOTS).astype(jnp.int32) for i in range(1, 4))

    def clear(i, carry):
        source[i] = -1
        place_of[i] = -1
        return carry

    lax.fori_loop(0, 4 * SLOTS, clear, 0, unroll=16)
    for i in range(16):
        counts[i] = 0
    for i in range(LATES):
        lates[i] = -1

    def keep(i, carry):
        slots[i] = 0
        return carry

    lax.fori_loop(0, SLOTS, keep, 0, unroll=16)

    def entry(e, carry):
        n, m, even, odd = carry
        s, d = mig_src[e], mig_dst[e]
        hs, hd = home(s), home(d)
        pair = hs * 4 + hd
        rank = counts[pair]
        counts[pair] = rank + 1
        channel = (hs ^ hd) - 1
        place = channel * MIG + rank
        source[d] = s
        place_of[d] = place
        misfit = ((channel == 1) | (rank >= FAST_PAGES)).astype(jnp.int32)
        even = even | misfit | (hs & 1)
        odd = odd | misfit | (1 - (hs & 1))

        slots[jnp.where(hs == me, s - base, SLOTS)] = 1
        slots[jnp.where(hd == me, d - base, SLOTS)] = 1
        gone[m] = s - base
        is_late = (hs == me) & (channel == 2) & (rank >= LATE) & (rank < FAST_PAGES)
        lates[jnp.where(is_late, rank - LATE, LATES)] = s - base
        moved[0, n] = d - base
        moved[1, n] = place
        return n + (hd == me).astype(jnp.int32), m + (hs == me).astype(jnp.int32), even, odd

    zero = jnp.int32(0)
    n_moved, n_gone, even, odd = lax.fori_loop(0, MIG, entry, (zero, zero, zero, zero), unroll=8)

    def sequence(b, carry):
        n, m = carry
        length = seq_lens[b]
        local, own, place = [], [], []
        for j in range(2):
            slot = new_table[j, b]
            src = source[slot]
            old = jnp.where(src >= 0, src, slot) - base
            mine = (old >= 0) & (old < SLOTS)
            local.append(old)
            own.append(mine)
            place.append(jnp.where(mine, place_of[slot], -1))
        items[0, n] = b
        items[1, n] = jnp.where(own[0], local[0], -1)
        items[2, n] = jnp.where(own[1], local[1], -1)
        items[3, n] = jnp.where(own[0], jnp.minimum(length, PAGE), 0)
        items[4, n] = jnp.where(own[1], jnp.maximum(length - PAGE, 0), 0)
        items[5, n] = place[0]
        items[6, n] = place[1]
        here = new_table[1, b] - base
        rows[0, m] = here
        rows[1, m] = length - PAGE
        rows[2, m] = b
        m = m + ((here >= 0) & (here < SLOTS)).astype(jnp.int32)
        return n + (own[0] | own[1]).astype(jnp.int32), m

    n_items, n_rows = lax.fori_loop(0, SEQS, sequence, (zero, zero), unroll=8)

    @pl.when(n_items > 0)
    def _():
        for i in range(UNROLL - 1):
            for f in range(5):
                items[f, n_items + i] = items[f, n_items - 1]
            for f in range(5, 7):
                items[f, n_items + i] = -1
    meta[0] = n_items
    meta[1] = jnp.where(even == 0, 0, jnp.where(odd == 0, 1, 2))
    lane[0] = jnp.where(even == 0, 0, 1)
    general[0] = jnp.where((even == 0) | (odd == 0), 0, 1)
    meta[2] = n_moved
    meta[3] = n_rows
    meta[4] = n_gone


def run_plan(new_table, seq_lens, mig_src, mig_dst):
    shapes = [(5,), (7, SEQS + UNROLL), (SLOTS + 1,), (MIG + 1,), (2, MIG + 1), (3, SEQS + 1), (LATES + 1,), (1,), (1,)]
    return pl.pallas_call(
        plan_kernel,
        name='plan',
        out_shape=[jax.ShapeDtypeStruct(shape, jnp.int32) for shape in shapes],
        in_specs=[SMEM] * 4,
        out_specs=[SMEM] * len(shapes),
        scratch_shapes=[pltpu.SMEM((4 * SLOTS,), jnp.int32), pltpu.SMEM((4 * SLOTS,), jnp.int32), pltpu.SMEM((16,), jnp.int32)],
    )(new_table.T, seq_lens, mig_src, mig_dst)


NBUF = 4
AFTER = 1
DIST = NBUF - AFTER
STEPS = SEQS // UNROLL
SLOTS_STEP = SLOTS // STEPS


def attend_kernel(layer, meta, table, slots, q_all, k_pool, v_pool, *refs):
    if layer == 0:
        lates, part_o, part_l, outbox, pool_out, late_box, *refs, late_buf, late_in, late_out = refs
    else:
        moved, inbox, spare, _, part_o, part_l, outbox, pool_out, k_out, *refs, pages, page_in, page_out = refs
    q_rows, kvbuf, ring, sems, out_sems, ring_in, ring_out = refs
    pool = (k_pool, v_pool)[layer]
    groups = (meta[0] + UNROLL - 1) // UNROLL

    def copies(g, start):
        slot = lax.rem(g, NBUF)
        for u in range(UNROLL):
            for j in range(2):
                page = table[1 + j, g * UNROLL + u]

                @pl.when(page >= 0)
                def _():
                    if start:
                        for p, ref in enumerate((k_pool, v_pool)):
                            pltpu.make_async_copy(ref.at[page, layer], kvbuf.at[slot, u, j, p], sems.at[slot]).start()
                    else:
                        pltpu.make_async_copy(outbox.at[0], kvbuf.at[slot, u, j], sems.at[slot]).wait()

    def packs(g, start):
        slot = lax.rem(g, NBUF)
        for u in range(UNROLL):
            for j in range(2):
                place = table[5 + j, g * UNROLL + u]

                @pl.when(place >= 0)
                def _():
                    copy = pltpu.make_async_copy(kvbuf.at[slot, u, j], outbox.at[place], out_sems.at[slot])
                    copy.start() if start else copy.wait()

    def keep(s, phase):
        place = lax.rem(s, NBUF)
        for i in range(SLOTS_STEP):
            slot = s * SLOTS_STEP + i

            @pl.when(slots[slot] == 0)
            def _():
                if phase < 2:
                    load = pltpu.make_async_copy(pool.at[slot], ring.at[place, i], ring_in.at[place, i])
                    load.wait() if phase else load.start()
                if phase > 0:
                    store = pltpu.make_async_copy(ring.at[place, i], pool_out.at[slot], ring_out.at[place, i])
                    store.start() if phase == 1 else store.wait()

    def settle(phase):
        def one(i, carry):
            place = moved[1, i]
            here = (place < 2 * MIG + LATE) | (meta[1] == 2)

            def move(box):
                for p, dst in enumerate((k_out, pool_out)):
                    if phase < 2:
                        copy = pltpu.make_async_copy(box.at[moved[1, i], p], pages.at[i, p], page_in)
                    else:
                        copy = pltpu.make_async_copy(pages.at[i, p], dst.at[moved[0, i], 0], page_out)
                    copy.wait() if phase % 2 else copy.start()

            if phase:
                pl.when(here)(lambda: move(inbox))
            else:
                pl.when(here & (meta[1] < 2))(lambda: move(inbox))
                pl.when(meta[1] == 2)(lambda: move(spare))
            return carry

        lax.fori_loop(0, meta[2], one, 0)

    def late(phase):
        def one(i, carry):
            @pl.when(lates[i] >= 0)
            def _():
                if phase == 0:
                    for p, ref in enumerate((k_pool, v_pool)):
                        pltpu.make_async_copy(ref.at[lates[i]], late_buf.at[i, p], late_in).start()
                elif phase == 1:
                    pltpu.make_async_copy(late_box.at[i], late_buf.at[i], late_in).wait()
                else:
                    copy = pltpu.make_async_copy(late_buf.at[i], late_box.at[i], late_out)
                    copy.wait() if phase == 3 else copy.start()
            return carry

        lax.fori_loop(0, LATES, one, 0)

    if layer == 1:
        settle(0)
    else:
        late(0)
    kvbuf[:, :, :, 1] = jnp.zeros((NBUF, UNROLL, 2) + kvbuf.shape[4:], BF16)
    for g in range(DIST):
        @pl.when(g < groups)
        def _():
            copies(g, True)
        keep(g, 0)
    part_o[...] = jnp.zeros_like(part_o)
    part_l[...] = jnp.full_like(part_l, NEG)

    for chip in range(2):
        for tile in range(8):
            for i in range(4):
                rows = q_all[chip, tile, :, i * HEAD:(i + 1) * HEAD].astype(F32)
                q_rows[pl.ds(chip * TOK * HEADS + tile * 4 + i, TOK, stride=HEADS), :] = rows

    row = lax.broadcasted_iota(jnp.int32, (2 * HEADS, 256), 0)
    col = lax.broadcasted_iota(jnp.int32, (2 * HEADS, 256), 1)
    pos = jnp.where((row % HEADS) // 4 == col % KV_HEADS, col // KV_HEADS, PAGE)

    def attend(g):
        slot = lax.rem(g, NBUF)
        outs = []
        for u in range(UNROLL):
            item = g * UNROLL + u
            seq = table[0, item]
            base = (seq // 32) * TOK * HEADS + (seq % 32) * HEADS
            q0 = q_rows[pl.ds(pl.multiple_of(base, HEADS), HEADS), :]
            q1 = q_rows[pl.ds(pl.multiple_of(base + 32 * HEADS, HEADS), HEADS), :]
            q = jnp.concatenate([q0, q1], axis=0).astype(BF16)
            scores = []
            for j in range(2):
                s = lax.dot_general(q, kvbuf[slot, u, j, 0], (((1,), (1,)), ((), ())), preferred_element_type=F32)
                scores.append(jnp.where(pos < table[3 + j, item], s, NEG))
            top = jnp.max(jnp.maximum(scores[0], scores[1]), axis=1, keepdims=True)
            probs = [jnp.exp2((s - top) * (SCALE * LOG2E)) for s in scores]
            total = jnp.sum(probs[0] + probs[1], axis=1, keepdims=True)
            out = sum(dot(p.astype(BF16), kvbuf[slot, u, j, 1]) for j, p in enumerate(probs))
            live = top > NEG
            lse = jnp.where(live, top * SCALE + jnp.log(total), NEG)
            outs.append((seq, jnp.where(live, out / total, 0.0), jnp.broadcast_to(lse, (2 * HEADS, HEAD))))
        for seq, out, lse in outs:
            for t in range(2):
                for half in range(2):
                    rows = slice(t * HEADS + half * HALF_HEADS, t * HEADS + (half + 1) * HALF_HEADS)
                    part_o[seq // 32, half, t * 32 + seq % 32] = out[rows]
                    part_l[seq // 32, half, t * 32 + seq % 32] = lse[rows]

    def step(g, carry):
        keep(g, 1)

        @pl.when(g == STEPS // 2)
        def _():
            for phase in (1, 2):
                settle(phase) if layer == 1 else late(phase)

        @pl.when(g < groups)
        def _():
            copies(g, False)
            packs(g, True)

        @pl.when(g >= AFTER)
        def _():
            keep(g - AFTER, 2)

        @pl.when((g >= AFTER) & (g - AFTER < groups))
        def _():
            packs(g - AFTER, False)

        @pl.when(g + DIST < STEPS)
        def _():
            keep(g + DIST, 0)

        @pl.when(g + DIST < groups)
        def _():
            copies(g + DIST, True)

        @pl.when(g < groups)
        def _():
            attend(g)
        return carry

    lax.fori_loop(0, STEPS, step, 0)
    for g in range(STEPS - AFTER, STEPS):
        keep(g, 2)

        @pl.when(g < groups)
        def _():
            packs(g, False)
    settle(3) if layer == 1 else late(3)


def run_attend(layer, meta, table, slots, q_all, k_flat, v_flat, *extra):
    shape = jax.ShapeDtypeStruct((2, 2, TOK, HALF_HEADS, HEAD), F32)
    page = (PAGE * KV_HEADS, HEAD)
    late = (LATES, 2, LAYERS) + page
    more = [jax.ShapeDtypeStruct(k_flat.shape if layer else late, BF16)]
    return pl.pallas_call(
        functools.partial(attend_kernel, layer),
        name=f'attend{layer}',
        out_shape=[shape, shape, BOX, jax.ShapeDtypeStruct(k_flat.shape, BF16)] + more,
        in_specs=[SMEM, SMEM, SMEM, VMEM, ANY, ANY, SMEM] + [ANY, ANY, ANY] * layer,
        out_specs=[VMEM, VMEM, ANY, ANY, ANY],
        input_output_aliases={9: 4} if layer else {},
        scratch_shapes=[
            pltpu.VMEM((2 * TOK * HEADS, HEAD), F32),
            pltpu.VMEM((NBUF, UNROLL, 2, 2) + page, BF16),
            pltpu.VMEM((NBUF, SLOTS_STEP) + k_flat.shape[1:], BF16),
            DMA((NBUF,)),
            DMA((NBUF,)),
            DMA((NBUF, SLOTS_STEP)),
            DMA((NBUF, SLOTS_STEP)),
            pltpu.VMEM(((MIG, 2) + page) if layer else late, BF16),
            DMA,
            DMA,
        ],
        cost_estimate=pl.CostEstimate(flops=2 * 10 ** 10, bytes_accessed=16 * 2 ** 20, transcendentals=0),
        compiler_params=pltpu.CompilerParams(vmem_limit_bytes=VMEM_LIMIT),
    )(meta, table, slots, q_all, k_flat, v_flat, *extra)


def merge(parts):
    top = functools.reduce(jnp.maximum, [l for _, l in parts])
    weights = [jnp.exp(l - top) for _, l in parts]
    total = functools.reduce(jnp.add, weights)
    out = functools.reduce(jnp.add, [w * o for w, (o, _) in zip(weights, parts)]) / total
    return out, top + jnp.log(total)


LANES = ([((0,), 2, LATE), ((0,), 0, FAST_PAGES)], [((1,), 2, LATE), ((1,), 0, FAST_PAGES)])
EVERYTHING = [((0, 1), i, MIG) for i in range(3)]
CHUNK = 4


class Boxes:
    def __init__(self, moves, outbox, inbox, send_sems, recv_sems):
        me, chip, self.core, partner, across, diag = places()
        self.peers = (partner, across, diag)
        self.moves, self.outbox, self.inbox, self.send_sems, self.recv_sems = moves, outbox, inbox, send_sems, recv_sems

    def each(self, sending, act):
        for cores, channel, pages in self.moves:
            def run(channel=channel, pages=pages):
                def one(i, carry):
                    rows = pl.ds(channel * MIG + i * CHUNK, CHUNK)
                    act(send(self.outbox.at[rows], self.inbox.at[rows], self.send_sems.at[channel, i], self.recv_sems.at[channel, i], self.peers[channel]))
                    return carry

                lax.fori_loop(0, pages // CHUNK, one, 0)

            if len(cores) == 2:
                run()
            else:
                cross = 0 if channel == 1 else 1
                at = cores[0] if sending else (cores[0] + cross) % 2
                pl.when(self.core == at)(run)

    def start(self):
        self.each(True, lambda copy: copy.start())

    def wait(self):
        self.each(True, lambda copy: copy.wait_send())
        self.each(False, lambda copy: copy.wait_recv())


RING_W = 20
SOON = 4
TK = 2048
UP_TILES = FF // 2 // TN
TD = FF // 8
OUT_END = D // TN
UP_END = OUT_END + 2 * UP_TILES
DOWN_END = UP_END + 4 * (D // TN)
QKV_END = DOWN_END + 12
PART = TOK // 2


def rest_kernel(layer, lane_core, h_in, q_all, kv, part_o, part_l, wo, w_up, w_down, outbox, *refs):
    last = layer == LAYERS - 1
    if last:
        out, kv_all, inbox, *refs = refs
    else:
        wq, wk, wv, out, kv_all, inbox, q_next, kv_next, *refs = refs
        *refs, qp_send, qp_recv, qx_send, qx_recv, qf_send, qf_recv = refs
    (ring, ring_sem, own_o, own_l, own_sem, got_o, got_l, mine_o, mine_l, give_o, give_l, far_o, far_l, q_rows, k_rows, v_rows, attn, act, h,
     psend, precv, dsend, drecv, xsend, xrecv, ssem, rsem, ksend, krecv, bsend, brecv) = refs
    me, chip, core, partner, across, diag = places()
    boxes = Boxes(LANES[lane_core], outbox, inbox, bsend, brecv)
    end = DOWN_END if last else QKV_END

    def tile_copy(t, kind):
        slot = lax.rem(t, RING_W)
        if kind == 0:
            src = wo.at[layer, pl.ds(pl.multiple_of(core * TK, TK), TK), pl.ds(pl.multiple_of(t * TN, TN), TN)]
        elif kind == 1:
            i = t - OUT_END
            src = w_up.at[layer, pl.ds(pl.multiple_of(lax.rem(i, 2) * TK, TK), TK), pl.ds(pl.multiple_of(core * (FF // 2) + (i // 2) * TN, TN), TN)]
        elif kind >= 3:
            i = t - DOWN_END
            rows = pl.ds(pl.multiple_of(lax.rem(i, 2) * TK, TK), TK)
            if kind == 3:
                src = wq.at[layer + 1, rows, pl.ds(pl.multiple_of(core * 2048 + (i // 2) * TN, TN), TN)]
            else:
                src = (wk, wv)[kind - 4].at[layer + 1, rows, pl.ds(pl.multiple_of(core * TN, TN), TN)]
        else:
            i = t - UP_END
            src = w_down.at[layer, pl.ds(pl.multiple_of(core * (FF // 2) + lax.rem(i, 4) * TD, TD), TD), pl.ds(pl.multiple_of((i // 4) * TN, TN), TN)]
        dst = ring.at[slot, pl.ds(0, TD)] if kind == 2 else ring.at[slot]
        return pltpu.make_async_copy(src, dst, ring_sem.at[slot])

    def fetch(t):
        pl.when(t < OUT_END)(lambda: tile_copy(t, 0).start())
        pl.when((t >= OUT_END) & (t < UP_END))(lambda: tile_copy(t, 1).start())
        pl.when((t >= UP_END) & (t < DOWN_END))(lambda: tile_copy(t, 2).start())
        if not last:
            pl.when((t >= DOWN_END) & (t < DOWN_END + 8))(lambda: tile_copy(t, 3).start())
            pl.when((t >= DOWN_END + 8) & (t < DOWN_END + 10))(lambda: tile_copy(t, 4).start())
            pl.when((t >= DOWN_END + 10) & (t < QKV_END))(lambda: tile_copy(t, 5).start())

    own, near = [], []
    for which, (owner, first, size) in enumerate(((1 - chip, 0, PART), (1 - chip, PART, PART), (chip, 0, TOK))):
        at = pl.ds(which * PART, size)
        rows = pl.ds(first, size)
        for i, (src, dst) in enumerate(((part_o, own_o), (part_l, own_l))):
            copy = pltpu.make_async_copy(src.at[owner, core, rows], dst.at[at], own_sem.at[which, i])
            copy.start()
            own.append(copy)
        near.append([
            send(part_o.at[owner, 1 - core, rows], got_o.at[at], dsend.at[which, 0], drecv.at[which, 0], partner),
            send(part_l.at[owner, 1 - core, rows], got_l.at[at], dsend.at[which, 1], drecv.at[which, 1], partner),
        ])
    lax.fori_loop(0, SOON, lambda t, carry: (fetch(t), carry)[1], 0)
    meet((partner, across, diag))
    for pair in near:
        for copy in pair:
            copy.start()
    lax.fori_loop(SOON, RING_W, lambda t, carry: (fetch(t), carry)[1], 0)

    lane = lax.broadcasted_iota(jnp.int32, (8, HEAD), 1)
    far = []
    for part in range(2):
        for copy in own[2 * part:2 * part + 2]:
            copy.wait()
        for copy in near[part]:
            copy.wait_recv()

        def chip_merge(i, compact, part=part):
            j = part * PART + i
            o, l = merge([(own_o[j], own_l[j]), (got_o[j], got_l[j])])
            give_o[j] = o
            compact = jnp.where(lane == 2 * i, l[:8], compact)
            return jnp.where(lane == 2 * i + 1, l[8:], compact)

        give_l[part] = lax.fori_loop(0, PART, chip_merge, jnp.zeros((8, HEAD), F32), unroll=8)
        rows = pl.ds(part * PART, PART)
        pair = [
            send(give_l.at[part], far_l.at[part], xsend.at[part, 0], xrecv.at[part, 0], across),
            send(give_o.at[rows], far_o.at[rows], xsend.at[part, 1], xrecv.at[part, 1], across),
        ]
        for copy in pair:
            copy.start()
        far.append(pair)

    kv_all[me] = kv[...]
    new_rows = [send(kv, kv_all.at[me], ksend.at[i], krecv.at[i], peer) for i, peer in enumerate((partner, across))]
    new_rows.append(send(kv_all.at[across], kv_all.at[across], ksend.at[2], krecv.at[2], partner))

    for head in range(HALF_HEADS):
        tile = core * 4 + head // 4
        rows = pl.ds(head, TOK, stride=HALF_HEADS)
        q_rows[rows, :] = q_all[chip, tile, :, (head % 4) * HEAD:(head % 4 + 1) * HEAD].astype(F32)
        k_rows[rows, :] = kv[:, (head // 4) * HEAD:(head // 4 + 1) * HEAD].astype(F32)
        v_rows[rows, :] = kv[:, TN + (head // 4) * HEAD:TN + (head // 4 + 1) * HEAD].astype(F32)
    for copy in own[4:]:
        copy.wait()
    for copy in near[2]:
        copy.wait_recv()

    half = ROWS // 2

    def score(q, k):
        s = jnp.sum(q * k, axis=1, keepdims=True) * SCALE
        return jnp.broadcast_to(s, q.shape)

    def own_merge(i, carry):
        a = pl.ds(pl.multiple_of(i * HALF_HEADS, HALF_HEADS), HALF_HEADS)
        b = pl.ds(pl.multiple_of(half + i * HALF_HEADS, HALF_HEADS), HALF_HEADS)
        k0, v0, k1, v1 = k_rows[a, :], v_rows[a, :], k_rows[b, :], v_rows[b, :]
        q0, q1 = q_rows[a, :], q_rows[b, :]
        j = i + PART
        m, n = TOK + i, TOK + j
        o, l = merge([(own_o[m], own_l[m]), (got_o[m], got_l[m]), (v0, score(q0, k0))])
        mine_o[i] = o
        mine_l[i] = l
        o, l = merge([(own_o[n], own_l[n]), (got_o[n], got_l[n]), (v0, score(q1, k0)), (v1, score(q1, k1))])
        mine_o[j] = o
        mine_l[j] = l
        return carry

    lax.fori_loop(0, PART, own_merge, 0, unroll=2)

    for part in range(2):
        for copy in far[part]:
            copy.wait_recv()
        if part == 1:
            for copy in new_rows[:2]:
                copy.start()
            boxes.start()
        spread = far_l[part]

        def last_merge(i, carry, part=part, spread=spread):
            l = jnp.concatenate([
                jnp.broadcast_to(jnp.sum(jnp.where(lane == 2 * i + k, spread, 0.0), axis=1, keepdims=True), (8, HEAD)) for k in range(2)
            ], axis=0)
            j = part * PART + i
            o, _ = merge([(mine_o[j], mine_l[j]), (far_o[j], l)])
            q_rows[pl.ds(pl.multiple_of(j * HALF_HEADS, HALF_HEADS), HALF_HEADS), :] = o
            return carry

        lax.fori_loop(0, PART, last_merge, 0, unroll=8)
    for head in range(HALF_HEADS):
        attn[:, head * HEAD:(head + 1) * HEAD] = q_rows[pl.ds(head, TOK, stride=HALF_HEADS), :].astype(BF16)

    def reduce(j):
        return send(psend.at[j], precv.at[j], ssem.at[j], rsem.at[j], partner)

    def finish_sum(first, res, target):
        reduce(first + 7).start()
        for j in range(8):
            reduce(first + j).wait_recv()
            cols = slice(j * TN, (j + 1) * TN)
            target[:, cols] = (res[:, cols].astype(F32) + (psend[first + j] + precv[first + j])).astype(BF16)

    def project(j, carry):
        tile_copy(j, 0).wait()
        psend[j] = dot(attn[...], ring[lax.rem(j, RING_W)])
        fetch(j + RING_W)

        @pl.when(j > 0)
        def _():
            reduce(j - 1).start()
        return carry

    lax.fori_loop(0, OUT_END, project, 0)
    finish_sum(0, h_in, h)

    def up(s, carry):
        u = None
        for k in range(2):
            t = OUT_END + 2 * s + k
            tile_copy(t, 1).wait()
            part = dot(h[:, k * TK:(k + 1) * TK], ring[lax.rem(t, RING_W)])
            u = part if u is None else u + part
            fetch(t + RING_W)
        a = jax.nn.gelu(u.astype(BF16).astype(F32), approximate=True).astype(BF16)
        act[:, pl.ds(pl.multiple_of(s * TN, TN), TN)] = a
        return carry

    lax.fori_loop(0, UP_TILES, up, 0)
    new_rows[1].wait_recv()
    new_rows[2].start()

    def down(j, carry):
        total = None
        for k in range(4):
            t = UP_END + 4 * j + k
            tile_copy(t, 2).wait()
            part = dot(act[:, k * TD:(k + 1) * TD], ring[lax.rem(t, RING_W), :TD])
            total = part if total is None else total + part
            fetch(t + RING_W)
        psend[8 + j] = total

        @pl.when(j > 0)
        def _():
            reduce(8 + j - 1).start()
        return carry

    lax.fori_loop(0, D // TN, down, 0)
    finish_sum(8, h, out)

    if not last:
        def to_partner(j):
            ref = q_next.at[chip, core * 4 + j]
            return send(ref, ref, qp_send.at[j], qp_recv.at[j], partner)

        def to_across(j):
            ref = q_next.at[chip, core * 4 + j]
            return send(ref, ref, qx_send.at[j], qx_recv.at[j], across)

        def forward(j):
            ref = q_next.at[1 - chip, core * 4 + j]
            return send(ref, ref, qf_send.at[j], qf_recv.at[j], partner)

        def project_next(j, carry):
            total = None
            for k in range(2):
                t = DOWN_END + 2 * j + k
                tile_copy(t, 4).wait()
                part = dot(out[:, k * TK:(k + 1) * TK], ring[lax.rem(t, RING_W)])
                total = part if total is None else total + part
            tile = total.astype(BF16)

            @pl.when(j < 4)
            def _():
                q_next[chip, core * 4 + j] = tile

            @pl.when(j >= 4)
            def _():
                kv_next[:, pl.ds(pl.multiple_of((j - 4) * TN, TN), TN)] = tile

            @pl.when(j < 4)
            def _():
                to_across(j).start()
                to_partner(j).start()
            return carry

        lax.fori_loop(0, 6, project_next, 0)
        for j in range(4):
            to_across(j).wait_recv()
            forward(j).start()
        for j in range(4):
            to_across(j).wait_send()
            to_partner(j).wait()
            forward(j).wait()
    for j in range(16):
        reduce(j).wait_send()
    for pair in near + far:
        for copy in pair:
            copy.wait_send()
    new_rows[0].wait()
    new_rows[1].wait_send()
    new_rows[2].wait()
    boxes.wait()


def run_rest(layer, lane_core, h, q_all, kv, part_o, part_l, outbox, w_out, w_up, w_down, *weights):
    more = [jax.ShapeDtypeStruct((2, 8, TOK, TN), BF16), jax.ShapeDtypeStruct((TOK, 2 * TN), BF16)] if weights else []
    token = (HALF_HEADS, HEAD)
    return pl.pallas_call(
        functools.partial(rest_kernel, layer, lane_core),
        name=f'rest{layer}_{lane_core}',
        out_shape=[jax.ShapeDtypeStruct((TOK, D), BF16), jax.ShapeDtypeStruct((4, TOK, 2 * TN), BF16), BOX] + more,
        in_specs=[VMEM] * 3 + [ANY] * (6 + len(weights)),
        out_specs=[VMEM, VMEM, ANY] + [VMEM] * len(more),
        scratch_shapes=[
            pltpu.VMEM((RING_W, TK, TN), BF16),
            DMA((RING_W,)),
            pltpu.VMEM((2 * TOK,) + token, F32),
            pltpu.VMEM((2 * TOK,) + token, F32),
            DMA((3, 2)),
            pltpu.VMEM((2 * TOK,) + token, F32),
            pltpu.VMEM((2 * TOK,) + token, F32),
            pltpu.VMEM((TOK,) + token, F32),
            pltpu.VMEM((TOK,) + token, F32),
            pltpu.VMEM((TOK,) + token, F32),
            pltpu.VMEM((2, 8, HEAD), F32),
            pltpu.VMEM((TOK,) + token, F32),
            pltpu.VMEM((2, 8, HEAD), F32),
            pltpu.VMEM((ROWS, HEAD), F32),
            pltpu.VMEM((ROWS, HEAD), F32),
            pltpu.VMEM((ROWS, HEAD), F32),
            pltpu.VMEM((TOK, 2048), BF16),
            pltpu.VMEM((TOK, FF // 2), BF16),
            pltpu.VMEM((TOK, D), BF16),
            pltpu.VMEM((16, TOK, TN), F32),
            pltpu.VMEM((16, TOK, TN), F32),
            DMA((3, 2)),
            DMA((3, 2)),
            DMA((2, 2)),
            DMA((2, 2)),
            DMA((16,)),
            DMA((16,)),
            DMA((3,)),
            DMA((3,)),
            DMA((3, MIG // CHUNK)),
            DMA((3, MIG // CHUNK)),
        ] + [DMA((4,))] * (6 if weights else 0),
        cost_estimate=pl.CostEstimate(flops=2 * TOK * D * FF * 8, bytes_accessed=D * FF * 2, transcendentals=0),
        compiler_params=pltpu.CompilerParams(collective_id=2 + layer * 2 + lane_core, has_side_effects=True, vmem_limit_bytes=67043328),
    )(h, q_all, kv, part_o, part_l, w_out, w_up, w_down, outbox, *weights)


def move_kernel(outbox, inbox, send_sems, recv_sems):
    me, chip, core, partner, across, diag = places()
    meet((partner, across, diag))
    boxes = Boxes(EVERYTHING, outbox, inbox, send_sems, recv_sems)
    boxes.start()
    boxes.wait()


def run_move(layer, outbox):
    return pl.pallas_call(
        move_kernel,
        name=f'move{layer}',
        out_shape=BOX,
        in_specs=[ANY],
        out_specs=ANY,
        scratch_shapes=[DMA((3, MIG // CHUNK)), DMA((3, MIG // CHUNK))],
        compiler_params=pltpu.CompilerParams(collective_id=6 + layer, has_side_effects=True),
    )(outbox)


def run_blank(layer):
    return pl.pallas_call(lambda box: None, name=f'blank{layer}', out_shape=BOX, out_specs=ANY)()


RING = 32
AHEAD = RING // 2


def finish_kernel(meta, moved, gone, rows, inbox, spare, late, kv0, kv1, k_in, v_in, k_out, v_out, wide, row_buf, zeros, buf, in_sem, out_sem, zero_sem, row_sem):
    del k_in, v_in
    outs = (k_out, v_out)
    count = meta[2]

    def loop(first, last, body):
        lax.fori_loop(first, last, lambda i, carry: (body(i), carry)[1], 0)

    def clear(i):
        return [pltpu.make_async_copy(zeros, out.at[gone[i]], zero_sem) for out in outs]

    def is_late(i):
        return (moved[1, i] >= 2 * MIG + LATE) & (meta[1] < 2)

    def load(i, box):
        slot = lax.rem(i, RING)
        return [pltpu.make_async_copy(box.at[moved[1, i], p], buf.at[slot, p, 1], in_sem.at[slot, p]) for p in range(2)]

    def load_late(i):
        slot = lax.rem(i, RING)
        return [pltpu.make_async_copy(late.at[moved[1, i] - (2 * MIG + LATE), p], buf.at[slot, p], in_sem.at[slot, p]) for p in range(2)]

    def store(i):
        slot = lax.rem(i, RING)
        return [pltpu.make_async_copy(buf.at[slot, p, 1], outs[p].at[moved[0, i], 1], out_sem.at[slot, p]) for p in range(2)]

    def store_late(i):
        slot = lax.rem(i, RING)
        return [pltpu.make_async_copy(buf.at[slot, p], outs[p].at[moved[0, i]], out_sem.at[slot, p]) for p in range(2)]

    def begin(group):
        for copy in group:
            copy.start()

    def end(group):
        for copy in group:
            copy.wait()

    def begin_load(i):
        pl.when((meta[1] < 2) & jnp.logical_not(is_late(i)))(lambda: begin(load(i, inbox)))
        pl.when(is_late(i))(lambda: begin(load_late(i)))
        pl.when(meta[1] == 2)(lambda: begin(load(i, spare)))

    def begin_store(i):
        @pl.when(is_late(i))
        def _():
            end(load_late(i))
            begin(store_late(i))

        @pl.when(jnp.logical_not(is_late(i)))
        def _():
            end(load(i, inbox))
            begin(store(i))

    def end_store(i):
        pl.when(is_late(i))(lambda: end(store_late(i)))
        pl.when(jnp.logical_not(is_late(i)))(lambda: end(store(i)))

    loop(0, jnp.minimum(count, AHEAD), begin_load)
    zeros[...] = jnp.zeros_like(zeros)
    loop(0, meta[4], lambda i: begin(clear(i)))

    for l, kv in enumerate((kv0, kv1)):
        for p in range(2):
            for dev in range(4):
                for i in range(4):
                    for t in range(2):
                        at = pl.ds((dev // 2) * TOK * KV_HEADS + t * KV_HEADS + (dev % 2) * 4 + i, TOK // 2, stride=2 * KV_HEADS)
                        wide[at, :] = kv[dev, t * 32:(t + 1) * 32, (p * 4 + i) * HEAD:(p * 4 + i + 1) * HEAD].astype(F32)
            row_buf[p, l] = wide[...].astype(BF16)

    def page(i):
        begin_store(i)

        @pl.when(i + AHEAD < count)
        def _():
            pl.when(i >= AHEAD)(lambda: end_store(i - AHEAD))
            begin_load(i + AHEAD)

    loop(0, count, page)
    loop(jnp.maximum(count - RING, 0), count, end_store)

    def row(i):
        at = pl.ds(pl.multiple_of(rows[1, i] * KV_HEADS, KV_HEADS), 2 * KV_HEADS)
        src = pl.ds(pl.multiple_of(rows[2, i] * 2 * KV_HEADS, 2 * KV_HEADS), 2 * KV_HEADS)
        return [pltpu.make_async_copy(row_buf.at[p, :, src, :], outs[p].at[rows[0, i], :, at, :], row_sem.at[p]) for p in range(2)]

    loop(0, meta[3], lambda i: begin(row(i)))
    loop(0, meta[3], lambda i: end(row(i)))
    loop(0, meta[4], lambda i: end(clear(i)))


def run_finish(meta, moved, gone, rows, boxes, kvs, k_part, v_part):
    shape = jax.ShapeDtypeStruct(k_part.shape, BF16)
    return pl.pallas_call(
        finish_kernel,
        name='finish',
        out_shape=[shape, shape],
        in_specs=[SMEM] * 4 + [ANY, ANY, ANY, VMEM, VMEM, ANY, ANY],
        out_specs=[ANY, ANY],
        scratch_shapes=[
            pltpu.VMEM((2 * TOK * KV_HEADS, HEAD), F32),
            pltpu.VMEM((2, LAYERS, 2 * TOK * KV_HEADS, HEAD), BF16),
            pltpu.VMEM(k_part.shape[1:], BF16),
            pltpu.VMEM((RING, 2) + k_part.shape[1:], BF16),
            DMA((RING, 2)),
            DMA((RING, 2)),
            DMA,
            DMA((2,)),
        ],
        input_output_aliases={9: 0, 10: 1},
        cost_estimate=pl.CostEstimate(flops=10 ** 10, bytes_accessed=16 * 2 ** 20, transcendentals=0),
        compiler_params=pltpu.CompilerParams(vmem_limit_bytes=VMEM_LIMIT),
    )(meta, moved, gone, rows, *boxes, *kvs, k_part, v_part)


def solution(mesh):
    pool_spec = P(('rep', 'kv'))
    tok_spec = P(None, ('rep', 'kv'), None)

    def device_fn(embeds, w_query, w_key, w_value, w_out, w_up, w_down, k_pool, v_pool, new_table, seq_lens, mig_src, mig_dst):
        me = lax.axis_index('kv')
        weights = (w_query, w_key, w_value)
        k_flat, v_flat = flat_pool(k_pool), flat_pool(v_pool)
        meta, items, slots, gone, moved, where, lates, lane, general = run_plan(new_table, seq_lens, mig_src, mig_dst)
        q_all, kv, h = run_qkv(0, embeds, weights, True)
        part_o, part_l, outbox, k_kept, late_box = run_attend(0, meta, items, slots, q_all, k_flat, v_flat, lates)

        def extra_boxes(layer, outbox):
            return lax.switch(general.reshape(()), [lambda box: run_blank(layer), functools.partial(run_move, layer)], outbox)

        def layers(core, h, q_all, kv, part_o, part_l, outbox, late_box, k_kept):
            h, kv_all0, inbox, q_all, kv = run_rest(0, core, h, q_all, kv, part_o, part_l, outbox, w_out, w_up, w_down, *weights)
            spare = extra_boxes(0, outbox)
            late_box, q_all = lax.optimization_barrier((late_box, q_all))
            late = lax.ppermute(late_box, 'kv', [(core, 3 - core), (2 + core, 1 - core)])
            part_o, part_l, outbox, v_kept, k_kept = run_attend(1, meta, items, slots, q_all, k_flat, v_flat, moved, inbox, spare, k_kept)
            h, kv_all1, inbox = run_rest(1, core, h, q_all, kv, part_o, part_l, outbox, w_out, w_up, w_down)
            return h, kv_all0, kv_all1, inbox, extra_boxes(1, outbox), late, k_kept, v_kept

        forms = [functools.partial(layers, core) for core in range(2)]
        h, kv_all0, kv_all1, inbox, spare, late, k_kept, v_kept = lax.switch(lane.reshape(()), forms, h, q_all, kv, part_o, part_l, outbox, late_box, k_kept)
        k_out, v_out = run_finish(meta, moved, gone, where, (inbox, spare, late), (kv_all0, kv_all1), k_kept, v_kept)
        k_out, v_out = k_out.reshape(k_pool.shape), v_out.reshape(v_pool.shape)
        y = lax.dynamic_slice_in_dim(h.reshape(2, 32, D), (me % 2) * 16, 16, axis=1)
        return y, k_out, v_out

    return jax.shard_map(device_fn, mesh=mesh, in_specs=(tok_spec, P(), P(), P(), P(), P(), P(), pool_spec, pool_spec, P('rep', None), P('rep'), P('rep'), P('rep')), out_specs=(tok_spec, pool_spec, pool_spec), check_vma=False)
```
